128 devices in a mesh: gx: 16 (over y, x), gy: 8 (over z, core).
Axes of the slice: x: 4, y: 4, z: 4, core: 2. Of those that a mesh axis runs over, the one named last changes fastest.
Arguments:
- point_feats: bfloat16 [1048576, 128], P(('gx', 'gy')), may hold values from -6 to 6
- point_tile: int32 [1048576, 1], P(('gx', 'gy')), may hold values from 0 to 127; in each aligned block of 8192 rows (0 to 8191, 8192 to 16383, ...) at most 80 rows name the same one
- point_cell: int32 [1048576], P(('gx', 'gy')), may hold values from 0 to 4095
- point_count: int32 [128], P(('gx', 'gy')), may hold values from 6144 to 8192, as said below
- conv_weight: bfloat16 [3, 3, 128, 128], replicated, may hold values from -0.1875 to 0.1875
- conv_bias: float32 [128], replicated, may hold values from -3 to 3
Outputs:
- bev_map: bfloat16 [256, 2048, 128], P('gx', 'gy')
- conv_out: bfloat16 [256, 2048, 128], P('gx', 'gy')
The draws below stay inside these ranges and needn't reach their ends.
Inputs may be any that keep to these rules, and one draw needn't show every extreme that they name: `point_tile`: among the 8192 rows of one device no tile is named by more than 80 rows, a bound that some block reaches. `point_count`: only slots below a device's count are live; some device has all 8192 slots live.
All inputs are finite; a program needn't handle non-finite values.
Results may differ from the reference program's by a relative error of at most 0.0045.
Values may be sent and summed in bfloat16 or wider, within the bound.
No kernel may reach another device: no remote copies, remote signals or barrier semaphores. Data moves between devices by JAX's collectives and lax.ppermute only.
A program may use at most 64 MiB of HBM per device.

```python
import math
import jax
import jax.numpy as jnp
import numpy as np
from jax import lax

C = 128
COLS_DEV = 256
ROWS_DEV = 16
P_DEV = 8192
CAP = 80
POINTS = 1048576
MAP_ROWS = 256
MAP_COLS = 2048
N_GY = 8
DEVICES = 128


def draw_point_count(key, part):
    counts = jax.random.randint(key, (DEVICES,), 3 * P_DEV // 4, P_DEV + 1).astype(jnp.int32)
    fullest = jax.random.randint(jax.random.fold_in(key, 7), (), 0, DEVICES)
    return counts.at[fullest].set(P_DEV)


def with_ends(array, key, low, high):
    longest = array.shape.index(max(array.shape))
    spots = []
    for shift in (0, 1):
        where = [jax.random.randint(jax.random.fold_in(key, axis), (), 0, length) for axis, length in enumerate(array.shape)]
        where[longest] = (where[longest] + shift) % array.shape[longest]
        spots.append(tuple(where))
    return array.at[spots[0]].set(low).at[spots[1]].set(high)


def level_of(own_key, dims, cuts, low, largest):
    loudness, own = 1.0, jax.random.fold_in(own_key, 6)
    for dim, blocks in cuts:
        steps = jnp.exp(jax.random.uniform(jax.random.fold_in(own, dim), (blocks,), jnp.float32, low / len(cuts), largest / len(cuts)))
        loudness = loudness * jnp.repeat(steps, dims[dim] // blocks).reshape([-1 if axis == dim else 1 for axis in range(len(dims))])
    return loudness


def routed_block(own_key, own, number, rows, count, top, most, slope):
    sequence = jax.random.permutation(own_key, count)
    packed, usual = load_shares(count, rows * top, most, slope, True), load_shares(count, rows * top, most, slope, False)
    places = jnp.arange(count)

    def named(lengths, rotation):
        used = int((lengths > 0).sum())
        fixed = max(1, used // 4)
        passed = fixed + (places - fixed + rotation * (used - fixed)) % max(1, count - fixed)
        return jnp.zeros((count,), jnp.int32).at[sequence[jnp.where(places < fixed, places, passed)]].set(jnp.asarray(lengths, jnp.int32))

    lengths = jnp.where(number % 4 == 0, named(packed, number // 4), named(usual, number - number // 4 - 1))
    mixed = jax.random.permutation(jax.random.fold_in(own, 3), count)
    source_of, sink = mixed[0:count // 2 * 2:2], mixed[1:count // 2 * 2:2]
    margin = jnp.minimum(lengths[source_of] - 1, most - lengths[sink]) // 2
    margin = jnp.where((source_of == sequence[0]) | (sink == sequence[0]) | (lengths[sink] == 0), 0, jnp.maximum(margin, 0))
    passed = jax.random.randint(jax.random.fold_in(own, 4), (count // 2,), 0, 1 << 20) % (margin + 1)
    lengths = lengths.at[source_of].add(-passed).at[sink].add(passed)
    labels = jnp.searchsorted(jnp.cumsum(lengths), jnp.arange(rows * top), side="right").astype(jnp.int32)
    grid = labels.reshape(top, rows).T
    grid = grid[jax.random.permutation(jax.random.fold_in(own, 1), rows)]
    rotation = jax.random.randint(jax.random.fold_in(own, 2), (rows, 1), 0, top)
    return jnp.take_along_axis(grid, (jnp.arange(top)[None, :] + rotation) % top, axis=1)


def load_shares(number_of, total, bound, lean, full):
    loads = [(1 << 20) // math.isqrt(grade ** lean) + 1 for grade in range(1, number_of + 1)]
    largest = bound if full else min(bound, max(-(-total // number_of), total * loads[0] // sum(loads)))
    least = 1 if total - largest >= number_of - 1 else 0
    holding, spare = [largest] + [least] * (number_of - 1), total - largest - least * (number_of - 1)
    while spare > 0:
        candidates = [i for i in range(1, number_of) if holding[i] < largest] or [i for i in range(1, number_of) if holding[i] < bound]
        pool, left = sum([loads[i] for i in candidates]), spare
        for i in candidates:
            more = min(bound - holding[i], max(1, left * loads[i] // pool), spare)
            holding[i] = holding[i] + more
            spare = spare - more
    return np.array(holding)


def scatter_about(own_key, dims, deviation, reach, cuts=(), kind=jnp.bfloat16):
    drawn = jax.random.normal(own_key, dims, jnp.float32) * deviation
    if len(cuts) > 0:
        drawn = level_of(own_key, dims, cuts, -0.22, 0.18) * drawn
    return jnp.clip(drawn, min=-reach, max=reach).astype(kind)


def setup_inputs(seed: int = 0) -> dict:
    seeds = jax.random.split(jax.random.key(seed), 7)
    point_feats = scatter_about(seeds[0], (POINTS, C), 1.0, 6.0, ((0, 128),))
    point_tile_keys = jax.random.split(jax.random.fold_in(seeds[1], 1), POINTS // P_DEV)
    point_tile_turns = jax.random.permutation(jax.random.fold_in(seeds[1], 3), POINTS // P_DEV)
    point_tile = jax.vmap(lambda own, number: routed_block(jax.random.fold_in(seeds[1], 2), own, number, P_DEV, DEVICES, 1, CAP, 2))(point_tile_keys, point_tile_turns).reshape((POINTS, 1))
    point_cell = with_ends(jax.random.randint(seeds[2], (POINTS,), 0, ROWS_DEV * COLS_DEV), jax.random.fold_in(seeds[2], 1), 0, (ROWS_DEV * COLS_DEV) - 1).astype(jnp.int32)
    point_count = draw_point_count(jax.random.fold_in(seeds[6], 71), 0)
    conv_weight = scatter_about(seeds[4], (3, 3, C, C), (9 * C) ** -0.5, 0.1875)
    conv_bias = scatter_about(seeds[5], (C,), 0.5, 3.0, (), jnp.float32)
    return dict(point_feats=point_feats, point_tile=point_tile, point_cell=point_cell, point_count=point_count, conv_weight=conv_weight, conv_bias=conv_bias)


def reference(point_feats, point_tile, point_cell, point_count, conv_weight, conv_bias):
    tile = point_tile[:, 0]
    rows = (tile // N_GY) * ROWS_DEV + point_cell // COLS_DEV
    cols = (tile % N_GY) * COLS_DEV + point_cell % COLS_DEV
    cell = rows * MAP_COLS + cols
    slot = jnp.arange(POINTS, dtype=jnp.int32)
    block = slot // P_DEV
    live = (slot % P_DEV) < point_count[block]
    feats = jnp.where(live[:, None], point_feats.astype(jnp.float32), 0.0)
    sums = jax.ops.segment_sum(feats, cell, num_segments=MAP_ROWS * MAP_COLS)
    bev_map = sums.reshape(MAP_ROWS, MAP_COLS, C).astype(jnp.bfloat16)
    conv = lax.conv_general_dilated(bev_map.astype(jnp.float32)[None], conv_weight.astype(jnp.float32), (1, 1), "SAME", dimension_numbers=("NHWC", "HWIO", "NHWC"), precision=lax.Precision.HIGHEST)[0]
    conv_out = jax.nn.relu(conv + conv_bias).astype(jnp.bfloat16)
    return bev_map, conv_out
```

```python
import jax
import jax.numpy as jnp
from jax import lax
from jax.experimental import pallas as pl
from jax.experimental.pallas import tpu as pltpu
from jax.sharding import PartitionSpec as P

COLS_DEV = 256
ROWS_DEV = 16
CELLS = ROWS_DEV * COLS_DEV
LANES = 128
CAP = 80
BLOCK = 88
SUMS = 4
DUMP = CELLS
GROUP = 8


def pack_kernel(
    count_ref, cell_ref, tile_ref, feats_ref, out_ref, rows, slots, pos_v, pos_s, cells_s, cells_v, sem
):
    count = count_ref[0]
    chunks = tile_ref.shape[0]
    tiles = out_ref.shape[0]
    tile_id = lax.broadcasted_iota(jnp.int32, (tiles, LANES), 0)
    lane = lax.broadcasted_iota(jnp.int32, (1, LANES), 1)
    base = (tile_id * LANES - 1).astype(jnp.float32)
    source = lax.broadcasted_iota(jnp.int32, (LANES, 2 * LANES), 0)
    column = lax.broadcasted_iota(jnp.int32, (LANES, 2 * LANES), 1)
    upto = jnp.where((source <= column) | (column >= LANES), 1.0, 0.0).astype(jnp.bfloat16)

    def rank(i, before):
        live = i * LANES + lane < count
        hit = tile_id == jnp.where(live, tile_ref[pl.ds(i, 1), :], -1)
        found = jnp.dot(
            jnp.where(hit, 1.0, 0.0).astype(jnp.bfloat16), upto, preferred_element_type=jnp.float32
        )
        place = found[:, :LANES] + before
        slot = jnp.sum(jnp.where(hit, place, 0.0), axis=0, keepdims=True)
        pos_v[pl.ds(i, 1), :] = jnp.where(live, slot.astype(jnp.int32), tiles * LANES - 1)
        return before + found[:, LANES:]

    total = lax.fori_loop(0, chunks, rank, base) - base
    to_smem = pltpu.make_async_copy(pos_v, pos_s, sem)
    to_smem.start()

    def widen(i, carry):
        at = pl.ds(pl.multiple_of(i * LANES, LANES), LANES)
        rows[at, :] = feats_ref[at, :].astype(jnp.float32)
        return carry

    lax.fori_loop(0, chunks, widen, 0)
    to_smem.wait()

    def move(i, carry):
        def few(g, inner):
            for j in range(GROUP):
                k = g * GROUP + j
                slot = pos_s[i, k]
                cells_s[lax.shift_right_logical(slot, 7), slot & (LANES - 1)] = cell_ref[i, k]
                slots[pl.ds(slot, 1), :] = rows[pl.ds(i * LANES + k, 1), :]
            return inner

        return lax.fori_loop(0, LANES // GROUP, few, carry)

    lax.fori_loop(0, (count + LANES - 1) // LANES, move, 0)
    to_vmem = pltpu.make_async_copy(cells_s, cells_v, sem)
    to_vmem.start()
    to_vmem.wait()
    number = total.astype(jnp.int32)
    cell = jnp.where(lane < number, cells_v[...], DUMP)
    cell = jnp.where(lane == LANES - 1, number, cell)
    slots[pl.ds(CAP, tiles, LANES), :] = lax.shift_right_logical(cell, 6).astype(jnp.float32)
    slots[pl.ds(CAP + 1, tiles, LANES), :] = (cell & 63).astype(jnp.float32)

    def narrow(t, carry):
        out_ref[t] = slots[pl.ds(pl.multiple_of(t * LANES, LANES), BLOCK), :].astype(jnp.bfloat16)
        return carry

    lax.fori_loop(0, tiles, narrow, 0)


def add_kernel(got_ref, out_ref, rows, cells_v, cells_s, sem, *sums):
    sources = got_ref.shape[0]

    def widen(s, carry):
        rows[pl.ds(pl.multiple_of(s * BLOCK, 8), BLOCK), :] = got_ref[s].astype(jnp.float32)
        return carry

    lax.fori_loop(0, sources, widen, 0)
    high = rows[pl.ds(CAP, sources, BLOCK), :].astype(jnp.int32)
    low = rows[pl.ds(CAP + 1, sources, BLOCK), :].astype(jnp.int32)
    cells_v[...] = high * 64 + low
    to_smem = pltpu.make_async_copy(cells_v, cells_s, sem)
    to_smem.start()
    for part in sums:
        part[...] = jnp.zeros_like(part)
    to_smem.wait()

    def one(s, carry):
        number = cells_s[s, LANES - 1]

        def few(g, inner):
            for j in range(GROUP):
                k = g * GROUP + j
                at = pl.ds(cells_s[s, k], 1)
                part = sums[j % SUMS]
                part[at, :] = part[at, :] + rows[pl.ds(s * BLOCK + k, 1), :]
            return inner

        return lax.fori_loop(0, (number + GROUP - 1) // GROUP, few, carry)

    lax.fori_loop(0, sources, one, 0)
    step = 256

    def close(i, carry):
        at = pl.ds(pl.multiple_of(i * step, step), step)
        total = sums[0][at, :]
        for part in sums[1:]:
            total = total + part[at, :]
        out_ref[at, :] = total.astype(jnp.bfloat16)
        return carry

    lax.fori_loop(0, CELLS // step, close, 0)


def with_halo(cells, sides, width):
    for axis, dim in sides:
        count = lax.axis_size(axis)
        ends = count - 1
        head = lax.slice_in_dim(cells, 0, width, axis=dim)
        tail = lax.slice_in_dim(cells, cells.shape[dim] - width, cells.shape[dim], axis=dim)
        cells = jnp.concatenate(
            [
                lax.ppermute(tail, axis, [(i, (i + 1) % count) for i in range(ends)]),
                cells,
                lax.ppermute(head, axis, [((i + 1) % count, i) for i in range(ends)]),
            ],
            axis=dim,
        )
    return cells


VMEM = pl.BlockSpec(memory_space=pltpu.VMEM)
SMEM = pl.BlockSpec(memory_space=pltpu.SMEM)


def pack(point_feats, point_tile, point_cell, point_count, devices):
    points, channels = point_feats.shape
    chunks = points // LANES
    return pl.pallas_call(
        pack_kernel,
        out_shape=jax.ShapeDtypeStruct((devices, BLOCK, channels), jnp.bfloat16),
        in_specs=[SMEM, SMEM, VMEM, VMEM],
        out_specs=VMEM,
        scratch_shapes=[
            pltpu.VMEM((points, channels), jnp.float32),
            pltpu.VMEM((devices * LANES, channels), jnp.float32),
            pltpu.VMEM((chunks, LANES), jnp.int32),
            pltpu.SMEM((chunks, LANES), jnp.int32),
            pltpu.SMEM((devices, LANES), jnp.int32),
            pltpu.VMEM((devices, LANES), jnp.int32),
            pltpu.SemaphoreType.DMA,
        ],
        name="pack",
    )(
        point_count,
        point_cell.reshape(chunks, LANES),
        point_tile.reshape(chunks, LANES),
        point_feats,
    )


def add_up(got):
    devices, block, channels = got.shape
    return pl.pallas_call(
        add_kernel,
        out_shape=jax.ShapeDtypeStruct((CELLS, channels), jnp.bfloat16),
        in_specs=[VMEM],
        out_specs=VMEM,
        scratch_shapes=[
            pltpu.VMEM((devices * block, channels), jnp.float32),
            pltpu.VMEM((devices, LANES), jnp.int32),
            pltpu.SMEM((devices, LANES), jnp.int32),
            pltpu.SemaphoreType.DMA,
        ]
        + [pltpu.VMEM((CELLS + 8, channels), jnp.float32)] * SUMS,
        name="add_up",
    )(got)


def shards(point_feats, point_tile, point_cell, point_count, conv_weight, conv_bias):
    devices = lax.axis_size("gx") * lax.axis_size("gy")
    channels = point_feats.shape[1]
    sent = pack(point_feats, point_tile, point_cell, point_count, devices)
    got = lax.all_to_all(sent, ("gx", "gy"), split_axis=0, concat_axis=0, tiled=True)
    bev_map = add_up(got).reshape(ROWS_DEV, COLS_DEV, channels)
    padded = with_halo(bev_map, (("gx", 0), ("gy", 1)), 1)
    total = lax.conv_general_dilated(
        padded[None],
        conv_weight,
        (1, 1),
        "VALID",
        dimension_numbers=("NHWC", "HWIO", "NHWC"),
        preferred_element_type=jnp.float32,
    )[0]
    conv_out = jax.nn.relu(total + conv_bias).astype(jnp.bfloat16)
    return (bev_map, conv_out)


def solution(mesh):
    in_specs = (
        P(("gx", "gy"), None),
        P(("gx", "gy"), None),
        P(("gx", "gy")),
        P(("gx", "gy")),
        P(),
        P(),
    )
    out_specs = (P("gx", "gy", None), P("gx", "gy", None))
    return jax.shard_map(shards, mesh=mesh, in_specs=in_specs, out_specs=out_specs, check_vma=False)
```

```python
import jax
import jax.numpy as jnp
from jax import lax
from jax.experimental import pallas as pl
from jax.experimental.pallas import tpu as pltpu
from jax.sharding import PartitionSpec as P

COLS_DEV = 256
ROWS_DEV = 16
CELLS = ROWS_DEV * COLS_DEV
LANES = 128
CAP = 80
BLOCK = 88
SUMS = 8
DUMP = CELLS
GROUP = 16


def pack_kernel(
    count_ref, cell_ref, tile_ref, feats_ref, out_ref, rows, slots, pos_v, pos_f, pos_s, coded, sem
):
    count = count_ref[0]
    chunks, width = tile_ref.shape
    tiles = out_ref.shape[0]
    tile_id = lax.broadcasted_iota(jnp.int32, (tiles, width), 0)
    lane = lax.broadcasted_iota(jnp.int32, (1, width), 1)
    source = lax.broadcasted_iota(jnp.int32, (width, width + LANES), 0)
    column = lax.broadcasted_iota(jnp.int32, (width, width + LANES), 1)
    upto = jnp.where((source <= column) | (column >= width), 1.0, 0.0).astype(jnp.bfloat16)
    first = (lax.broadcasted_iota(jnp.int32, (tiles, LANES), 0) * LANES - 1).astype(jnp.float32)

    def rank(i, before):
        live = i * width + lane < count
        hit = tile_id == jnp.where(live, tile_ref[pl.ds(i, 1), :], -1)
        found = jnp.dot(
            jnp.where(hit, 1.0, 0.0).astype(jnp.bfloat16), upto, preferred_element_type=jnp.float32
        )
        place = found[:, :width] + jnp.concatenate([before] * (width // LANES), axis=1)
        slot = jnp.sum(jnp.where(hit, place, 0.0), axis=0, keepdims=True)
        pos_v[pl.ds(i, 1), :] = jnp.where(live, slot.astype(jnp.int32), tiles * LANES - 1)
        at = pl.ds(pl.multiple_of(i * width, width), width)
        rows[at, :] = feats_ref[at, :].astype(jnp.float32)
        return before + found[:, width:]

    total = lax.fori_loop(0, chunks, rank, first, unroll=4) - first
    for i in range(chunks):
        pos_f[pl.ds(i * width, width)] = pos_v[i, :]
    to_smem = pltpu.make_async_copy(pos_f, pos_s, sem)
    to_smem.start()
    coded[...] = jnp.zeros_like(coded)
    to_smem.wait()

    def move(i, carry):
        start = i * width
        for k in range(width):
            slots[pl.ds(pos_s[start + k], 1), :] = rows[pl.ds(start + k, 1), :]
        live = start + lane < count
        hit = tile_id == jnp.where(live, tile_ref[pl.ds(i, 1), :], -1)
        level = pos_v[pl.ds(i, 1), :] & (LANES - 1)
        at_level = lax.broadcasted_iota(jnp.int32, (LANES, width), 0) == level
        cell = cell_ref[pl.ds(i, 1), :]
        high = lax.shift_right_logical(cell, 6).astype(jnp.float32)
        low = (cell & 63).astype(jnp.float32)
        values = jnp.concatenate([jnp.where(hit, high, 0.0), jnp.where(hit, low, 0.0)], axis=0)
        coded[...] += lax.dot_general(
            values.astype(jnp.bfloat16),
            jnp.where(at_level, 1.0, 0.0).astype(jnp.bfloat16),
            (((1,), (1,)), ((), ())),
            preferred_element_type=jnp.float32,
        )
        return carry

    lax.fori_loop(0, (count + width - 1) // width, move, 0)
    spot = lax.broadcasted_iota(jnp.int32, (tiles, LANES), 1).astype(jnp.float32)
    high = jnp.where(spot < total, coded[:tiles, :], float(DUMP // 64))
    low = jnp.where(spot < total, coded[tiles:, :], 0.0)
    slots[pl.ds(CAP, tiles, LANES), :] = jnp.where(spot == LANES - 1, 0.0, high)
    slots[pl.ds(CAP + 1, tiles, LANES), :] = jnp.where(spot == LANES - 1, total, low)

    def narrow(t, carry):
        out_ref[t] = slots[pl.ds(pl.multiple_of(t * LANES, LANES), BLOCK), :].astype(jnp.bfloat16)
        return carry

    lax.fori_loop(0, tiles, narrow, 0, unroll=4)


def add_kernel(got_ref, out_ref, rows, cells_f, cells_s, sem, *sums):
    sources = got_ref.shape[0]

    def widen(s, carry):
        rows[pl.ds(pl.multiple_of(s * BLOCK, 8), BLOCK), :] = got_ref[s].astype(jnp.float32)
        return carry

    lax.fori_loop(0, sources, widen, 0, unroll=4)
    high = rows[pl.ds(CAP, sources, BLOCK), :].astype(jnp.int32)
    low = rows[pl.ds(CAP + 1, sources, BLOCK), :].astype(jnp.int32)
    cells_f[...] = (high * 64 + low).reshape(sources * LANES)
    to_smem = pltpu.make_async_copy(cells_f, cells_s, sem)
    to_smem.start()

    def clear(i, carry):
        for part in sums:
            part[pl.ds(pl.multiple_of(i * 256, 256), 256), :] = jnp.zeros((256, LANES), jnp.float32)
        return carry

    lax.fori_loop(0, CELLS // 256, clear, 0)
    for part in sums:
        part[pl.ds(CELLS, 8), :] = jnp.zeros((8, LANES), jnp.float32)
    to_smem.wait()

    def one(s, carry):
        number = cells_s[s * LANES + LANES - 1]

        def few(g, inner):
            at = s * LANES + g * GROUP
            base = s * BLOCK + g * GROUP
            for j in range(GROUP):
                cell = pl.ds(cells_s[at + j], 1)
                part = sums[j % SUMS]
                part[cell, :] = part[cell, :] + rows[pl.ds(base + j, 1), :]
            return inner

        return lax.fori_loop(0, lax.shift_right_logical(number + (GROUP - 1), 4), few, carry)

    lax.fori_loop(0, sources, one, 0)
    step = 256

    def close(i, carry):
        at = pl.ds(pl.multiple_of(i * step, step), step)
        total = sums[0][at, :]
        for part in sums[1:]:
            total = total + part[at, :]
        out_ref[at, :] = total.astype(jnp.bfloat16)
        return carry

    lax.fori_loop(0, CELLS // step, close, 0)


def with_halo(cells, sides, width):
    for axis, dim in sides:
        count = lax.axis_size(axis)
        ends = count - 1
        head = lax.slice_in_dim(cells, 0, width, axis=dim)
        tail = lax.slice_in_dim(cells, cells.shape[dim] - width, cells.shape[dim], axis=dim)
        cells = jnp.concatenate(
            [
                lax.ppermute(tail, axis, [(i, (i + 1) % count) for i in range(ends)]),
                cells,
                lax.ppermute(head, axis, [((i + 1) % count, i) for i in range(ends)]),
            ],
            axis=dim,
        )
    return cells


VMEM = pl.BlockSpec(memory_space=pltpu.VMEM)
SMEM = pl.BlockSpec(memory_space=pltpu.SMEM)


def pack(point_feats, point_tile, point_cell, point_count, devices):
    points, channels = point_feats.shape
    width = 2 * LANES
    chunks = points // width
    return pl.pallas_call(
        pack_kernel,
        out_shape=jax.ShapeDtypeStruct((devices, BLOCK, channels), jnp.bfloat16),
        in_specs=[SMEM, VMEM, VMEM, VMEM],
        out_specs=VMEM,
        scratch_shapes=[
            pltpu.VMEM((points, channels), jnp.float32),
            pltpu.VMEM((devices * LANES, channels), jnp.float32),
            pltpu.VMEM((chunks, width), jnp.int32),
            pltpu.VMEM((points,), jnp.int32),
            pltpu.SMEM((points,), jnp.int32),
            pltpu.VMEM((2 * devices, LANES), jnp.float32),
            pltpu.SemaphoreType.DMA,
        ],
        name="pack",
    )(
        point_count,
        point_cell.reshape(chunks, width),
        point_tile.reshape(chunks, width),
        point_feats,
    )


def add_up(got):
    devices, block, channels = got.shape
    return pl.pallas_call(
        add_kernel,
        out_shape=jax.ShapeDtypeStruct((CELLS, channels), jnp.bfloat16),
        in_specs=[VMEM],
        out_specs=VMEM,
        scratch_shapes=[
            pltpu.VMEM((devices * block, channels), jnp.float32),
            pltpu.VMEM((devices * LANES,), jnp.int32),
            pltpu.SMEM((devices * LANES,), jnp.int32),
            pltpu.SemaphoreType.DMA,
        ]
        + [pltpu.VMEM((CELLS + 8, channels), jnp.float32)] * SUMS,
        name="add_up",
    )(got)


def shards(point_feats, point_tile, point_cell, point_count, conv_weight, conv_bias):
    devices = lax.axis_size("gx") * lax.axis_size("gy")
    channels = point_feats.shape[1]
    sent = pack(point_feats, point_tile, point_cell, point_count, devices)
    got = lax.all_to_all(sent, ("gx", "gy"), split_axis=0, concat_axis=0, tiled=True)
    bev_map = add_up(got).reshape(ROWS_DEV, COLS_DEV, channels)
    padded = with_halo(bev_map, (("gx", 0), ("gy", 1)), 1)
    total = lax.conv_general_dilated(
        padded[None],
        conv_weight,
        (1, 1),
        "VALID",
        dimension_numbers=("NHWC", "HWIO", "NHWC"),
        preferred_element_type=jnp.float32,
    )[0]
    conv_out = jax.nn.relu(total + conv_bias).astype(jnp.bfloat16)
    return (bev_map, conv_out)


def solution(mesh):
    in_specs = (
        P(("gx", "gy"), None),
        P(("gx", "gy"), None),
        P(("gx", "gy")),
        P(("gx", "gy")),
        P(),
        P(),
    )
    out_specs = (P("gx", "gy", None), P("gx", "gy", None))
    return jax.shard_map(shards, mesh=mesh, in_specs=in_specs, out_specs=out_specs, check_vma=False)
```

```python
import jax
import jax.numpy as jnp
from jax import lax
from jax.experimental import pallas as pl
from jax.experimental.pallas import tpu as pltpu
from jax.sharding import PartitionSpec as P

COLS_DEV = 256
ROWS_DEV = 16
CELLS = ROWS_DEV * COLS_DEV
LANES = 128
CAP = 80
BLOCK = 88
SUMS = 8
DUMP = CELLS
GROUP = 16
EDGE = 16


def pack_kernel(
    count_ref, cell_ref, tile_ref, feats_ref, out_ref, rows, slots, pos_v, pos_f, pos_s, coded, sem
):
    count = count_ref[0]
    width = 2 * LANES
    chunks = tile_ref.shape[1] // width
    tiles = out_ref.shape[0]
    tile_id = lax.broadcasted_iota(jnp.int32, (tiles, width), 0)
    lane = lax.broadcasted_iota(jnp.int32, (1, width), 1)
    source = lax.broadcasted_iota(jnp.int32, (width, width + LANES), 0)
    column = lax.broadcasted_iota(jnp.int32, (width, width + LANES), 1)
    upto = jnp.where((source <= column) | (column >= width), 1.0, 0.0).astype(jnp.bfloat16)
    first = (lax.broadcasted_iota(jnp.int32, (tiles, LANES), 0) * LANES - 1).astype(jnp.float32)

    def rank(i, before):
        live = i * width + lane < count
        here = pl.ds(pl.multiple_of(i * width, width), width)
        hit = tile_id == jnp.where(live, tile_ref[:, here], -1)
        found = jnp.dot(
            jnp.where(hit, 1.0, 0.0).astype(jnp.bfloat16), upto, preferred_element_type=jnp.float32
        )
        place = found[:, :width] + jnp.concatenate([before] * (width // LANES), axis=1)
        slot = jnp.sum(jnp.where(hit, place, 0.0), axis=0, keepdims=True)
        pos_v[pl.ds(i, 1), :] = jnp.where(live, slot.astype(jnp.int32), tiles * LANES - 1)
        at = pl.ds(pl.multiple_of(i * width, width), width)
        rows[at, :] = feats_ref[at, :].astype(jnp.float32)
        return before + found[:, width:]

    total = lax.fori_loop(0, chunks, rank, first, unroll=4) - first
    for i in range(chunks):
        pos_f[pl.ds(i * width, width)] = pos_v[i, :]
    to_smem = pltpu.make_async_copy(pos_f, pos_s, sem)
    to_smem.start()
    coded[...] = jnp.zeros_like(coded)
    to_smem.wait()

    def move(i, carry):
        start = i * width
        for k in range(width):
            slots[pl.ds(pos_s[start + k], 1), :] = rows[pl.ds(start + k, 1), :]
        live = start + lane < count
        here = pl.ds(pl.multiple_of(start, width), width)
        hit = tile_id == jnp.where(live, tile_ref[:, here], -1)
        level = pos_v[pl.ds(i, 1), :] & (LANES - 1)
        at_level = lax.broadcasted_iota(jnp.int32, (LANES, width), 0) == level
        cell = cell_ref[:, here]
        high = lax.shift_right_logical(cell, 6).astype(jnp.float32)
        low = (cell & 63).astype(jnp.float32)
        values = jnp.concatenate([jnp.where(hit, high, 0.0), jnp.where(hit, low, 0.0)], axis=0)
        coded[...] += lax.dot_general(
            values.astype(jnp.bfloat16),
            jnp.where(at_level, 1.0, 0.0).astype(jnp.bfloat16),
            (((1,), (1,)), ((), ())),
            preferred_element_type=jnp.float32,
        )
        return carry

    lax.fori_loop(0, (count + width - 1) // width, move, 0)
    spot = lax.broadcasted_iota(jnp.int32, (tiles, LANES), 1).astype(jnp.float32)
    high = jnp.where(spot < total, coded[:tiles, :], float(DUMP // 64))
    low = jnp.where(spot < total, coded[tiles:, :], 0.0)
    slots[pl.ds(CAP, tiles, LANES), :] = jnp.where(spot == LANES - 1, 0.0, high)
    slots[pl.ds(CAP + 1, tiles, LANES), :] = jnp.where(spot == LANES - 1, total, low)

    def narrow(t, carry):
        out_ref[t] = slots[pl.ds(pl.multiple_of(t * LANES, LANES), BLOCK), :].astype(jnp.bfloat16)
        return carry

    lax.fori_loop(0, tiles, narrow, 0, unroll=4)


def add_kernel(got_ref, out_ref, top_ref, bottom_ref, left_ref, right_ref, rows, cells_f, cells_s, sem, *sums):
    sources = got_ref.shape[0]

    def widen(s, carry):
        rows[pl.ds(pl.multiple_of(s * BLOCK, 8), BLOCK), :] = got_ref[s].astype(jnp.float32)
        return carry

    lax.fori_loop(0, sources, widen, 0, unroll=4)
    high = rows[pl.ds(CAP, sources, BLOCK), :].astype(jnp.int32)
    low = rows[pl.ds(CAP + 1, sources, BLOCK), :].astype(jnp.int32)
    cells_f[...] = (high * 64 + low).reshape(sources * LANES)
    to_smem = pltpu.make_async_copy(cells_f, cells_s, sem)
    to_smem.start()

    def clear(i, carry):
        for part in sums:
            part[pl.ds(pl.multiple_of(i * 256, 256), 256), :] = jnp.zeros((256, LANES), jnp.float32)
        return carry

    lax.fori_loop(0, CELLS // 256, clear, 0)
    for part in sums:
        part[pl.ds(CELLS, 8), :] = jnp.zeros((8, LANES), jnp.float32)
    to_smem.wait()

    def one(s, carry):
        number = cells_s[s * LANES + LANES - 1]

        def few(g, inner):
            at = s * LANES + g * GROUP
            base = s * BLOCK + g * GROUP
            for j in range(GROUP):
                cell = pl.ds(cells_s[at + j], 1)
                part = sums[j % SUMS]
                part[cell, :] = part[cell, :] + rows[pl.ds(base + j, 1), :]
            return inner

        return lax.fori_loop(0, lax.shift_right_logical(number + (GROUP - 1), 4), few, carry)

    lax.fori_loop(0, sources, one, 0)
    step = 256

    def close(i, carry):
        at = pl.ds(pl.multiple_of(i * step, step), step)
        total = sums[0][at, :]
        for part in sums[1:]:
            total = total + part[at, :]
        out_ref[at, :] = total.astype(jnp.bfloat16)
        return carry

    lax.fori_loop(0, CELLS // step, close, 0)
    top_ref[...] = out_ref[:COLS_DEV, :]
    bottom_ref[...] = out_ref[CELLS - COLS_DEV :, :]
    for ref, column in ((left_ref, 0), (right_ref, COLS_DEV - 1)):
        total = sums[0][pl.ds(column, ROWS_DEV, COLS_DEV), :]
        for part in sums[1:]:
            total = total + part[pl.ds(column, ROWS_DEV, COLS_DEV), :]
        ref[...] = total.astype(jnp.bfloat16)


def conv_kernel(
    bev_ref, up_ref, down_ref, weight_ref, bias_ref,
    out_ref, left_ref, right_ref, first_ref, last_ref, wide, before, after,
):
    for i in range(4):
        for b in range(3):
            for o in range(2):
                block = (slice(i * LANES, (i + 1) * LANES), slice((2 * b + o) * LANES, (2 * b + o + 1) * LANES))
                wide[block] = weight_ref[i - o, b] if 0 <= i - o < 3 else jnp.zeros((LANES, LANES), jnp.bfloat16)
    before[:8, :] = jnp.zeros((8, 2 * LANES), jnp.float32)
    after[COLS_DEV:, :] = jnp.zeros((8, 2 * LANES), jnp.float32)
    bias = bias_ref[...]

    def row(r):
        if r < 0:
            return up_ref[...]
        if r >= ROWS_DEV:
            return down_ref[...]
        return bev_ref[r * COLS_DEV : (r + 1) * COLS_DEV, :]

    for p in range(ROWS_DEV // 2):
        four = jnp.concatenate([row(2 * p - 1 + i) for i in range(4)], axis=1)
        taps = jnp.dot(four, wide[...], preferred_element_type=jnp.float32)
        before[8:, :] = taps[:, : 2 * LANES]
        after[:COLS_DEV, :] = taps[:, 4 * LANES :]
        total = taps[:, 2 * LANES : 4 * LANES] + before[7 : 7 + COLS_DEV, :] + after[1 : 1 + COLS_DEV, :]
        for o in range(2):
            r = 2 * p + o
            part = total[:, o * LANES : (o + 1) * LANES]
            left_ref[r : r + 1, :] = part[:1, :]
            right_ref[r : r + 1, :] = part[COLS_DEV - 1 :, :]
            done = jnp.maximum(part + bias, 0.0).astype(jnp.bfloat16)
            out_ref[r * COLS_DEV : (r + 1) * COLS_DEV, :] = done
            first_ref[r] = done[:EDGE, :]
            last_ref[r] = done[COLS_DEV - EDGE :, :]


def edge_kernel(
    conv_ref, left_ref, right_ref, first_ref, last_ref, west_ref, east_ref, weight_ref, bias_ref,
    out_ref, halo, blocks, sems,
):
    bias = bias_ref[...]
    column = lax.broadcasted_iota(jnp.int32, (ROWS_DEV, EDGE, LANES), 1)
    sides = (
        (left_ref, first_ref, west_ref, 0, 0, 0),
        (right_ref, last_ref, east_ref, 2, EDGE - 1, COLS_DEV - EDGE),
    )
    copies = []
    for k, (sum_ref, block_ref, halo_ref, b, spot, start) in enumerate(sides):
        halo[: ROWS_DEV + 2, :] = halo_ref[...].astype(jnp.float32)
        total = sum_ref[...]
        for a in range(3):
            total = total + jnp.dot(
                halo[a : a + ROWS_DEV, :].astype(jnp.bfloat16),
                weight_ref[a, b],
                preferred_element_type=jnp.float32,
            )
        done = jnp.maximum(total + bias, 0.0)
        block = jnp.where(column == spot, done[:, None, :], block_ref[...].astype(jnp.float32))
        blocks[k] = block.astype(jnp.bfloat16)
        copy = pltpu.make_async_copy(blocks.at[k], out_ref.at[:, pl.ds(start, EDGE), :], sems.at[k])
        copy.start()
        copies.append(copy)
    for copy in copies:
        copy.wait()


VMEM = pl.BlockSpec(memory_space=pltpu.VMEM)
SMEM = pl.BlockSpec(memory_space=pltpu.SMEM)


def pack(point_feats, point_tile, point_cell, point_count, devices):
    points, channels = point_feats.shape
    width = 2 * LANES
    chunks = points // width
    return pl.pallas_call(
        pack_kernel,
        out_shape=jax.ShapeDtypeStruct((devices, BLOCK, channels), jnp.bfloat16),
        in_specs=[SMEM, VMEM, VMEM, VMEM],
        out_specs=VMEM,
        scratch_shapes=[
            pltpu.VMEM((points, channels), jnp.float32),
            pltpu.VMEM((devices * LANES, channels), jnp.float32),
            pltpu.VMEM((chunks, width), jnp.int32),
            pltpu.VMEM((points,), jnp.int32),
            pltpu.SMEM((points,), jnp.int32),
            pltpu.VMEM((2 * devices, LANES), jnp.float32),
            pltpu.SemaphoreType.DMA,
        ],
        name="pack",
    )(
        point_count,
        point_cell.reshape(1, points),
        point_tile.reshape(1, points),
        point_feats,
    )


def add_up(got):
    devices, block, channels = got.shape
    return pl.pallas_call(
        add_kernel,
        out_shape=[
            jax.ShapeDtypeStruct((rows, channels), jnp.bfloat16)
            for rows in (CELLS, COLS_DEV, COLS_DEV, ROWS_DEV, ROWS_DEV)
        ],
        in_specs=[VMEM],
        out_specs=[VMEM] * 5,
        scratch_shapes=[
            pltpu.VMEM((devices * block, channels), jnp.float32),
            pltpu.VMEM((devices * LANES,), jnp.int32),
            pltpu.SMEM((devices * LANES,), jnp.int32),
            pltpu.SemaphoreType.DMA,
        ]
        + [pltpu.VMEM((CELLS + 8, channels), jnp.float32)] * SUMS,
        name="add_up",
    )(got)


def shift(cells, axis, step):
    count = lax.axis_size(axis)
    pairs = [(i, i + step) for i in range(count) if 0 <= i + step < count]
    return lax.ppermute(cells, axis, pairs)


def conv(bev, up, down, weight, bias):
    cells, channels = bev.shape
    bf16, f32 = jnp.bfloat16, jnp.float32
    edge = (ROWS_DEV, EDGE, channels)
    return pl.pallas_call(
        conv_kernel,
        out_shape=[
            jax.ShapeDtypeStruct((cells, channels), bf16),
            jax.ShapeDtypeStruct((ROWS_DEV, channels), f32),
            jax.ShapeDtypeStruct((ROWS_DEV, channels), f32),
            jax.ShapeDtypeStruct(edge, bf16),
            jax.ShapeDtypeStruct(edge, bf16),
        ],
        in_specs=[VMEM] * 5,
        out_specs=[VMEM] * 5,
        scratch_shapes=[
            pltpu.VMEM((4 * channels, 6 * channels), bf16),
            pltpu.VMEM((COLS_DEV + 8, 2 * channels), f32),
            pltpu.VMEM((COLS_DEV + 8, 2 * channels), f32),
        ],
        cost_estimate=pl.CostEstimate(
            flops=2 * cells * 9 * channels * channels, bytes_accessed=4 * cells * channels, transcendentals=0
        ),
        name="conv",
    )(bev, up, down, weight, bias)


def close_edges(inner, sums_left, sums_right, first, last, west, east, weight, bias):
    channels = weight.shape[-1]
    whole = (ROWS_DEV, COLS_DEV, channels)
    anywhere = pl.BlockSpec(memory_space=pl.ANY)
    return pl.pallas_call(
        edge_kernel,
        out_shape=jax.ShapeDtypeStruct(whole, jnp.bfloat16),
        in_specs=[anywhere] + [VMEM] * 8,
        out_specs=anywhere,
        input_output_aliases={0: 0},
        scratch_shapes=[
            pltpu.VMEM((ROWS_DEV + 8, channels), jnp.float32),
            pltpu.VMEM((2, ROWS_DEV, EDGE, channels), jnp.bfloat16),
            pltpu.SemaphoreType.DMA((2,)),
        ],
        name="edges",
    )(inner.reshape(whole), sums_left, sums_right, first, last, west, east, weight, bias)


def shards(point_feats, point_tile, point_cell, point_count, conv_weight, conv_bias):
    devices = lax.axis_size("gx") * lax.axis_size("gy")
    channels = point_feats.shape[1]
    sent = pack(point_feats, point_tile, point_cell, point_count, devices)
    got = lax.all_to_all(sent, ("gx", "gy"), split_axis=0, concat_axis=0, tiled=True)
    bev, top, bottom, left, right = add_up(got)
    up = shift(bottom, "gx", 1)
    down = shift(top, "gx", -1)
    bias = conv_bias.reshape(1, channels)
    last = COLS_DEV - 1
    west = shift(jnp.concatenate([up[last:], right, down[last:]], axis=0), "gy", 1)
    east = shift(jnp.concatenate([up[:1], left, down[:1]], axis=0), "gy", -1)
    inner, *edges = conv(bev, up, down, conv_weight, bias)
    conv_out = close_edges(inner, *edges, west, east, conv_weight, bias)
    return (bev.reshape(ROWS_DEV, COLS_DEV, channels), conv_out)


def solution(mesh):
    in_specs = (
        P(("gx", "gy"), None),
        P(("gx", "gy"), None),
        P(("gx", "gy")),
        P(("gx", "gy")),
        P(),
        P(),
    )
    out_specs = (P("gx", "gy", None), P("gx", "gy", None))
    return jax.shard_map(shards, mesh=mesh, in_specs=in_specs, out_specs=out_specs, check_vma=False)
```

```python
import jax
import jax.numpy as jnp
from jax import lax
from jax.experimental import pallas as pl
from jax.experimental.pallas import tpu as pltpu
from jax.sharding import PartitionSpec as P

COLS_DEV = 256
ROWS_DEV = 16
CELLS = ROWS_DEV * COLS_DEV
LANES = 128
CAP = 80
BLOCK = 88
SUMS = 8
DUMP = CELLS
EDGE = 16
TOGETHER = 4


def pack_kernel(
    count_ref, cell_ref, tile_ref, feats_hbm, out_hbm,
    feats, even, odd, slots, pos_f, pos_s, hits, coded, sent, sem, in_sem, out_sems,
):
    count = count_ref[0]
    width = 2 * LANES
    points = tile_ref.shape[1]
    chunks = points // width
    tiles = out_hbm.shape[0]
    load = pltpu.make_async_copy(feats_hbm, feats, in_sem)
    load.start()
    tile_id = lax.broadcasted_iota(jnp.int32, (tiles, width), 0)
    lane = lax.broadcasted_iota(jnp.int32, (1, width), 1)
    source = lax.broadcasted_iota(jnp.int32, (width, width + LANES), 0)
    column = lax.broadcasted_iota(jnp.int32, (width, width + LANES), 1)
    upto = jnp.where((source <= column) | (column >= width), 1.0, 0.0).astype(jnp.bfloat16)
    first = (lax.broadcasted_iota(jnp.int32, (tiles, LANES), 0) * LANES - 1).astype(jnp.float32)

    tile_mark = tile_id.astype(jnp.float32).astype(jnp.bfloat16)
    one, zero = jnp.ones((), jnp.bfloat16), jnp.zeros((), jnp.bfloat16)

    def rank(g, before):
        marks, hit = [], []
        for c in range(TOGETHER):
            i = g * TOGETHER + c
            here = pl.ds(pl.multiple_of(i * width, width), width)
            live = i * width + lane < count
            tile = jnp.where(live, tile_ref[:, here], tiles)
            mark = jnp.where(tile_mark == tile.astype(jnp.float32).astype(jnp.bfloat16), one, zero)
            hits[:, here] = mark
            marks.append(mark)
            hit.append((tile_id == tile, live, here, i))
        found = jnp.dot(jnp.concatenate(marks, axis=0), upto, preferred_element_type=jnp.float32)
        for c in range(TOGETHER):
            match, live, here, i = hit[c]
            mine = found[c * tiles : (c + 1) * tiles, :]
            place = mine[:, :width] + jnp.concatenate([before] * (width // LANES), axis=1)
            slot = jnp.sum(jnp.where(match, place, 0.0), axis=0, keepdims=True).astype(jnp.int32)
            pos_f[pl.ds(pl.multiple_of(i * width, width), width)] = jnp.where(live, slot, tiles * LANES - 1).reshape(width)
            level = (slot & (LANES - 1)).astype(jnp.float32).astype(jnp.bfloat16)
            at_level = tile_mark == level
            cell = cell_ref[:, here]
            high = lax.shift_right_logical(cell, 6).astype(jnp.float32).astype(jnp.bfloat16)
            low = (cell & 63).astype(jnp.float32).astype(jnp.bfloat16)
            coded[:LANES, here] = jnp.where(at_level, high, zero)
            coded[LANES:, here] = jnp.where(at_level, low, zero)
            before = before + mine[:, width:]
        return before

    total = lax.fori_loop(0, chunks // TOGETHER, rank, first) - first
    to_smem = pltpu.make_async_copy(pos_f, pos_s, sem)
    to_smem.start()
    cells = lax.dot_general(
        hits[...], coded[...], (((1,), (1,)), ((), ())), preferred_element_type=jnp.float32
    )
    load.wait()

    def widen(i, rows):
        at = pl.ds(pl.multiple_of(jnp.minimum(i, chunks - 1) * width, width), width)
        rows[...] = feats[at, :].astype(jnp.float32)

    def move(i, rows):
        for k in range(width):
            slot = pos_s.at[pl.ds(k, points - width + 1)][i * width]
            slots[pl.ds(slot, 1), :] = rows[k : k + 1, :]

    widen(0, even)
    to_smem.wait()

    def two(q, carry):
        widen(2 * q + 1, odd)
        move(2 * q, even)
        widen(2 * q + 2, even)
        move(2 * q + 1, odd)
        return carry

    lax.fori_loop(0, lax.shift_right_logical(count + (2 * width - 1), 9), two, 0)
    spot = lax.broadcasted_iota(jnp.int32, (tiles, LANES), 1).astype(jnp.float32)
    high = jnp.where(spot < total, cells[:, :LANES], float(DUMP // 64))
    low = jnp.where(spot < total, cells[:, LANES:], 0.0)
    slots[pl.ds(CAP, tiles, LANES), :] = high
    slots[pl.ds(CAP + 1, tiles, LANES), :] = low

    def narrow(t, carry):
        sent[t] = slots[pl.ds(pl.multiple_of(t * LANES, LANES), BLOCK), :].astype(jnp.bfloat16)
        return carry

    parts = out_sems.shape[0]
    share = tiles // parts
    stores = []
    for k in range(parts):
        lax.fori_loop(k * share, (k + 1) * share, narrow, 0, unroll=4)
        part = pl.ds(k * share, share)
        stores.append(pltpu.make_async_copy(sent.at[part], out_hbm.at[part], out_sems.at[k]))
        stores[-1].start()
    for store in stores:
        store.wait()


def add_kernel(
    got_hbm, out_ref, top_ref, bottom_ref, left_ref, right_ref,
    got, even, odd, meta, coded, cells_f, cells_s, sem, meta_sem, in_sems, *sums,
):
    sources = got_hbm.shape[0]
    codes = pltpu.make_async_copy(got_hbm.at[:, pl.ds(CAP, 8), :], meta, meta_sem)
    codes.start()
    parts = in_sems.shape[0]
    share = sources // parts
    loads = []
    for k in range(parts):
        part = pl.ds(k * share, share)
        loads.append(pltpu.make_async_copy(got_hbm.at[part, pl.ds(0, CAP), :], got.at[part], in_sems.at[k]))
        loads[-1].start()
    codes.wait()
    coded[...] = meta[...].astype(jnp.float32).reshape(coded.shape)
    high = coded[pl.ds(0, sources, 8), :].astype(jnp.int32)
    low = coded[pl.ds(1, sources, 8), :].astype(jnp.int32)
    cells_f[...] = (high * 64 + low).reshape(sources * LANES)
    to_smem = pltpu.make_async_copy(cells_f, cells_s, sem)
    to_smem.start()

    def clear(i, carry):
        for part in sums:
            part[pl.ds(pl.multiple_of(i * 256, 256), 256), :] = jnp.zeros((256, LANES), jnp.float32)
        return carry

    lax.fori_loop(0, CELLS // 256, clear, 0)
    for part in sums:
        part[pl.ds(CELLS, 8), :] = jnp.zeros((8, LANES), jnp.float32)

    def widen(s, rows):
        rows[...] = got[jnp.minimum(s, sources - 1)].astype(jnp.float32)

    def add(s, rows):
        for j in range(CAP):
            cell = pl.ds(cells_s.at[pl.ds(j, (sources - 1) * LANES + 1)][s * LANES], 1)
            part = sums[j % SUMS]
            part[cell, :] = part[cell, :] + rows[j : j + 1, :]

    def two(q, carry):
        widen(2 * q + 1, odd)
        add(2 * q, even)
        widen(2 * q + 2, even)
        add(2 * q + 1, odd)
        return carry

    to_smem.wait()
    for load in loads:
        load.wait()
    widen(0, even)
    lax.fori_loop(0, sources // 2, two, 0)
    step = 256

    def close(i, carry):
        at = pl.ds(pl.multiple_of(i * step, step), step)
        total = sums[0][at, :]
        for part in sums[1:]:
            total = total + part[at, :]
        out_ref[at, :] = total.astype(jnp.bfloat16)
        return carry

    lax.fori_loop(0, CELLS // step, close, 0)
    top_ref[...] = out_ref[:COLS_DEV, :]
    bottom_ref[...] = out_ref[CELLS - COLS_DEV :, :]
    for ref, column in ((left_ref, 0), (right_ref, COLS_DEV - 1)):
        total = sums[0][pl.ds(column, ROWS_DEV, COLS_DEV), :]
        for part in sums[1:]:
            total = total + part[pl.ds(column, ROWS_DEV, COLS_DEV), :]
        ref[...] = total.astype(jnp.bfloat16)


def conv_kernel(
    bev_ref, up_ref, down_ref, weight_ref, bias_ref,
    out_ref, left_ref, right_ref, first_ref, last_ref, wide, before, after,
):
    for i in range(4):
        for b in range(3):
            for o in range(2):
                block = (slice(i * LANES, (i + 1) * LANES), slice((2 * b + o) * LANES, (2 * b + o + 1) * LANES))
                wide[block] = weight_ref[i - o, b] if 0 <= i - o < 3 else jnp.zeros((LANES, LANES), jnp.bfloat16)
    before[:8, :] = jnp.zeros((8, 2 * LANES), jnp.float32)
    after[COLS_DEV:, :] = jnp.zeros((8, 2 * LANES), jnp.float32)
    bias = bias_ref[...]

    def row(r):
        if r < 0:
            return up_ref[...]
        if r >= ROWS_DEV:
            return down_ref[...]
        return bev_ref[r * COLS_DEV : (r + 1) * COLS_DEV, :]

    for p in range(ROWS_DEV // 2):
        four = jnp.concatenate([row(2 * p - 1 + i) for i in range(4)], axis=1)
        taps = jnp.dot(four, wide[...], preferred_element_type=jnp.float32)
        before[8:, :] = taps[:, : 2 * LANES]
        after[:COLS_DEV, :] = taps[:, 4 * LANES :]
        total = taps[:, 2 * LANES : 4 * LANES] + before[7 : 7 + COLS_DEV, :] + after[1 : 1 + COLS_DEV, :]
        for o in range(2):
            r = 2 * p + o
            part = total[:, o * LANES : (o + 1) * LANES]
            left_ref[r : r + 1, :] = part[:1, :]
            right_ref[r : r + 1, :] = part[COLS_DEV - 1 :, :]
            done = jnp.maximum(part + bias, 0.0).astype(jnp.bfloat16)
            out_ref[r * COLS_DEV : (r + 1) * COLS_DEV, :] = done
            first_ref[r] = done[:EDGE, :]
            last_ref[r] = done[COLS_DEV - EDGE :, :]


def edge_kernel(
    conv_ref, left_ref, right_ref, first_ref, last_ref, west_ref, east_ref, weight_ref, bias_ref,
    out_ref, halo, blocks, sems,
):
    bias = bias_ref[...]
    column = lax.broadcasted_iota(jnp.int32, (ROWS_DEV, EDGE, LANES), 1)
    sides = (
        (left_ref, first_ref, west_ref, 0, 0, 0),
        (right_ref, last_ref, east_ref, 2, EDGE - 1, COLS_DEV - EDGE),
    )
    copies = []
    for k, (sum_ref, block_ref, halo_ref, b, spot, start) in enumerate(sides):
        halo[: ROWS_DEV + 2, :] = halo_ref[...].astype(jnp.float32)
        total = sum_ref[...]
        for a in range(3):
            total = total + jnp.dot(
                halo[a : a + ROWS_DEV, :].astype(jnp.bfloat16),
                weight_ref[a, b],
                preferred_element_type=jnp.float32,
            )
        done = jnp.maximum(total + bias, 0.0)
        block = jnp.where(column == spot, done[:, None, :], block_ref[...].astype(jnp.float32))
        blocks[k] = block.astype(jnp.bfloat16)
        copy = pltpu.make_async_copy(blocks.at[k], out_ref.at[:, pl.ds(start, EDGE), :], sems.at[k])
        copy.start()
        copies.append(copy)
    for copy in copies:
        copy.wait()


VMEM = pl.BlockSpec(memory_space=pltpu.VMEM)
SMEM = pl.BlockSpec(memory_space=pltpu.SMEM)
ANY = pl.BlockSpec(memory_space=pl.ANY)


def pack(point_feats, point_tile, point_cell, point_count, devices):
    points, channels = point_feats.shape
    width = 2 * LANES
    chunks = points // width
    bf16, f32 = jnp.bfloat16, jnp.float32
    return pl.pallas_call(
        pack_kernel,
        out_shape=jax.ShapeDtypeStruct((devices, BLOCK, channels), bf16),
        in_specs=[SMEM, VMEM, VMEM, ANY],
        out_specs=ANY,
        scratch_shapes=[
            pltpu.VMEM((points, channels), bf16),
            pltpu.VMEM((width, channels), f32),
            pltpu.VMEM((width, channels), f32),
            pltpu.VMEM((devices * LANES, channels), f32),
            pltpu.VMEM((points,), jnp.int32),
            pltpu.SMEM((points,), jnp.int32),
            pltpu.VMEM((devices, points), bf16),
            pltpu.VMEM((2 * LANES, points), bf16),
            pltpu.VMEM((devices, BLOCK, channels), bf16),
            pltpu.SemaphoreType.DMA,
            pltpu.SemaphoreType.DMA,
            pltpu.SemaphoreType.DMA((4,)),
        ],
        name="pack",
    )(
        point_count,
        point_cell.reshape(1, points),
        point_tile.reshape(1, points),
        point_feats,
    )


def add_up(got):
    devices, block, channels = got.shape
    bf16, f32 = jnp.bfloat16, jnp.float32
    return pl.pallas_call(
        add_kernel,
        out_shape=[
            jax.ShapeDtypeStruct((rows, channels), bf16)
            for rows in (CELLS, COLS_DEV, COLS_DEV, ROWS_DEV, ROWS_DEV)
        ],
        in_specs=[ANY],
        out_specs=[VMEM] * 5,
        scratch_shapes=[
            pltpu.VMEM((devices, CAP, channels), bf16),
            pltpu.VMEM((CAP, channels), f32),
            pltpu.VMEM((CAP, channels), f32),
            pltpu.VMEM((devices, 8, channels), bf16),
            pltpu.VMEM((devices * 8, channels), f32),
            pltpu.VMEM((devices * LANES,), jnp.int32),
            pltpu.SMEM((devices * LANES,), jnp.int32),
            pltpu.SemaphoreType.DMA,
            pltpu.SemaphoreType.DMA,
            pltpu.SemaphoreType.DMA((4,)),
        ]
        + [pltpu.VMEM((CELLS + 8, channels), f32)] * SUMS,
        name="add_up",
    )(got)


def shift(cells, axis, step):
    count = lax.axis_size(axis)
    pairs = [(i, i + step) for i in range(count) if 0 <= i + step < count]
    return lax.ppermute(cells, axis, pairs)


def conv(bev, up, down, weight, bias):
    cells, channels = bev.shape
    bf16, f32 = jnp.bfloat16, jnp.float32
    edge = (ROWS_DEV, EDGE, channels)
    return pl.pallas_call(
        conv_kernel,
        out_shape=[
            jax.ShapeDtypeStruct((cells, channels), bf16),
            jax.ShapeDtypeStruct((ROWS_DEV, channels), f32),
            jax.ShapeDtypeStruct((ROWS_DEV, channels), f32),
            jax.ShapeDtypeStruct(edge, bf16),
            jax.ShapeDtypeStruct(edge, bf16),
        ],
        in_specs=[VMEM] * 5,
        out_specs=[VMEM] * 5,
        scratch_shapes=[
            pltpu.VMEM((4 * channels, 6 * channels), bf16),
            pltpu.VMEM((COLS_DEV + 8, 2 * channels), f32),
            pltpu.VMEM((COLS_DEV + 8, 2 * channels), f32),
        ],
        cost_estimate=pl.CostEstimate(
            flops=2 * cells * 9 * channels * channels, bytes_accessed=4 * cells * channels, transcendentals=0
        ),
        name="conv",
    )(bev, up, down, weight, bias)


def close_edges(inner, sums_left, sums_right, first, last, west, east, weight, bias):
    channels = weight.shape[-1]
    whole = (ROWS_DEV, COLS_DEV, channels)
    return pl.pallas_call(
        edge_kernel,
        out_shape=jax.ShapeDtypeStruct(whole, jnp.bfloat16),
        in_specs=[ANY] + [VMEM] * 8,
        out_specs=ANY,
        input_output_aliases={0: 0},
        scratch_shapes=[
            pltpu.VMEM((ROWS_DEV + 8, channels), jnp.float32),
            pltpu.VMEM((2, ROWS_DEV, EDGE, channels), jnp.bfloat16),
            pltpu.SemaphoreType.DMA((2,)),
        ],
        name="edges",
    )(inner.reshape(whole), sums_left, sums_right, first, last, west, east, weight, bias)


def shards(point_feats, point_tile, point_cell, point_count, conv_weight, conv_bias):
    devices = lax.axis_size("gx") * lax.axis_size("gy")
    channels = point_feats.shape[1]
    sent = pack(point_feats, point_tile, point_cell, point_count, devices)
    got = lax.all_to_all(sent, ("gx", "gy"), split_axis=0, concat_axis=0, tiled=True)
    bev, top, bottom, left, right = add_up(got)
    up = shift(bottom, "gx", 1)
    down = shift(top, "gx", -1)
    bias = conv_bias.reshape(1, channels)
    last = COLS_DEV - 1
    west = shift(jnp.concatenate([up[last:], right, down[last:]], axis=0), "gy", 1)
    east = shift(jnp.concatenate([up[:1], left, down[:1]], axis=0), "gy", -1)
    inner, *edges = conv(bev, up, down, conv_weight, bias)
    conv_out = close_edges(inner, *edges, west, east, conv_weight, bias)
    return (bev.reshape(ROWS_DEV, COLS_DEV, channels), conv_out)


def solution(mesh):
    in_specs = (
        P(("gx", "gy"), None),
        P(("gx", "gy"), None),
        P(("gx", "gy")),
        P(("gx", "gy")),
        P(),
        P(),
    )
    out_specs = (P("gx", "gy", None), P("gx", "gy", None))
    return jax.shard_map(shards, mesh=mesh, in_specs=in_specs, out_specs=out_specs, check_vma=False)
```

```python
import functools

import jax
import jax.numpy as jnp
from jax import lax
from jax.experimental import pallas as pl
from jax.experimental.pallas import tpu as pltpu
from jax.sharding import PartitionSpec as P

COLS_DEV = 256
ROWS_DEV = 16
CELLS = ROWS_DEV * COLS_DEV
LANES = 128
CAP = 80
BLOCK = 88
SUMS = 8
SPARE = 6
HALO = 2 * ROWS_DEV
DUMP = CELLS + HALO
EDGE = 16
MOVES = 512
TOGETHER = 4


def pack_kernel(
    across, count_ref, cell_ref, tile_ref, feats_hbm, out_hbm,
    feats, rows, slots, pos_f, pos_s, hits, coded, twins, twin_code, twin_f, twin_s, sent,
    sem, twin_sem, in_sem, out_sems,
):
    count = count_ref[0]
    width = 2 * LANES
    points = tile_ref.shape[1]
    chunks = points // width
    tiles = out_hbm.shape[0]
    load = pltpu.make_async_copy(feats_hbm, feats, in_sem)
    load.start()
    tile_id = lax.broadcasted_iota(jnp.int32, (tiles, width), 0)
    lane = lax.broadcasted_iota(jnp.int32, (1, width), 1)
    source = lax.broadcasted_iota(jnp.int32, (width, width + LANES), 0)
    column = lax.broadcasted_iota(jnp.int32, (width, width + LANES), 1)
    one, zero = jnp.ones((), jnp.bfloat16), jnp.zeros((), jnp.bfloat16)
    upto = jnp.where((source <= column) | (column >= width), 1.0, 0.0).astype(jnp.bfloat16)
    first = (lax.broadcasted_iota(jnp.int32, (tiles, LANES), 0) * LANES - 1).astype(jnp.float32)
    tile_mark = tile_id.astype(jnp.float32).astype(jnp.bfloat16)
    spare_id = lax.broadcasted_iota(jnp.int32, (8, width), 0)
    nothing = jnp.zeros((8, width), jnp.float32)
    twin_code[16:80, :] = jnp.zeros((64, points), jnp.bfloat16)
    twin_code[96:, :] = jnp.zeros((32, points), jnp.bfloat16)

    def as_bf16(x):
        return x.astype(jnp.float32).astype(jnp.bfloat16)

    def rank(g, befores):
        before, twin_before = befores
        marks, twin_marks, info = [], [], []
        for c in range(TOGETHER):
            i = g * TOGETHER + c
            here = pl.ds(pl.multiple_of(i * width, width), width)
            live = i * width + lane < count
            tile = jnp.where(live, tile_ref[:, here], tiles)
            mark = jnp.where(tile_mark == as_bf16(tile), one, zero)
            hits[:, here] = mark
            marks.append(mark)
            cell = cell_ref[:, here]
            along = cell & (COLS_DEV - 1)
            place = tile & (across - 1)
            west = live & (along == 0) & (place > 0)
            east = live & (along == COLS_DEV - 1) & (place < across - 1)
            twin = jnp.where(west, tile - 1, jnp.where(east, tile + 1, tiles))
            twin_mark = jnp.where(tile_mark == as_bf16(twin), one, zero)
            twins[:, here] = twin_mark
            twin_marks.append(twin_mark)
            code = jnp.where(west, ROWS_DEV, 0) + lax.shift_right_logical(cell, 8)
            info.append((tile, live, here, i, cell, twin, code))
        found = jnp.dot(jnp.concatenate(marks, axis=0), upto, preferred_element_type=jnp.float32)
        twin_found = jnp.dot(jnp.concatenate(twin_marks, axis=0), upto, preferred_element_type=jnp.float32)
        for c in range(TOGETHER):
            tile, live, here, i, cell, twin, code = info[c]
            mine = found[c * tiles : (c + 1) * tiles, :]
            place = mine[:, :width] + jnp.concatenate([before] * (width // LANES), axis=1)
            slot = jnp.sum(jnp.where(tile_id == tile, place, 0.0), axis=0, keepdims=True).astype(jnp.int32)
            pos_f[pl.ds(pl.multiple_of(i * width, width), width)] = jnp.where(live, slot, tiles * LANES - 1).reshape(width)
            at_level = tile_mark == as_bf16(slot & (LANES - 1))
            coded[:LANES, here] = jnp.where(at_level, as_bf16(lax.shift_right_logical(cell, 6)), zero)
            coded[LANES:, here] = jnp.where(at_level, as_bf16(cell & 63), zero)
            before = before + mine[:, width:]
            theirs = twin_found[c * tiles : (c + 1) * tiles, :]
            place = theirs[:, :width] + jnp.concatenate([twin_before] * (width // LANES), axis=1)
            order = jnp.sum(jnp.where(tile_id == twin, place, 0.0), axis=0, keepdims=True).astype(jnp.int32) - 1
            at_order = spare_id == order
            point = i * width + lane
            high = jnp.where(at_order, (point & -LANES).astype(jnp.float32), nothing)
            low = jnp.where(at_order, (point & (LANES - 1)).astype(jnp.float32), nothing)
            value = jnp.where(at_order, code.astype(jnp.float32), nothing)
            twin_code[:16, here] = jnp.concatenate([high, low], axis=0).astype(jnp.bfloat16)
            twin_code[80:96, here] = jnp.concatenate([value, nothing], axis=0).astype(jnp.bfloat16)
            twin_before = twin_before + theirs[:, width:]
        return before, twin_before

    before, twin_total = lax.fori_loop(
        0, chunks // TOGETHER, rank, (first, jnp.zeros((tiles, LANES), jnp.float32))
    )
    total = before - first
    to_smem = pltpu.make_async_copy(pos_f, pos_s, sem)
    to_smem.start()
    across_lanes = (((1,), (1,)), ((), ()))
    extra = lax.dot_general(twins[...], twin_code[...], across_lanes, preferred_element_type=jnp.float32)
    origin = (extra + pltpu.roll(extra, LANES - 8, 1)).astype(jnp.int32)
    spot = lax.broadcasted_iota(jnp.int32, (tiles, LANES), 1).astype(jnp.float32)
    known = spot < jnp.minimum(twin_total, float(SPARE))
    twin_f[...] = jnp.where(known, origin, 0).reshape(tiles * LANES)
    twins_to_smem = pltpu.make_async_copy(twin_f, twin_s, twin_sem)
    twins_to_smem.start()
    load.wait()
    rows[...] = feats[...].astype(jnp.float32)
    cells = lax.dot_general(hits[...], coded[...], across_lanes, preferred_element_type=jnp.float32)
    to_smem.wait()

    def move(i, carry):
        for k in range(MOVES):
            slot = pos_s.at[pl.ds(k, points - MOVES + 1)][i * MOVES]
            slots[pl.ds(slot, 1), :] = rows[pl.ds(i * MOVES + k, 1), :]
        return carry

    lax.fori_loop(0, (count + (MOVES - 1)) // MOVES, move, 0)
    twins_to_smem.wait()

    def move_twins(t, carry):
        for u in range(8):
            for j in range(SPARE):
                point = twin_s.at[pl.ds(u * LANES + j, (tiles - 8) * LANES + 1)][t * (8 * LANES)]
                slots[pl.ds(t * (8 * LANES) + u * LANES + CAP + 2 + j, 1), :] = rows[pl.ds(point, 1), :]
        return carry

    lax.fori_loop(0, tiles // 8, move_twins, 0)
    high = jnp.where(spot < total, cells[:, :LANES], float(DUMP // 64))
    low = jnp.where(spot < total, cells[:, LANES:], float(DUMP % 64))
    low = jnp.where((spot >= CAP) & (spot - CAP < jnp.minimum(twin_total, float(SPARE))), extra, low)
    full = jnp.max(twin_total, axis=0, keepdims=True) > SPARE
    high = jnp.where(spot == LANES - 1, 0.0, high)
    low = jnp.where(spot == LANES - 1, jnp.where(full, 1.0, 0.0), low)
    slots[pl.ds(CAP, tiles, LANES), :] = high
    slots[pl.ds(CAP + 1, tiles, LANES), :] = low

    def narrow(t, carry):
        sent[t] = slots[pl.ds(pl.multiple_of(t * LANES, LANES), BLOCK), :].astype(jnp.bfloat16)
        return carry

    parts = out_sems.shape[0]
    share = tiles // parts
    stores = []
    for k in range(parts):
        lax.fori_loop(k * share, (k + 1) * share, narrow, 0, unroll=4)
        part = pl.ds(k * share, share)
        stores.append(pltpu.make_async_copy(sent.at[part], out_hbm.at[part], out_sems.at[k]))
        stores[-1].start()
    for store in stores:
        store.wait()


def add_kernel(
    got_hbm, out_ref, top_ref, bottom_ref, left_ref, right_ref, west_ref, east_ref, full_ref,
    got, even, odd, meta, coded, cells_f, cells_s, sem, meta_sem, in_sems, *sums,
):
    sources = got_hbm.shape[0]
    codes = pltpu.make_async_copy(got_hbm.at[:, pl.ds(CAP, 8), :], meta, meta_sem)
    codes.start()
    parts = in_sems.shape[0]
    share = sources // parts
    loads = []
    for k in range(parts):
        part = pl.ds(k * share, share)
        loads.append(pltpu.make_async_copy(got_hbm.at[part], got.at[part], in_sems.at[k]))
        loads[-1].start()
    codes.wait()
    coded[...] = meta[...].astype(jnp.float32).reshape(coded.shape)
    high = coded[pl.ds(0, sources, 8), :].astype(jnp.int32)
    low = coded[pl.ds(1, sources, 8), :].astype(jnp.int32)
    cells = high * 64 + low
    full_ref[...] = jnp.broadcast_to(jnp.max(cells[:, LANES - 1 :], axis=0, keepdims=True), full_ref.shape)
    cells_f[...] = cells.reshape(sources * LANES)
    to_smem = pltpu.make_async_copy(cells_f, cells_s, sem)
    to_smem.start()

    def clear(i, carry):
        for part in sums:
            part[pl.ds(pl.multiple_of(i * 256, 256), 256), :] = jnp.zeros((256, LANES), jnp.float32)
        return carry

    lax.fori_loop(0, CELLS // 256, clear, 0)
    for part in sums:
        part[pl.ds(CELLS, HALO + 8), :] = jnp.zeros((HALO + 8, LANES), jnp.float32)

    def widen(s, rows):
        rows[...] = got[jnp.minimum(s, sources - 1)].astype(jnp.float32)

    def add(s, rows):
        for j in range(CAP + SPARE):
            cell = pl.ds(cells_s.at[pl.ds(j, (sources - 1) * LANES + 1)][s * LANES], 1)
            part = sums[j % SUMS]
            k = j if j < CAP else j + 2
            part[cell, :] = part[cell, :] + rows[k : k + 1, :]

    def two(q, carry):
        widen(2 * q + 1, odd)
        add(2 * q, even)
        widen(2 * q + 2, even)
        add(2 * q + 1, odd)
        return carry

    to_smem.wait()
    for load in loads:
        load.wait()
    widen(0, even)
    lax.fori_loop(0, sources // 2, two, 0)
    step = 256

    def close(i, carry):
        at = pl.ds(pl.multiple_of(i * step, step), step)
        total = sums[0][at, :]
        for part in sums[1:]:
            total = total + part[at, :]
        out_ref[at, :] = total.astype(jnp.bfloat16)
        return carry

    lax.fori_loop(0, CELLS // step, close, 0)

    def column(start, stride):
        at = pl.ds(start, ROWS_DEV, stride)
        total = sums[0][at, :]
        for part in sums[1:]:
            total = total + part[at, :]
        return total

    left_ref[...] = column(0, COLS_DEV).astype(jnp.bfloat16)
    right_ref[...] = column(COLS_DEV - 1, COLS_DEV).astype(jnp.bfloat16)
    west, east = column(CELLS, 1), column(CELLS + ROWS_DEV, 1)
    west_ref[...] = west.astype(jnp.bfloat16)
    east_ref[...] = east.astype(jnp.bfloat16)
    spot = lax.broadcasted_iota(jnp.int32, (EDGE, LANES), 0)
    for ref, r in ((top_ref, 0), (bottom_ref, ROWS_DEV - 1)):
        ref[:COLS_DEV, :] = out_ref[r * COLS_DEV : (r + 1) * COLS_DEV, :]
        corners = jnp.where(spot == 0, west[r : r + 1, :], jnp.where(spot == 1, east[r : r + 1, :], 0.0))
        ref[COLS_DEV:, :] = corners.astype(jnp.bfloat16)


def conv_kernel(
    bev_ref, up_ref, down_ref, west_ref, east_ref, weight_ref, bias_ref,
    out_ref, wide, before, after, side,
):
    for i in range(4):
        for b in range(3):
            for o in range(2):
                block = (slice(i * LANES, (i + 1) * LANES), slice((2 * b + o) * LANES, (2 * b + o + 1) * LANES))
                wide[block] = weight_ref[i - o, b] if 0 <= i - o < 3 else jnp.zeros((LANES, LANES), jnp.bfloat16)
    bias = bias_ref[...]
    pairs = ROWS_DEV // 2
    above = up_ref[COLS_DEV:, :].astype(jnp.float32)
    below = down_ref[COLS_DEV:, :].astype(jnp.float32)

    def beside(ref, corner, start):
        side[:1, :] = above[corner : corner + 1, :]
        side[1 : ROWS_DEV + 1, :] = ref[...].astype(jnp.float32)
        side[ROWS_DEV + 1 : ROWS_DEV + 2, :] = below[corner : corner + 1, :]
        four = jnp.concatenate([side[pl.ds(i, pairs, 2), :] for i in range(4)], axis=1)
        return jnp.dot(
            four.astype(jnp.bfloat16), wide[:, start : start + 2 * LANES], preferred_element_type=jnp.float32
        )

    west = beside(west_ref, 0, 0)
    east = beside(east_ref, 1, 4 * LANES)

    def row(r):
        if r < 0:
            return up_ref[:COLS_DEV, :]
        if r >= ROWS_DEV:
            return down_ref[:COLS_DEV, :]
        return bev_ref[r * COLS_DEV : (r + 1) * COLS_DEV, :]

    for p in range(pairs):
        four = jnp.concatenate([row(2 * p - 1 + i) for i in range(4)], axis=1)
        taps = jnp.dot(four, wide[...], preferred_element_type=jnp.float32)
        before[7:8, :] = west[p : p + 1, :]
        before[8:, :] = taps[:, : 2 * LANES]
        after[:COLS_DEV, :] = taps[:, 4 * LANES :]
        after[COLS_DEV : COLS_DEV + 1, :] = east[p : p + 1, :]
        total = taps[:, 2 * LANES : 4 * LANES] + before[7 : 7 + COLS_DEV, :] + after[1 : 1 + COLS_DEV, :]
        for o in range(2):
            r = 2 * p + o
            part = total[:, o * LANES : (o + 1) * LANES]
            out_ref[r * COLS_DEV : (r + 1) * COLS_DEV, :] = jnp.maximum(part + bias, 0.0).astype(jnp.bfloat16)


VMEM = pl.BlockSpec(memory_space=pltpu.VMEM)
SMEM = pl.BlockSpec(memory_space=pltpu.SMEM)
ANY = pl.BlockSpec(memory_space=pl.ANY)


def pack(point_feats, point_tile, point_cell, point_count, devices, across=8):
    points, channels = point_feats.shape
    if across & (across - 1):
        raise ValueError("across")
    bf16, f32, i32 = jnp.bfloat16, jnp.float32, jnp.int32
    return pl.pallas_call(
        functools.partial(pack_kernel, across),
        out_shape=jax.ShapeDtypeStruct((devices, BLOCK, channels), bf16),
        in_specs=[SMEM, VMEM, VMEM, ANY],
        out_specs=ANY,
        scratch_shapes=[
            pltpu.VMEM((points, channels), bf16),
            pltpu.VMEM((points, channels), f32),
            pltpu.VMEM((devices * LANES, channels), f32),
            pltpu.VMEM((points,), i32),
            pltpu.SMEM((points,), i32),
            pltpu.VMEM((devices, points), bf16),
            pltpu.VMEM((2 * LANES, points), bf16),
            pltpu.VMEM((devices, points), bf16),
            pltpu.VMEM((LANES, points), bf16),
            pltpu.VMEM((devices * LANES,), i32),
            pltpu.SMEM((devices * LANES,), i32),
            pltpu.VMEM((devices, BLOCK, channels), bf16),
            pltpu.SemaphoreType.DMA,
            pltpu.SemaphoreType.DMA,
            pltpu.SemaphoreType.DMA,
            pltpu.SemaphoreType.DMA((4,)),
        ],
        name="pack",
    )(
        point_count,
        point_cell.reshape(1, points),
        point_tile.reshape(1, points),
        point_feats,
    )


def add_up(got):
    devices, block, channels = got.shape
    bf16, f32, i32 = jnp.bfloat16, jnp.float32, jnp.int32
    heights = (CELLS, COLS_DEV + EDGE, COLS_DEV + EDGE) + (ROWS_DEV,) * 4
    return pl.pallas_call(
        add_kernel,
        out_shape=[jax.ShapeDtypeStruct((height, channels), bf16) for height in heights]
        + [jax.ShapeDtypeStruct((8, LANES), i32)],
        in_specs=[ANY],
        out_specs=[VMEM] * 8,
        scratch_shapes=[
            pltpu.VMEM((devices, block, channels), bf16),
            pltpu.VMEM((block, channels), f32),
            pltpu.VMEM((block, channels), f32),
            pltpu.VMEM((devices, 8, channels), bf16),
            pltpu.VMEM((devices * 8, channels), f32),
            pltpu.VMEM((devices * LANES,), i32),
            pltpu.SMEM((devices * LANES,), i32),
            pltpu.SemaphoreType.DMA,
            pltpu.SemaphoreType.DMA,
            pltpu.SemaphoreType.DMA((4,)),
        ]
        + [pltpu.VMEM((CELLS + HALO + 8, channels), f32)] * SUMS,
        name="add_up",
    )(got)


def shift(cells, axis, step):
    count = lax.axis_size(axis)
    pairs = [(i, i + step) for i in range(count) if 0 <= i + step < count]
    return lax.ppermute(cells, axis, pairs)


def conv(bev, up, down, west, east, weight, bias):
    cells, channels = bev.shape
    bf16, f32 = jnp.bfloat16, jnp.float32
    return pl.pallas_call(
        conv_kernel,
        out_shape=jax.ShapeDtypeStruct((cells, channels), bf16),
        in_specs=[VMEM] * 7,
        out_specs=VMEM,
        scratch_shapes=[
            pltpu.VMEM((4 * channels, 6 * channels), bf16),
            pltpu.VMEM((COLS_DEV + 8, 2 * channels), f32),
            pltpu.VMEM((COLS_DEV + 8, 2 * channels), f32),
            pltpu.VMEM((ROWS_DEV + 8, channels), f32),
        ],
        name="conv",
    )(bev, up, down, west, east, weight, bias)


def exchange_columns(top, bottom, left, right, west, east):
    west, east = shift(right, "gy", 1), shift(left, "gy", -1)
    rest = jnp.zeros((EDGE - 2, west.shape[1]), west.dtype)
    top = jnp.concatenate([top[:COLS_DEV], west[:1], east[:1], rest], axis=0)
    bottom = jnp.concatenate([bottom[:COLS_DEV], west[ROWS_DEV - 1 :], east[ROWS_DEV - 1 :], rest], axis=0)
    return top, bottom, west, east


def keep_columns(top, bottom, left, right, west, east):
    return top, bottom, west, east


def shards(point_feats, point_tile, point_cell, point_count, conv_weight, conv_bias):
    across = lax.axis_size("gy")
    devices = lax.axis_size("gx") * across
    channels = point_feats.shape[1]
    sent = pack(point_feats, point_tile, point_cell, point_count, devices, across)
    got = lax.all_to_all(sent, ("gx", "gy"), split_axis=0, concat_axis=0, tiled=True)
    bev, top, bottom, left, right, west, east, full = add_up(got)
    top, bottom, west, east = lax.cond(
        full[0, 0] > 0, exchange_columns, keep_columns, top, bottom, left, right, west, east
    )
    up = shift(bottom, "gx", 1)
    down = shift(top, "gx", -1)
    conv_out = conv(bev, up, down, west, east, conv_weight, conv_bias.reshape(1, channels))
    whole = (ROWS_DEV, COLS_DEV, channels)
    return (bev.reshape(whole), conv_out.reshape(whole))


def solution(mesh):
    in_specs = (
        P(("gx", "gy"), None),
        P(("gx", "gy"), None),
        P(("gx", "gy")),
        P(("gx", "gy")),
        P(),
        P(),
    )
    out_specs = (P("gx", "gy", None), P("gx", "gy", None))
    return jax.shard_map(shards, mesh=mesh, in_specs=in_specs, out_specs=out_specs, check_vma=False)
```

```python
import functools

import jax
import jax.numpy as jnp
from jax import lax
from jax.experimental import pallas as pl
from jax.experimental.pallas import tpu as pltpu
from jax.sharding import PartitionSpec as P

COLS_DEV = 256
ROWS_DEV = 16
CELLS = ROWS_DEV * COLS_DEV
LANES = 128
CAP = 80
BLOCK = 88
SUMS = 8
SPARE = 6
HALO = 2 * ROWS_DEV
DUMP = CELLS + HALO
EDGE = 16
MOVES = 512
TOGETHER = 8


def pack_kernel(
    across, count_ref, cell_ref, tile_ref, feats_hbm, out_hbm,
    feats, rows, slots, pos_f, pos_s, hits, coded, twins, twin_code, twin_f, twin_s, sent,
    sem, twin_sem, in_sem, out_sems,
):
    count = count_ref[0]
    width = 2 * LANES
    points = tile_ref.shape[1]
    chunks = points // width
    tiles = out_hbm.shape[0]
    load = pltpu.make_async_copy(feats_hbm, feats, in_sem)
    load.start()
    tile_id = lax.broadcasted_iota(jnp.int32, (tiles, width), 0)
    lane = lax.broadcasted_iota(jnp.int32, (1, width), 1)
    source = lax.broadcasted_iota(jnp.int32, (width, width + LANES), 0)
    column = lax.broadcasted_iota(jnp.int32, (width, width + LANES), 1)
    one, zero = jnp.ones((), jnp.bfloat16), jnp.zeros((), jnp.bfloat16)
    upto = jnp.where((source <= column) | (column >= width), 1.0, 0.0).astype(jnp.bfloat16)
    tile_mark = tile_id.astype(jnp.float32).astype(jnp.bfloat16)
    spare_id = lax.broadcasted_iota(jnp.int32, (8, width), 0)
    nothing = jnp.zeros((8, width), jnp.float32)

    def as_bf16(x):
        return x.astype(jnp.float32).astype(jnp.bfloat16)

    def pick(mark, found, before):
        place = found[:, :width].astype(jnp.bfloat16) + jnp.concatenate([before] * (width // LANES), axis=1)
        place = jnp.where(mark, place, zero)
        while place.shape[0] > 16:
            half = place.shape[0] // 2
            place = place[:half, :] + place[half:, :]
        order = jnp.sum(place.astype(jnp.float32), axis=0, keepdims=True).astype(jnp.int32) - 1
        return order, before + found[:, width:].astype(jnp.bfloat16)

    def rank(g, befores):
        before, twin_before = befores
        marks, twin_marks, info = [], [], []
        for c in range(TOGETHER):
            i = g * TOGETHER + c
            here = pl.ds(pl.multiple_of(i * width, width), width)
            live = i * width + lane < count
            tile = jnp.where(live, tile_ref[:, here], tiles)
            match = tile_mark == as_bf16(tile)
            mark = jnp.where(match, one, zero)
            hits[:, here] = mark
            marks.append(mark)
            cell = cell_ref[:, here]
            along = cell & (COLS_DEV - 1)
            place = tile & (across - 1)
            west = live & (along == 0) & (place > 0)
            east = live & (along == COLS_DEV - 1) & (place < across - 1)
            twin = jnp.where(west, tile - 1, jnp.where(east, tile + 1, tiles))
            twin_match = tile_mark == as_bf16(twin)
            twin_mark = jnp.where(twin_match, one, zero)
            twins[:, here] = twin_mark
            twin_marks.append(twin_mark)
            code = jnp.where(west, ROWS_DEV, 0) + lax.shift_right_logical(cell, 8)
            info.append((tile, live, here, i, cell, code, match, twin_match))
        found = jnp.dot(jnp.concatenate(marks, axis=0), upto, preferred_element_type=jnp.float32)
        twin_found = jnp.dot(jnp.concatenate(twin_marks, axis=0), upto, preferred_element_type=jnp.float32)
        for c in range(TOGETHER):
            tile, live, here, i, cell, code, match, twin_match = info[c]
            level, before = pick(match, found[c * tiles : (c + 1) * tiles, :], before)
            slot = jnp.where(live, tile * LANES + level, tiles * LANES - 1)
            pos_f[pl.ds(pl.multiple_of(i * width, width), width)] = slot.reshape(width)
            at_level = tile_mark == as_bf16(level)
            coded[:LANES, here] = jnp.where(at_level, as_bf16(lax.shift_right_logical(cell, 6)), zero)
            coded[LANES:, here] = jnp.where(at_level, as_bf16(cell & 63), zero)
            order, twin_before = pick(twin_match, twin_found[c * tiles : (c + 1) * tiles, :], twin_before)
            at_order = spare_id == order
            point = i * width + lane
            high = jnp.where(at_order, (point & -LANES).astype(jnp.float32), nothing)
            low = jnp.where(at_order, (point & (LANES - 1)).astype(jnp.float32), nothing)
            value = jnp.where(at_order, code.astype(jnp.float32), nothing)
            twin_code[:16, here] = jnp.concatenate([high, low], axis=0).astype(jnp.bfloat16)
            twin_code[16:, here] = jnp.concatenate([value, nothing], axis=0).astype(jnp.bfloat16)
        return before, twin_before

    start = jnp.zeros((tiles, LANES), jnp.bfloat16)
    total, twin_total = lax.fori_loop(0, chunks // TOGETHER, rank, (start, start))
    total, twin_total = total.astype(jnp.float32), twin_total.astype(jnp.float32)
    to_smem = pltpu.make_async_copy(pos_f, pos_s, sem)
    to_smem.start()
    across_lanes = (((1,), (1,)), ((), ()))
    extra = lax.dot_general(twin_code[...], twins[...], across_lanes, preferred_element_type=jnp.float32)
    twin_f[...] = (extra[:8, :] + extra[8:16, :]).astype(jnp.int32).reshape(8 * tiles)
    twins_to_smem = pltpu.make_async_copy(twin_f, twin_s, twin_sem)
    twins_to_smem.start()
    spot = lax.broadcasted_iota(jnp.int32, (tiles, LANES), 1).astype(jnp.float32)
    blank = jnp.zeros((CAP, tiles), jnp.float32)
    codes = jnp.concatenate([blank, extra[16:, :], jnp.zeros((LANES - CAP - 16, tiles), jnp.float32)], axis=0).T
    load.wait()
    rows[...] = feats[...].astype(jnp.float32)
    cells = lax.dot_general(hits[...], coded[...], across_lanes, preferred_element_type=jnp.float32)
    to_smem.wait()

    def move(i, carry):
        for k in range(MOVES):
            slot = pos_s.at[pl.ds(k, points - MOVES + 1)][i * MOVES]
            slots[pl.ds(slot, 1), :] = rows[pl.ds(i * MOVES + k, 1), :]
        return carry

    lax.fori_loop(0, (count + (MOVES - 1)) // MOVES, move, 0)
    twins_to_smem.wait()

    def move_twins(t, carry):
        for u in range(8):
            for j in range(SPARE):
                point = twin_s.at[pl.ds(j * tiles + u, tiles - 7)][t * 8]
                slots[pl.ds(t * (8 * LANES) + u * LANES + CAP + 2 + j, 1), :] = rows[pl.ds(point, 1), :]
        return carry

    lax.fori_loop(0, tiles // 8, move_twins, 0)
    high = jnp.where(spot < total, cells[:, :LANES], float(DUMP // 64))
    low = jnp.where(spot < total, cells[:, LANES:], float(DUMP % 64))
    low = jnp.where((spot >= CAP) & (spot - CAP < jnp.minimum(twin_total, float(SPARE))), codes, low)
    full = jnp.max(twin_total, axis=0, keepdims=True) > SPARE
    high = jnp.where(spot == LANES - 1, 0.0, high)
    low = jnp.where(spot == LANES - 1, jnp.where(full, 1.0, 0.0), low)
    slots[pl.ds(CAP, tiles, LANES), :] = high
    slots[pl.ds(CAP + 1, tiles, LANES), :] = low

    def narrow(t, carry):
        sent[t] = slots[pl.ds(pl.multiple_of(t * LANES, LANES), BLOCK), :].astype(jnp.bfloat16)
        return carry

    parts = out_sems.shape[0]
    share = tiles // parts
    stores = []
    for k in range(parts):
        lax.fori_loop(k * share, (k + 1) * share, narrow, 0, unroll=4)
        part = pl.ds(k * share, share)
        stores.append(pltpu.make_async_copy(sent.at[part], out_hbm.at[part], out_sems.at[k]))
        stores[-1].start()
    for store in stores:
        store.wait()


def add_kernel(
    got_hbm, out_ref, top_ref, bottom_ref, sides_ref, full_ref,
    got, even, odd, meta, coded, cells_f, cells_s, sem, meta_sem, in_sems, *sums,
):
    sources = got_hbm.shape[0]
    codes = pltpu.make_async_copy(got_hbm.at[:, pl.ds(CAP, 8), :], meta, meta_sem)
    codes.start()
    parts = in_sems.shape[0]
    share = sources // parts
    loads = []
    for k in range(parts):
        part = pl.ds(k * share, share)
        loads.append(pltpu.make_async_copy(got_hbm.at[part], got.at[part], in_sems.at[k]))
        loads[-1].start()
    codes.wait()
    coded[...] = meta[...].astype(jnp.float32).reshape(coded.shape)
    high = coded[pl.ds(0, sources, 8), :].astype(jnp.int32)
    low = coded[pl.ds(1, sources, 8), :].astype(jnp.int32)
    cells = high * 64 + low
    full_ref[0] = jnp.max(cells[:, LANES - 1 :])
    cells_f[...] = cells.reshape(sources * LANES)
    to_smem = pltpu.make_async_copy(cells_f, cells_s, sem)
    to_smem.start()

    def clear(i, carry):
        for part in sums:
            part[pl.ds(pl.multiple_of(i * 256, 256), 256), :] = jnp.zeros((256, LANES), jnp.float32)
        return carry

    lax.fori_loop(0, CELLS // 256, clear, 0)
    for part in sums:
        part[pl.ds(CELLS, HALO + 8), :] = jnp.zeros((HALO + 8, LANES), jnp.float32)

    def widen(s, rows):
        rows[...] = got[jnp.minimum(s, sources - 1)].astype(jnp.float32)

    def add(s, rows):
        for j in range(CAP + SPARE):
            cell = pl.ds(cells_s.at[pl.ds(j, (sources - 1) * LANES + 1)][s * LANES], 1)
            part = sums[j % SUMS]
            k = j if j < CAP else j + 2
            part[cell, :] = part[cell, :] + rows[k : k + 1, :]

    def two(q, carry):
        widen(2 * q + 1, odd)
        add(2 * q, even)
        widen(2 * q + 2, even)
        add(2 * q + 1, odd)
        return carry

    to_smem.wait()
    for load in loads:
        load.wait()
    widen(0, even)
    lax.fori_loop(0, sources // 2, two, 0)
    step = 256

    def close(i, carry):
        at = pl.ds(pl.multiple_of(i * step, step), step)
        total = sums[0][at, :]
        for part in sums[1:]:
            total = total + part[at, :]
        out_ref[at, :] = total.astype(jnp.bfloat16)
        return carry

    lax.fori_loop(0, CELLS // step, close, 0)

    def column(start, stride):
        at = pl.ds(start, ROWS_DEV, stride)
        total = sums[0][at, :]
        for part in sums[1:]:
            total = total + part[at, :]
        return total

    west, east = column(CELLS, 1), column(CELLS + ROWS_DEV, 1)
    sides_ref[:ROWS_DEV, :] = west.astype(jnp.bfloat16)
    sides_ref[ROWS_DEV:, :] = east.astype(jnp.bfloat16)
    spot = lax.broadcasted_iota(jnp.int32, (EDGE, LANES), 0)
    for ref, r in ((top_ref, 0), (bottom_ref, ROWS_DEV - 1)):
        ref[:COLS_DEV, :] = out_ref[r * COLS_DEV : (r + 1) * COLS_DEV, :]
        corners = jnp.where(spot == 0, west[r : r + 1, :], jnp.where(spot == 1, east[r : r + 1, :], 0.0))
        ref[COLS_DEV:, :] = corners.astype(jnp.bfloat16)


def conv_kernel(
    bev_ref, up_ref, down_ref, sides_ref, weight_ref, bias_ref,
    out_ref, wide, before, after, side,
):
    for i in range(4):
        for b in range(3):
            for o in range(2):
                block = (slice(i * LANES, (i + 1) * LANES), slice((2 * b + o) * LANES, (2 * b + o + 1) * LANES))
                wide[block] = weight_ref[i - o, b] if 0 <= i - o < 3 else jnp.zeros((LANES, LANES), jnp.bfloat16)
    bias = bias_ref[...]
    pairs = ROWS_DEV // 2
    above = up_ref[COLS_DEV:, :].astype(jnp.float32)
    below = down_ref[COLS_DEV:, :].astype(jnp.float32)

    def beside(corner, start):
        side[:1, :] = above[corner : corner + 1, :]
        side[1 : ROWS_DEV + 1, :] = sides_ref[corner * ROWS_DEV : (corner + 1) * ROWS_DEV, :].astype(jnp.float32)
        side[ROWS_DEV + 1 : ROWS_DEV + 2, :] = below[corner : corner + 1, :]
        four = jnp.concatenate([side[pl.ds(i, pairs, 2), :] for i in range(4)], axis=1)
        return jnp.dot(
            four.astype(jnp.bfloat16), wide[:, start : start + 2 * LANES], preferred_element_type=jnp.float32
        )

    west = beside(0, 0)
    east = beside(1, 4 * LANES)

    def row(r):
        if r < 0:
            return up_ref[:COLS_DEV, :]
        if r >= ROWS_DEV:
            return down_ref[:COLS_DEV, :]
        return bev_ref[r * COLS_DEV : (r + 1) * COLS_DEV, :]

    for p in range(pairs):
        four = jnp.concatenate([row(2 * p - 1 + i) for i in range(4)], axis=1)
        taps = jnp.dot(four, wide[...], preferred_element_type=jnp.float32)
        before[7:8, :] = west[p : p + 1, :]
        before[8:, :] = taps[:, : 2 * LANES]
        after[:COLS_DEV, :] = taps[:, 4 * LANES :]
        after[COLS_DEV : COLS_DEV + 1, :] = east[p : p + 1, :]
        total = taps[:, 2 * LANES : 4 * LANES] + before[7 : 7 + COLS_DEV, :] + after[1 : 1 + COLS_DEV, :]
        for o in range(2):
            r = 2 * p + o
            part = total[:, o * LANES : (o + 1) * LANES]
            out_ref[r * COLS_DEV : (r + 1) * COLS_DEV, :] = jnp.maximum(part + bias, 0.0).astype(jnp.bfloat16)


VMEM = pl.BlockSpec(memory_space=pltpu.VMEM)
SMEM = pl.BlockSpec(memory_space=pltpu.SMEM)
ANY = pl.BlockSpec(memory_space=pl.ANY)


def pack(point_feats, point_tile, point_cell, point_count, devices, across=8):
    points, channels = point_feats.shape
    if across & (across - 1):
        raise ValueError("across")
    bf16, f32, i32 = jnp.bfloat16, jnp.float32, jnp.int32
    return pl.pallas_call(
        functools.partial(pack_kernel, across),
        out_shape=jax.ShapeDtypeStruct((devices, BLOCK, channels), bf16),
        in_specs=[SMEM, VMEM, VMEM, ANY],
        out_specs=ANY,
        scratch_shapes=[
            pltpu.VMEM((points, channels), bf16),
            pltpu.VMEM((points, channels), f32),
            pltpu.VMEM((devices * LANES, channels), f32),
            pltpu.VMEM((points,), i32),
            pltpu.SMEM((points,), i32),
            pltpu.VMEM((devices, points), bf16),
            pltpu.VMEM((2 * LANES, points), bf16),
            pltpu.VMEM((devices, points), bf16),
            pltpu.VMEM((32, points), bf16),
            pltpu.VMEM((devices * 8,), i32),
            pltpu.SMEM((devices * 8,), i32),
            pltpu.VMEM((devices, BLOCK, channels), bf16),
            pltpu.SemaphoreType.DMA,
            pltpu.SemaphoreType.DMA,
            pltpu.SemaphoreType.DMA,
            pltpu.SemaphoreType.DMA((4,)),
        ],
        name="pack",
    )(
        point_count,
        point_cell.reshape(1, points),
        point_tile.reshape(1, points),
        point_feats,
    )


def add_up(got):
    devices, block, channels = got.shape
    bf16, f32, i32 = jnp.bfloat16, jnp.float32, jnp.int32
    heights = (CELLS, COLS_DEV + EDGE, COLS_DEV + EDGE, HALO)
    return pl.pallas_call(
        add_kernel,
        out_shape=[jax.ShapeDtypeStruct((height, channels), bf16) for height in heights]
        + [jax.ShapeDtypeStruct((1,), i32)],
        in_specs=[ANY],
        out_specs=[VMEM] * 4 + [SMEM],
        scratch_shapes=[
            pltpu.VMEM((devices, block, channels), bf16),
            pltpu.VMEM((block, channels), f32),
            pltpu.VMEM((block, channels), f32),
            pltpu.VMEM((devices, 8, channels), bf16),
            pltpu.VMEM((devices * 8, channels), f32),
            pltpu.VMEM((devices * LANES,), i32),
            pltpu.SMEM((devices * LANES,), i32),
            pltpu.SemaphoreType.DMA,
            pltpu.SemaphoreType.DMA,
            pltpu.SemaphoreType.DMA((4,)),
        ]
        + [pltpu.VMEM((CELLS + HALO + 8, channels), f32)] * SUMS,
        name="add_up",
    )(got)


def shift(cells, axis, step):
    count = lax.axis_size(axis)
    pairs = [(i, i + step) for i in range(count) if 0 <= i + step < count]
    return lax.ppermute(cells, axis, pairs)


def conv(bev, up, down, sides, weight, bias):
    cells, channels = bev.shape
    bf16, f32 = jnp.bfloat16, jnp.float32
    return pl.pallas_call(
        conv_kernel,
        out_shape=jax.ShapeDtypeStruct((cells, channels), bf16),
        in_specs=[VMEM] * 6,
        out_specs=VMEM,
        scratch_shapes=[
            pltpu.VMEM((4 * channels, 6 * channels), bf16),
            pltpu.VMEM((COLS_DEV + 8, 2 * channels), f32),
            pltpu.VMEM((COLS_DEV + 8, 2 * channels), f32),
            pltpu.VMEM((ROWS_DEV + 8, channels), f32),
        ],
        name="conv",
    )(bev, up, down, sides, weight, bias)


def exchange_columns(bev, top, bottom, sides):
    cells = bev.reshape(ROWS_DEV, COLS_DEV, -1)
    west, east = shift(cells[:, -1], "gy", 1), shift(cells[:, 0], "gy", -1)
    rest = jnp.zeros((EDGE - 2, west.shape[1]), west.dtype)
    top = jnp.concatenate([top[:COLS_DEV], west[:1], east[:1], rest], axis=0)
    bottom = jnp.concatenate([bottom[:COLS_DEV], west[ROWS_DEV - 1 :], east[ROWS_DEV - 1 :], rest], axis=0)
    return top, bottom, jnp.concatenate([west, east], axis=0)


def keep_columns(bev, top, bottom, sides):
    return top, bottom, sides


def shards(point_feats, point_tile, point_cell, point_count, conv_weight, conv_bias):
    across = lax.axis_size("gy")
    devices = lax.axis_size("gx") * across
    channels = point_feats.shape[1]
    sent = pack(point_feats, point_tile, point_cell, point_count, devices, across)
    got = lax.all_to_all(sent, ("gx", "gy"), split_axis=0, concat_axis=0, tiled=True)
    bev, top, bottom, sides, full = add_up(got)
    top, bottom, sides = lax.switch(full[0], (keep_columns, exchange_columns), bev, top, bottom, sides)
    up = shift(bottom, "gx", 1)
    down = shift(top, "gx", -1)
    conv_out = conv(bev, up, down, sides, conv_weight, conv_bias.reshape(1, channels))
    whole = (ROWS_DEV, COLS_DEV, channels)
    return (bev.reshape(whole), conv_out.reshape(whole))


def solution(mesh):
    in_specs = (
        P(("gx", "gy"), None),
        P(("gx", "gy"), None),
        P(("gx", "gy")),
        P(("gx", "gy")),
        P(),
        P(),
    )
    out_specs = (P("gx", "gy", None), P("gx", "gy", None))
    return jax.shard_map(shards, mesh=mesh, in_specs=in_specs, out_specs=out_specs, check_vma=False)
```

```python
import functools

import jax
import jax.numpy as jnp
from jax import lax
from jax.experimental import pallas as pl
from jax.experimental.pallas import tpu as pltpu
from jax.sharding import PartitionSpec as P

COLS_DEV = 256
ROWS_DEV = 16
CELLS = ROWS_DEV * COLS_DEV
LANES = 128
CAP = 80
BLOCK = 88
SUMS = 8
SPARE = 6
HALO = 2 * ROWS_DEV
DUMP = CELLS + HALO
EDGE = 16
MOVES = 512
TOGETHER = 8


def pack_kernel(
    across, count_ref, cell_ref, tile_ref, feats_hbm, out_hbm,
    feats, rows, slots, pos_f, pos_s, hits, coded, twins, twin_code, twin_f, twin_s, sent,
    sem, twin_sem, in_sem, out_sems,
):
    count = count_ref[0]
    width = 2 * LANES
    points = tile_ref.shape[1]
    chunks = points // width
    tiles = out_hbm.shape[0]
    load = pltpu.make_async_copy(feats_hbm, feats, in_sem)
    load.start()
    tile_id = lax.broadcasted_iota(jnp.int32, (tiles, width), 0)
    lane = lax.broadcasted_iota(jnp.int32, (1, width), 1)
    source = lax.broadcasted_iota(jnp.int32, (width, width + LANES), 0)
    column = lax.broadcasted_iota(jnp.int32, (width, width + LANES), 1)
    one, zero = jnp.ones((), jnp.bfloat16), jnp.zeros((), jnp.bfloat16)
    upto = jnp.where((source <= column) | (column >= width), 1.0, 0.0).astype(jnp.bfloat16)
    tile_mark = tile_id.astype(jnp.float32).astype(jnp.bfloat16)
    spare_id = lax.broadcasted_iota(jnp.int32, (8, width), 0)
    nothing = jnp.zeros((8, width), jnp.float32)

    def as_bf16(x):
        return x.astype(jnp.float32).astype(jnp.bfloat16)

    def pick(mark, found, before):
        place = found[:, :width].astype(jnp.bfloat16) + jnp.concatenate([before] * (width // LANES), axis=1)
        place = jnp.where(mark, place, zero)
        while place.shape[0] > 16:
            half = place.shape[0] // 2
            place = place[:half, :] + place[half:, :]
        order = jnp.sum(place.astype(jnp.float32), axis=0, keepdims=True).astype(jnp.int32) - 1
        return order, before + found[:, width:].astype(jnp.bfloat16)

    def rank(g, befores):
        before, twin_before = befores
        marks, twin_marks, info = [], [], []
        for c in range(TOGETHER):
            i = g * TOGETHER + c
            here = pl.ds(pl.multiple_of(i * width, width), width)
            live = i * width + lane < count
            tile = jnp.where(live, tile_ref[:, here], tiles)
            match = tile_mark == as_bf16(tile)
            mark = jnp.where(match, one, zero)
            hits[:, here] = mark
            marks.append(mark)
            cell = cell_ref[:, here]
            along = cell & (COLS_DEV - 1)
            place = tile & (across - 1)
            west = live & (along == 0) & (place > 0)
            east = live & (along == COLS_DEV - 1) & (place < across - 1)
            twin = jnp.where(west, tile - 1, jnp.where(east, tile + 1, tiles))
            twin_match = tile_mark == as_bf16(twin)
            twin_mark = jnp.where(twin_match, one, zero)
            twins[:, here] = twin_mark
            twin_marks.append(twin_mark)
            code = jnp.where(west, ROWS_DEV, 0) + lax.shift_right_logical(cell, 8)
            info.append((tile, live, here, i, cell, code, match, twin_match))
        found = jnp.dot(jnp.concatenate(marks, axis=0), upto, preferred_element_type=jnp.float32)
        twin_found = jnp.dot(jnp.concatenate(twin_marks, axis=0), upto, preferred_element_type=jnp.float32)
        for c in range(TOGETHER):
            tile, live, here, i, cell, code, match, twin_match = info[c]
            level, before = pick(match, found[c * tiles : (c + 1) * tiles, :], before)
            slot = jnp.where(live, tile * LANES + level, tiles * LANES - 1)
            pos_f[pl.ds(pl.multiple_of(i * width, width), width)] = slot.reshape(width)
            at_level = tile_mark[:CAP, :] == as_bf16(level)
            coded[:CAP, here] = jnp.where(at_level, as_bf16(lax.shift_right_logical(cell, 6)), zero)
            coded[CAP:, here] = jnp.where(at_level, as_bf16(cell & 63), zero)
            order, twin_before = pick(twin_match, twin_found[c * tiles : (c + 1) * tiles, :], twin_before)
            at_order = spare_id == order
            point = i * width + lane
            high = jnp.where(at_order, (point & -LANES).astype(jnp.float32), nothing)
            low = jnp.where(at_order, (point & (LANES - 1)).astype(jnp.float32), nothing)
            value = jnp.where(at_order, code.astype(jnp.float32), nothing)
            twin_code[:16, here] = jnp.concatenate([high, low], axis=0).astype(jnp.bfloat16)
            twin_code[16:, here] = jnp.concatenate([value, nothing], axis=0).astype(jnp.bfloat16)
        return before, twin_before

    start = jnp.zeros((tiles, LANES), jnp.bfloat16)
    total, twin_total = lax.fori_loop(0, chunks // TOGETHER, rank, (start, start))
    total, twin_total = total.astype(jnp.float32), twin_total.astype(jnp.float32)
    to_smem = pltpu.make_async_copy(pos_f, pos_s, sem)
    to_smem.start()
    across_lanes = (((1,), (1,)), ((), ()))
    extra = lax.dot_general(twin_code[...], twins[...], across_lanes, preferred_element_type=jnp.float32)
    twin_f[...] = (extra[:8, :] + extra[8:16, :]).astype(jnp.int32).reshape(8 * tiles)
    twins_to_smem = pltpu.make_async_copy(twin_f, twin_s, twin_sem)
    twins_to_smem.start()
    spot = lax.broadcasted_iota(jnp.int32, (tiles, LANES), 1).astype(jnp.float32)
    blank = jnp.zeros((CAP, tiles), jnp.float32)
    codes = jnp.concatenate([blank, extra[16:, :], jnp.zeros((LANES - CAP - 16, tiles), jnp.float32)], axis=0).T
    load.wait()
    rows[...] = feats[...].astype(jnp.float32)
    cells = lax.dot_general(coded[...], hits[...], across_lanes, preferred_element_type=jnp.float32)
    filler = jnp.zeros((LANES - CAP, tiles), jnp.float32)
    to_smem.wait()

    def move(i, carry):
        for k in range(MOVES):
            slot = pos_s.at[pl.ds(k, points - MOVES + 1)][i * MOVES]
            slots[pl.ds(slot, 1), :] = rows[pl.ds(i * MOVES + k, 1), :]
        return carry

    lax.fori_loop(0, (count + (MOVES - 1)) // MOVES, move, 0)
    twins_to_smem.wait()

    def move_twins(t, carry):
        for u in range(8):
            for j in range(SPARE):
                point = twin_s.at[pl.ds(j * tiles + u, tiles - 7)][t * 8]
                slots[pl.ds(t * (8 * LANES) + u * LANES + CAP + 2 + j, 1), :] = rows[pl.ds(point, 1), :]
        return carry

    lax.fori_loop(0, tiles // 8, move_twins, 0)
    high = jnp.where(spot < total, jnp.concatenate([cells[:CAP, :], filler], axis=0).T, float(DUMP // 64))
    low = jnp.where(spot < total, jnp.concatenate([cells[CAP:, :], filler], axis=0).T, float(DUMP % 64))
    low = jnp.where((spot >= CAP) & (spot - CAP < jnp.minimum(twin_total, float(SPARE))), codes, low)
    full = jnp.max(twin_total, axis=0, keepdims=True) > SPARE
    high = jnp.where(spot == LANES - 1, 0.0, high)
    low = jnp.where(spot == LANES - 1, jnp.where(full, 1.0, 0.0), low)
    slots[pl.ds(CAP, tiles, LANES), :] = high
    slots[pl.ds(CAP + 1, tiles, LANES), :] = low

    def narrow(t, carry):
        sent[t] = slots[pl.ds(pl.multiple_of(t * LANES, LANES), BLOCK), :].astype(jnp.bfloat16)
        return carry

    parts = out_sems.shape[0]
    share = tiles // parts
    stores = []
    for k in range(parts):
        lax.fori_loop(k * share, (k + 1) * share, narrow, 0, unroll=4)
        part = pl.ds(k * share, share)
        stores.append(pltpu.make_async_copy(sent.at[part], out_hbm.at[part], out_sems.at[k]))
        stores[-1].start()
    for store in stores:
        store.wait()


def add_kernel(
    got_hbm, out_ref, top_ref, bottom_ref, sides_ref, full_ref,
    got, even, odd, meta, coded, cells_f, cells_s, sem, meta_sem, in_sems, *sums,
):
    sources = got_hbm.shape[0]
    codes = pltpu.make_async_copy(got_hbm.at[:, pl.ds(CAP, 8), :], meta, meta_sem)
    codes.start()
    parts = in_sems.shape[0]
    share = sources // parts
    loads = []
    for k in range(parts):
        part = pl.ds(k * share, share)
        loads.append(pltpu.make_async_copy(got_hbm.at[part], got.at[part], in_sems.at[k]))
        loads[-1].start()
    codes.wait()
    coded[...] = meta[...].astype(jnp.float32).reshape(coded.shape)
    high = coded[pl.ds(0, sources, 8), :].astype(jnp.int32)
    low = coded[pl.ds(1, sources, 8), :].astype(jnp.int32)
    cells = high * 64 + low
    full_ref[0] = jnp.max(cells[:, LANES - 1 :])
    cells_f[...] = cells.reshape(sources * LANES)
    to_smem = pltpu.make_async_copy(cells_f, cells_s, sem)
    to_smem.start()

    def clear(i, carry):
        for part in sums:
            part[pl.ds(pl.multiple_of(i * 256, 256), 256), :] = jnp.zeros((256, LANES), jnp.float32)
        return carry

    lax.fori_loop(0, CELLS // 256, clear, 0)
    for part in sums:
        part[pl.ds(CELLS, HALO + 8), :] = jnp.zeros((HALO + 8, LANES), jnp.float32)

    def widen(s, rows):
        rows[...] = got[jnp.minimum(s, sources - 1)].astype(jnp.float32)

    def add(s, rows):
        for j in range(CAP + SPARE):
            cell = pl.ds(cells_s.at[pl.ds(j, (sources - 1) * LANES + 1)][s * LANES], 1)
            part = sums[j % SUMS]
            k = j if j < CAP else j + 2
            part[cell, :] = part[cell, :] + rows[k : k + 1, :]

    def two(q, carry):
        widen(2 * q + 1, odd)
        add(2 * q, even)
        widen(2 * q + 2, even)
        add(2 * q + 1, odd)
        return carry

    to_smem.wait()
    for load in loads:
        load.wait()
    widen(0, even)
    lax.fori_loop(0, sources // 2, two, 0)
    step = 256

    def close(i, carry):
        at = pl.ds(pl.multiple_of(i * step, step), step)
        total = sums[0][at, :]
        for part in sums[1:]:
            total = total + part[at, :]
        out_ref[at, :] = total.astype(jnp.bfloat16)
        return carry

    lax.fori_loop(0, CELLS // step, close, 0)

    def column(start, stride):
        at = pl.ds(start, ROWS_DEV, stride)
        total = sums[0][at, :]
        for part in sums[1:]:
            total = total + part[at, :]
        return total

    west, east = column(CELLS, 1), column(CELLS + ROWS_DEV, 1)
    sides_ref[:ROWS_DEV, :] = west.astype(jnp.bfloat16)
    sides_ref[ROWS_DEV:, :] = east.astype(jnp.bfloat16)
    spot = lax.broadcasted_iota(jnp.int32, (EDGE, LANES), 0)
    for ref, r in ((top_ref, 0), (bottom_ref, ROWS_DEV - 1)):
        ref[:COLS_DEV, :] = out_ref[r * COLS_DEV : (r + 1) * COLS_DEV, :]
        corners = jnp.where(spot == 0, west[r : r + 1, :], jnp.where(spot == 1, east[r : r + 1, :], 0.0))
        ref[COLS_DEV:, :] = corners.astype(jnp.bfloat16)


def fill_wide(weight_ref, wide):
    for i in range(4):
        for b in range(3):
            for o in range(2):
                block = (slice(i * LANES, (i + 1) * LANES), slice((2 * b + o) * LANES, (2 * b + o + 1) * LANES))
                wide[block] = weight_ref[i - o, b] if 0 <= i - o < 3 else jnp.zeros((LANES, LANES), jnp.bfloat16)


def conv_rows(row, pairs, west, east, bias, out_ref, wide, before, after):
    for k, p in enumerate(pairs):
        four = jnp.concatenate([row(2 * p - 1 + i) for i in range(4)], axis=1)
        taps = jnp.dot(four, wide[...], preferred_element_type=jnp.float32)
        before[7:8, :] = west[k : k + 1, :]
        before[8:, :] = taps[:, : 2 * LANES]
        after[:COLS_DEV, :] = taps[:, 4 * LANES :]
        after[COLS_DEV : COLS_DEV + 1, :] = east[k : k + 1, :]
        total = taps[:, 2 * LANES : 4 * LANES] + before[7 : 7 + COLS_DEV, :] + after[1 : 1 + COLS_DEV, :]
        done = jnp.maximum(total + jnp.concatenate([bias, bias], axis=1), 0.0).astype(jnp.bfloat16)
        out_ref[2 * k * COLS_DEV : (2 * k + 1) * COLS_DEV, :] = done[:, :LANES]
        out_ref[(2 * k + 1) * COLS_DEV : (2 * k + 2) * COLS_DEV, :] = done[:, LANES:]


def beside(corner, start, above, below, sides_ref, wide, side):
    side[:1, :] = above[corner : corner + 1, :]
    side[1 : ROWS_DEV + 1, :] = sides_ref[corner * ROWS_DEV : (corner + 1) * ROWS_DEV, :].astype(jnp.float32)
    side[ROWS_DEV + 1 : ROWS_DEV + 2, :] = below[corner : corner + 1, :]
    four = jnp.concatenate([side[pl.ds(i, ROWS_DEV // 2, 2), :] for i in range(4)], axis=1)
    return jnp.dot(four.astype(jnp.bfloat16), wide[:, start : start + 2 * LANES], preferred_element_type=jnp.float32)


def inner_kernel(bev_ref, sides_ref, weight_ref, bias_ref, out_hbm, out, wide, before, after, side, sem):
    fill_wide(weight_ref, wide)
    nothing = jnp.zeros((EDGE, LANES), jnp.float32)
    west = beside(0, 0, nothing, nothing, sides_ref, wide, side)
    east = beside(1, 4 * LANES, nothing, nothing, sides_ref, wide, side)

    def row(r):
        return bev_ref[r * COLS_DEV : (r + 1) * COLS_DEV, :]

    last = ROWS_DEV // 2 - 1
    conv_rows(row, range(1, last), west[1:last, :], east[1:last, :], bias_ref[...], out, wide, before, after)
    part = pl.ds(2 * COLS_DEV, (ROWS_DEV - 4) * COLS_DEV)
    store = pltpu.make_async_copy(out, out_hbm.at[part], sem)
    store.start()
    store.wait()


def outer_kernel(
    conv_ref, bev_ref, up_ref, down_ref, sides_ref, weight_ref, bias_ref,
    out_hbm, out, wide, before, after, side, sems,
):
    fill_wide(weight_ref, wide)
    above = up_ref[COLS_DEV:, :].astype(jnp.float32)
    below = down_ref[COLS_DEV:, :].astype(jnp.float32)
    west = beside(0, 0, above, below, sides_ref, wide, side)
    east = beside(1, 4 * LANES, above, below, sides_ref, wide, side)

    def row(r):
        if r < 0:
            return up_ref[:COLS_DEV, :]
        if r >= ROWS_DEV:
            return down_ref[:COLS_DEV, :]
        return bev_ref[r * COLS_DEV : (r + 1) * COLS_DEV, :]

    last = ROWS_DEV // 2 - 1
    ends = (0, last)
    pick = [jnp.concatenate([x[:1, :], x[last:, :]], axis=0) for x in (west, east)]
    conv_rows(row, ends, *pick, bias_ref[...], out, wide, before, after)
    size = 2 * COLS_DEV
    stores = [
        pltpu.make_async_copy(out.at[pl.ds(k * size, size)], out_hbm.at[pl.ds(p * size, size)], sems.at[k])
        for k, p in enumerate(ends)
    ]
    for store in stores:
        store.start()
    for store in stores:
        store.wait()


VMEM = pl.BlockSpec(memory_space=pltpu.VMEM)
SMEM = pl.BlockSpec(memory_space=pltpu.SMEM)
ANY = pl.BlockSpec(memory_space=pl.ANY)


def pack(point_feats, point_tile, point_cell, point_count, devices, across=8):
    points, channels = point_feats.shape
    if across & (across - 1):
        raise ValueError("across")
    bf16, f32, i32 = jnp.bfloat16, jnp.float32, jnp.int32
    return pl.pallas_call(
        functools.partial(pack_kernel, across),
        out_shape=jax.ShapeDtypeStruct((devices, BLOCK, channels), bf16),
        in_specs=[SMEM, VMEM, VMEM, ANY],
        out_specs=ANY,
        scratch_shapes=[
            pltpu.VMEM((points, channels), bf16),
            pltpu.VMEM((points, channels), f32),
            pltpu.VMEM((devices * LANES, channels), f32),
            pltpu.VMEM((points,), i32),
            pltpu.SMEM((points,), i32),
            pltpu.VMEM((devices, points), bf16),
            pltpu.VMEM((2 * CAP, points), bf16),
            pltpu.VMEM((devices, points), bf16),
            pltpu.VMEM((32, points), bf16),
            pltpu.VMEM((devices * 8,), i32),
            pltpu.SMEM((devices * 8,), i32),
            pltpu.VMEM((devices, BLOCK, channels), bf16),
            pltpu.SemaphoreType.DMA,
            pltpu.SemaphoreType.DMA,
            pltpu.SemaphoreType.DMA,
            pltpu.SemaphoreType.DMA((4,)),
        ],
        name="pack",
    )(
        point_count,
        point_cell.reshape(1, points),
        point_tile.reshape(1, points),
        point_feats,
    )


def add_up(got):
    devices, block, channels = got.shape
    bf16, f32, i32 = jnp.bfloat16, jnp.float32, jnp.int32
    heights = (CELLS, COLS_DEV + EDGE, COLS_DEV + EDGE, HALO)
    return pl.pallas_call(
        add_kernel,
        out_shape=[jax.ShapeDtypeStruct((height, channels), bf16) for height in heights]
        + [jax.ShapeDtypeStruct((1,), i32)],
        in_specs=[ANY],
        out_specs=[VMEM] * 4 + [SMEM],
        scratch_shapes=[
            pltpu.VMEM((devices, block, channels), bf16),
            pltpu.VMEM((block, channels), f32),
            pltpu.VMEM((block, channels), f32),
            pltpu.VMEM((devices, 8, channels), bf16),
            pltpu.VMEM((devices * 8, channels), f32),
            pltpu.VMEM((devices * LANES,), i32),
            pltpu.SMEM((devices * LANES,), i32),
            pltpu.SemaphoreType.DMA,
            pltpu.SemaphoreType.DMA,
            pltpu.SemaphoreType.DMA((4,)),
        ]
        + [pltpu.VMEM((CELLS + HALO + 8, channels), f32)] * SUMS,
        name="add_up",
    )(got)


def shift(cells, axis, step):
    count = lax.axis_size(axis)
    pairs = [(i, i + step) for i in range(count) if 0 <= i + step < count]
    return lax.ppermute(cells, axis, pairs)


def conv_call(kernel, name, ins, rows, sems, aliases, flops, *operands):
    bev, channels = operands[-4 if len(ins) == 4 else 1], LANES
    bf16, f32 = jnp.bfloat16, jnp.float32
    return pl.pallas_call(
        kernel,
        out_shape=jax.ShapeDtypeStruct(bev.shape, bf16),
        in_specs=ins,
        out_specs=ANY,
        input_output_aliases=aliases,
        scratch_shapes=[
            pltpu.VMEM((rows * COLS_DEV, channels), bf16),
            pltpu.VMEM((4 * channels, 6 * channels), bf16),
            pltpu.VMEM((COLS_DEV + 8, 2 * channels), f32),
            pltpu.VMEM((COLS_DEV + 8, 2 * channels), f32),
            pltpu.VMEM((ROWS_DEV + 8, channels), f32),
            sems,
        ],
        cost_estimate=pl.CostEstimate(flops=flops, bytes_accessed=2 * rows * COLS_DEV * channels, transcendentals=0),
        name=name,
    )(*operands)


def exchange_columns(bev, top, bottom, sides):
    cells = bev.reshape(ROWS_DEV, COLS_DEV, -1)
    west, east = shift(cells[:, -1], "gy", 1), shift(cells[:, 0], "gy", -1)
    rest = jnp.zeros((EDGE - 2, west.shape[1]), west.dtype)
    top = jnp.concatenate([top[:COLS_DEV], west[:1], east[:1], rest], axis=0)
    bottom = jnp.concatenate([bottom[:COLS_DEV], west[ROWS_DEV - 1 :], east[ROWS_DEV - 1 :], rest], axis=0)
    return top, bottom, jnp.concatenate([west, east], axis=0)


def keep_columns(bev, top, bottom, sides):
    return top, bottom, sides


def shards(point_feats, point_tile, point_cell, point_count, conv_weight, conv_bias):
    across = lax.axis_size("gy")
    devices = lax.axis_size("gx") * across
    channels = point_feats.shape[1]
    sent = pack(point_feats, point_tile, point_cell, point_count, devices, across)
    got = lax.all_to_all(sent, ("gx", "gy"), split_axis=0, concat_axis=0, tiled=True)
    bev, top, bottom, sides, full = add_up(got)
    top, bottom, sides = lax.switch(full[0], (keep_columns, exchange_columns), bev, top, bottom, sides)
    up = shift(bottom, "gx", 1)
    down = shift(top, "gx", -1)
    bias = conv_bias.reshape(1, channels)
    dma = pltpu.SemaphoreType.DMA
    work = 2 * CELLS * 9 * channels * channels
    inner = conv_call(
        inner_kernel, "inner", [VMEM] * 4, ROWS_DEV - 4, dma, {}, work, bev, sides, conv_weight, bias
    )
    conv_out = conv_call(
        outer_kernel, "outer", [ANY] + [VMEM] * 6, 4, dma((2,)), {0: 0}, work // 4,
        inner, bev, up, down, sides, conv_weight, bias,
    )
    whole = (ROWS_DEV, COLS_DEV, channels)
    return (bev.reshape(whole), conv_out.reshape(whole))


def solution(mesh):
    in_specs = (
        P(("gx", "gy"), None),
        P(("gx", "gy"), None),
        P(("gx", "gy")),
        P(("gx", "gy")),
        P(),
        P(),
    )
    out_specs = (P("gx", "gy", None), P("gx", "gy", None))
    return jax.shard_map(shards, mesh=mesh, in_specs=in_specs, out_specs=out_specs, check_vma=False)
```

```python
import functools

import jax
import jax.numpy as jnp
from jax import lax
from jax.experimental import pallas as pl
from jax.experimental.pallas import tpu as pltpu
from jax.sharding import PartitionSpec as P

COLS_DEV = 256
ROWS_DEV = 16
CELLS = ROWS_DEV * COLS_DEV
LANES = 128
CAP = 80
BLOCK = 88
SUMS = 8
SPARE = 6
HALO = 2 * ROWS_DEV
DUMP = CELLS + HALO
EDGE = 16
PACK_VMEM = 60 * 2**20
ADD_VMEM = 32 * 2**20
MOVES = 512
TOGETHER = 8


def pack_kernel(
    across, count_ref, cell_ref, tile_ref, feats_hbm, out_ref,
    feats, rows, slots, pos_f, pos_s, hits, coded, twins, twin_code, twin_f, twin_s,
    sem, twin_sem, in_sem,
):
    count = count_ref[0]
    width = 2 * LANES
    points = tile_ref.shape[1]
    chunks = points // width
    tiles = out_ref.shape[0]
    load = pltpu.make_async_copy(feats_hbm, feats, in_sem)
    load.start()
    tile_id = lax.broadcasted_iota(jnp.int32, (tiles, width), 0)
    lane = lax.broadcasted_iota(jnp.int32, (1, width), 1)
    source = lax.broadcasted_iota(jnp.int32, (width, width + LANES), 0)
    column = lax.broadcasted_iota(jnp.int32, (width, width + LANES), 1)
    one, zero = jnp.ones((), jnp.bfloat16), jnp.zeros((), jnp.bfloat16)
    upto = jnp.where((source <= column) | (column >= width), 1.0, 0.0).astype(jnp.bfloat16)
    tile_mark = tile_id.astype(jnp.float32).astype(jnp.bfloat16)
    spare_id = lax.broadcasted_iota(jnp.int32, (8, width), 0)
    nothing = jnp.zeros((8, width), jnp.float32)

    def as_bf16(x):
        return x.astype(jnp.float32).astype(jnp.bfloat16)

    def pick(mark, found, before):
        place = found[:, :width].astype(jnp.bfloat16) + jnp.concatenate([before] * (width // LANES), axis=1)
        place = jnp.where(mark, place, zero)
        while place.shape[0] > 16:
            half = place.shape[0] // 2
            place = place[:half, :] + place[half:, :]
        order = jnp.sum(place.astype(jnp.float32), axis=0, keepdims=True).astype(jnp.int32) - 1
        return order, before + found[:, width:].astype(jnp.bfloat16)

    def rank(g, befores):
        before, twin_before = befores
        marks, twin_marks, info = [], [], []
        for c in range(TOGETHER):
            i = g * TOGETHER + c
            here = pl.ds(pl.multiple_of(i * width, width), width)
            live = i * width + lane < count
            tile = jnp.where(live, tile_ref[:, here], tiles)
            match = tile_mark == as_bf16(tile)
            mark = jnp.where(match, one, zero)
            hits[:, here] = mark
            marks.append(mark)
            cell = cell_ref[:, here]
            along = cell & (COLS_DEV - 1)
            place = tile & (across - 1)
            west = live & (along == 0) & (place > 0)
            east = live & (along == COLS_DEV - 1) & (place < across - 1)
            twin = jnp.where(west, tile - 1, jnp.where(east, tile + 1, tiles))
            twin_match = tile_mark == as_bf16(twin)
            twin_mark = jnp.where(twin_match, one, zero)
            twins[:, here] = twin_mark
            twin_marks.append(twin_mark)
            code = jnp.where(west, ROWS_DEV, 0) + lax.shift_right_logical(cell, 8)
            info.append((tile, live, here, i, cell, code, match, twin_match))
        found = jnp.dot(jnp.concatenate(marks, axis=0), upto, preferred_element_type=jnp.float32)
        twin_found = jnp.dot(jnp.concatenate(twin_marks, axis=0), upto, preferred_element_type=jnp.float32)
        for c in range(TOGETHER):
            tile, live, here, i, cell, code, match, twin_match = info[c]
            level, before = pick(match, found[c * tiles : (c + 1) * tiles, :], before)
            slot = jnp.where(live, tile * LANES + level, tiles * LANES - 1)
            pos_f[pl.ds(pl.multiple_of(i * width, width), width)] = slot.reshape(width)
            at_level = tile_mark[:CAP, :] == as_bf16(level)
            coded[:CAP, here] = jnp.where(at_level, as_bf16(lax.shift_right_logical(cell, 6)), zero)
            coded[CAP:, here] = jnp.where(at_level, as_bf16(cell & 63), zero)
            order, twin_before = pick(twin_match, twin_found[c * tiles : (c + 1) * tiles, :], twin_before)
            at_order = spare_id == order
            point = i * width + lane
            high = jnp.where(at_order, (point & -LANES).astype(jnp.float32), nothing)
            low = jnp.where(at_order, (point & (LANES - 1)).astype(jnp.float32), nothing)
            value = jnp.where(at_order, code.astype(jnp.float32), nothing)
            twin_code[:16, here] = jnp.concatenate([high, low], axis=0).astype(jnp.bfloat16)
            twin_code[16:, here] = jnp.concatenate([value, nothing], axis=0).astype(jnp.bfloat16)
        return before, twin_before

    start = jnp.zeros((tiles, LANES), jnp.bfloat16)
    total, twin_total = lax.fori_loop(0, chunks // TOGETHER, rank, (start, start))
    total, twin_total = total.astype(jnp.float32), twin_total.astype(jnp.float32)
    to_smem = pltpu.make_async_copy(pos_f, pos_s, sem)
    to_smem.start()
    across_lanes = (((1,), (1,)), ((), ()))
    extra = lax.dot_general(twin_code[...], twins[...], across_lanes, preferred_element_type=jnp.float32)
    twin_f[...] = (extra[:8, :] + extra[8:16, :]).astype(jnp.int32).reshape(8 * tiles)
    twins_to_smem = pltpu.make_async_copy(twin_f, twin_s, twin_sem)
    twins_to_smem.start()
    spot = lax.broadcasted_iota(jnp.int32, (tiles, LANES), 1).astype(jnp.float32)
    blank = jnp.zeros((CAP, tiles), jnp.float32)
    codes = jnp.concatenate([blank, extra[16:, :], jnp.zeros((LANES - CAP - 16, tiles), jnp.float32)], axis=0).T
    load.wait()
    rows[...] = feats[...].astype(jnp.float32)
    cells = lax.dot_general(coded[...], hits[...], across_lanes, preferred_element_type=jnp.float32)
    filler = jnp.zeros((LANES - CAP, tiles), jnp.float32)
    to_smem.wait()

    def move(i, carry):
        for k in range(MOVES):
            slot = pos_s.at[pl.ds(k, points - MOVES + 1)][i * MOVES]
            slots[pl.ds(slot, 1), :] = rows[pl.ds(i * MOVES + k, 1), :]
        return carry

    lax.fori_loop(0, (count + (MOVES - 1)) // MOVES, move, 0)
    twins_to_smem.wait()

    def move_twins(t, carry):
        for u in range(8):
            for j in range(SPARE):
                point = twin_s.at[pl.ds(j * tiles + u, tiles - 7)][t * 8]
                slots[pl.ds(t * (8 * LANES) + u * LANES + CAP + 2 + j, 1), :] = rows[pl.ds(point, 1), :]
        return carry

    lax.fori_loop(0, tiles // 8, move_twins, 0)
    high = jnp.where(spot < total, jnp.concatenate([cells[:CAP, :], filler], axis=0).T, float(DUMP // 64))
    low = jnp.where(spot < total, jnp.concatenate([cells[CAP:, :], filler], axis=0).T, float(DUMP % 64))
    low = jnp.where((spot >= CAP) & (spot - CAP < jnp.minimum(twin_total, float(SPARE))), codes, low)
    full = jnp.max(twin_total, axis=0, keepdims=True) > SPARE
    high = jnp.where(spot == LANES - 1, 0.0, high)
    low = jnp.where(spot == LANES - 1, jnp.where(full, 1.0, 0.0), low)
    slots[pl.ds(CAP, tiles, LANES), :] = high
    slots[pl.ds(CAP + 1, tiles, LANES), :] = low

    def narrow(t, carry):
        out_ref[t] = slots[pl.ds(pl.multiple_of(t * LANES, LANES), BLOCK), :].astype(jnp.bfloat16)
        return carry

    lax.fori_loop(0, tiles, narrow, 0, unroll=4)


def add_kernel(
    got_ref, out_ref, top_ref, bottom_ref, sides_ref, full_ref,
    even, odd, coded, cells_f, cells_s, sem, *sums,
):
    sources = got_ref.shape[0]
    coded[...] = got_ref[:, CAP:, :].astype(jnp.float32).reshape(coded.shape)
    high = coded[pl.ds(0, sources, 8), :].astype(jnp.int32)
    low = coded[pl.ds(1, sources, 8), :].astype(jnp.int32)
    cells = high * 64 + low
    full_ref[0] = jnp.max(cells[:, LANES - 1 :])
    cells_f[...] = cells.reshape(sources * LANES)
    to_smem = pltpu.make_async_copy(cells_f, cells_s, sem)
    to_smem.start()

    def clear(i, carry):
        for part in sums:
            part[pl.ds(pl.multiple_of(i * 256, 256), 256), :] = jnp.zeros((256, LANES), jnp.float32)
        return carry

    lax.fori_loop(0, CELLS // 256, clear, 0)
    for part in sums:
        part[pl.ds(CELLS, HALO + 8), :] = jnp.zeros((HALO + 8, LANES), jnp.float32)

    def widen(s, rows):
        rows[...] = got_ref[jnp.minimum(s, sources - 1)].astype(jnp.float32)

    def add(s, rows):
        for j in range(CAP + SPARE):
            cell = pl.ds(cells_s.at[pl.ds(j, (sources - 1) * LANES + 1)][s * LANES], 1)
            part = sums[j % SUMS]
            k = j if j < CAP else j + 2
            part[cell, :] = part[cell, :] + rows[k : k + 1, :]

    def two(q, carry):
        widen(2 * q + 1, odd)
        add(2 * q, even)
        widen(2 * q + 2, even)
        add(2 * q + 1, odd)
        return carry

    to_smem.wait()
    widen(0, even)
    lax.fori_loop(0, sources // 2, two, 0)
    step = 256

    def close(i, carry):
        at = pl.ds(pl.multiple_of(i * step, step), step)
        total = sums[0][at, :]
        for part in sums[1:]:
            total = total + part[at, :]
        out_ref[at, :] = total.astype(jnp.bfloat16)
        return carry

    lax.fori_loop(0, CELLS // step, close, 0)

    def column(start, stride):
        at = pl.ds(start, ROWS_DEV, stride)
        total = sums[0][at, :]
        for part in sums[1:]:
            total = total + part[at, :]
        return total

    west, east = column(CELLS, 1), column(CELLS + ROWS_DEV, 1)
    sides_ref[:ROWS_DEV, :] = west.astype(jnp.bfloat16)
    sides_ref[ROWS_DEV:, :] = east.astype(jnp.bfloat16)
    spot = lax.broadcasted_iota(jnp.int32, (EDGE, LANES), 0)
    for ref, r in ((top_ref, 0), (bottom_ref, ROWS_DEV - 1)):
        ref[:COLS_DEV, :] = out_ref[r * COLS_DEV : (r + 1) * COLS_DEV, :]
        corners = jnp.where(spot == 0, west[r : r + 1, :], jnp.where(spot == 1, east[r : r + 1, :], 0.0))
        ref[COLS_DEV:, :] = corners.astype(jnp.bfloat16)


def fill_wide(weight_ref, wide):
    for i in range(4):
        for b in range(3):
            for o in range(2):
                block = (slice(i * LANES, (i + 1) * LANES), slice((2 * b + o) * LANES, (2 * b + o + 1) * LANES))
                wide[block] = weight_ref[i - o, b] if 0 <= i - o < 3 else jnp.zeros((LANES, LANES), jnp.bfloat16)


def conv_rows(row, pairs, west, east, bias, out_ref, wide, before, after):
    for k, p in enumerate(pairs):
        four = jnp.concatenate([row(2 * p - 1 + i) for i in range(4)], axis=1)
        taps = jnp.dot(four, wide[...], preferred_element_type=jnp.float32)
        before[7:8, :] = west[k : k + 1, :]
        before[8:, :] = taps[:, : 2 * LANES]
        after[:COLS_DEV, :] = taps[:, 4 * LANES :]
        after[COLS_DEV : COLS_DEV + 1, :] = east[k : k + 1, :]
        total = taps[:, 2 * LANES : 4 * LANES] + before[7 : 7 + COLS_DEV, :] + after[1 : 1 + COLS_DEV, :]
        done = jnp.maximum(total + jnp.concatenate([bias, bias], axis=1), 0.0).astype(jnp.bfloat16)
        out_ref[2 * k * COLS_DEV : (2 * k + 1) * COLS_DEV, :] = done[:, :LANES]
        out_ref[(2 * k + 1) * COLS_DEV : (2 * k + 2) * COLS_DEV, :] = done[:, LANES:]


def beside(corner, start, above, below, sides_ref, wide, side):
    side[:1, :] = above[corner : corner + 1, :]
    side[1 : ROWS_DEV + 1, :] = sides_ref[corner * ROWS_DEV : (corner + 1) * ROWS_DEV, :].astype(jnp.float32)
    side[ROWS_DEV + 1 : ROWS_DEV + 2, :] = below[corner : corner + 1, :]
    four = jnp.concatenate([side[pl.ds(i, ROWS_DEV // 2, 2), :] for i in range(4)], axis=1)
    return jnp.dot(four.astype(jnp.bfloat16), wide[:, start : start + 2 * LANES], preferred_element_type=jnp.float32)


def inner_kernel(bev_ref, sides_ref, weight_ref, bias_ref, out_hbm, out, wide, before, after, side, sem):
    fill_wide(weight_ref, wide)
    nothing = jnp.zeros((EDGE, LANES), jnp.float32)
    west = beside(0, 0, nothing, nothing, sides_ref, wide, side)
    east = beside(1, 4 * LANES, nothing, nothing, sides_ref, wide, side)

    def row(r):
        return bev_ref[r * COLS_DEV : (r + 1) * COLS_DEV, :]

    last = ROWS_DEV // 2 - 1
    conv_rows(row, range(1, last), west[1:last, :], east[1:last, :], bias_ref[...], out, wide, before, after)
    part = pl.ds(2 * COLS_DEV, (ROWS_DEV - 4) * COLS_DEV)
    store = pltpu.make_async_copy(out, out_hbm.at[part], sem)
    store.start()
    store.wait()


def outer_kernel(
    conv_ref, bev_ref, up_ref, down_ref, sides_ref, weight_ref, bias_ref,
    out_hbm, out, wide, before, after, side, sems,
):
    fill_wide(weight_ref, wide)
    above = up_ref[COLS_DEV:, :].astype(jnp.float32)
    below = down_ref[COLS_DEV:, :].astype(jnp.float32)
    west = beside(0, 0, above, below, sides_ref, wide, side)
    east = beside(1, 4 * LANES, above, below, sides_ref, wide, side)

    def row(r):
        if r < 0:
            return up_ref[:COLS_DEV, :]
        if r >= ROWS_DEV:
            return down_ref[:COLS_DEV, :]
        return bev_ref[r * COLS_DEV : (r + 1) * COLS_DEV, :]

    last = ROWS_DEV // 2 - 1
    ends = (0, last)
    pick = [jnp.concatenate([x[:1, :], x[last:, :]], axis=0) for x in (west, east)]
    conv_rows(row, ends, *pick, bias_ref[...], out, wide, before, after)
    size = 2 * COLS_DEV
    stores = [
        pltpu.make_async_copy(out.at[pl.ds(k * size, size)], out_hbm.at[pl.ds(p * size, size)], sems.at[k])
        for k, p in enumerate(ends)
    ]
    for store in stores:
        store.start()
    for store in stores:
        store.wait()


VMEM = pl.BlockSpec(memory_space=pltpu.VMEM)
SMEM = pl.BlockSpec(memory_space=pltpu.SMEM)
ANY = pl.BlockSpec(memory_space=pl.ANY)


def pack(point_feats, point_tile, point_cell, point_count, devices, across=8):
    points, channels = point_feats.shape
    if across & (across - 1):
        raise ValueError("across")
    bf16, f32, i32 = jnp.bfloat16, jnp.float32, jnp.int32
    return pl.pallas_call(
        functools.partial(pack_kernel, across),
        out_shape=jax.ShapeDtypeStruct((devices, BLOCK, channels), bf16),
        in_specs=[SMEM, VMEM, VMEM, ANY],
        out_specs=VMEM,
        scratch_shapes=[
            pltpu.VMEM((points, channels), bf16),
            pltpu.VMEM((points, channels), f32),
            pltpu.VMEM((devices * LANES, channels), f32),
            pltpu.VMEM((points,), i32),
            pltpu.SMEM((points,), i32),
            pltpu.VMEM((devices, points), bf16),
            pltpu.VMEM((2 * CAP, points), bf16),
            pltpu.VMEM((devices, points), bf16),
            pltpu.VMEM((32, points), bf16),
            pltpu.VMEM((devices * 8,), i32),
            pltpu.SMEM((devices * 8,), i32),
            pltpu.SemaphoreType.DMA,
            pltpu.SemaphoreType.DMA,
            pltpu.SemaphoreType.DMA,
        ],
        compiler_params=pltpu.CompilerParams(vmem_limit_bytes=PACK_VMEM),
        name="pack",
    )(
        point_count,
        point_cell.reshape(1, points),
        point_tile.reshape(1, points),
        point_feats,
    )


def add_up(got):
    devices, block, channels = got.shape
    bf16, f32, i32 = jnp.bfloat16, jnp.float32, jnp.int32
    heights = (CELLS, COLS_DEV + EDGE, COLS_DEV + EDGE, HALO)
    return pl.pallas_call(
        add_kernel,
        out_shape=[jax.ShapeDtypeStruct((height, channels), bf16) for height in heights]
        + [jax.ShapeDtypeStruct((1,), i32)],
        in_specs=[VMEM],
        out_specs=[VMEM] * 4 + [SMEM],
        compiler_params=pltpu.CompilerParams(vmem_limit_bytes=ADD_VMEM),
        scratch_shapes=[
            pltpu.VMEM((block, channels), f32),
            pltpu.VMEM((block, channels), f32),
            pltpu.VMEM((devices * 8, channels), f32),
            pltpu.VMEM((devices * LANES,), i32),
            pltpu.SMEM((devices * LANES,), i32),
            pltpu.SemaphoreType.DMA,
        ]
        + [pltpu.VMEM((CELLS + HALO + 8, channels), f32)] * SUMS,
        name="add_up",
    )(got)


def shift(cells, axis, step):
    count = lax.axis_size(axis)
    pairs = [(i, i + step) for i in range(count) if 0 <= i + step < count]
    return lax.ppermute(cells, axis, pairs)


def conv_call(kernel, name, ins, rows, sems, aliases, flops, *operands):
    bev, channels = operands[-4 if len(ins) == 4 else 1], LANES
    bf16, f32 = jnp.bfloat16, jnp.float32
    return pl.pallas_call(
        kernel,
        out_shape=jax.ShapeDtypeStruct(bev.shape, bf16),
        in_specs=ins,
        out_specs=ANY,
        input_output_aliases=aliases,
        scratch_shapes=[
            pltpu.VMEM((rows * COLS_DEV, channels), bf16),
            pltpu.VMEM((4 * channels, 6 * channels), bf16),
            pltpu.VMEM((COLS_DEV + 8, 2 * channels), f32),
            pltpu.VMEM((COLS_DEV + 8, 2 * channels), f32),
            pltpu.VMEM((ROWS_DEV + 8, channels), f32),
            sems,
        ],
        compiler_params=pltpu.CompilerParams(vmem_limit_bytes=16 * 2**20),
        cost_estimate=pl.CostEstimate(flops=flops, bytes_accessed=2 * rows * COLS_DEV * channels, transcendentals=0),
        name=name,
    )(*operands)


def exchange_columns(bev, top, bottom, sides):
    cells = bev.reshape(ROWS_DEV, COLS_DEV, -1)
    west, east = shift(cells[:, -1], "gy", 1), shift(cells[:, 0], "gy", -1)
    rest = jnp.zeros((EDGE - 2, west.shape[1]), west.dtype)
    top = jnp.concatenate([top[:COLS_DEV], west[:1], east[:1], rest], axis=0)
    bottom = jnp.concatenate([bottom[:COLS_DEV], west[ROWS_DEV - 1 :], east[ROWS_DEV - 1 :], rest], axis=0)
    return top, bottom, jnp.concatenate([west, east], axis=0)


def keep_columns(bev, top, bottom, sides):
    return top, bottom, sides


def shards(point_feats, point_tile, point_cell, point_count, conv_weight, conv_bias):
    across = lax.axis_size("gy")
    devices = lax.axis_size("gx") * across
    channels = point_feats.shape[1]
    sent = pack(point_feats, point_tile, point_cell, point_count, devices, across)
    got = lax.all_to_all(sent, ("gx", "gy"), split_axis=0, concat_axis=0, tiled=True)
    bev, top, bottom, sides, full = add_up(got)
    top, bottom, sides = lax.switch(full[0], (keep_columns, exchange_columns), bev, top, bottom, sides)
    up = shift(bottom, "gx", 1)
    down = shift(top, "gx", -1)
    bias = conv_bias.reshape(1, channels)
    dma = pltpu.SemaphoreType.DMA
    work = 2 * CELLS * 9 * channels * channels
    inner = conv_call(
        inner_kernel, "inner", [VMEM] * 4, ROWS_DEV - 4, dma, {}, work, bev, sides, conv_weight, bias
    )
    conv_out = conv_call(
        outer_kernel, "outer", [ANY] + [VMEM] * 6, 4, dma((2,)), {0: 0}, work // 4,
        inner, bev, up, down, sides, conv_weight, bias,
    )
    whole = (ROWS_DEV, COLS_DEV, channels)
    return (bev.reshape(whole), conv_out.reshape(whole))


def solution(mesh):
    in_specs = (
        P(("gx", "gy"), None),
        P(("gx", "gy"), None),
        P(("gx", "gy")),
        P(("gx", "gy")),
        P(),
        P(),
    )
    out_specs = (P("gx", "gy", None), P("gx", "gy", None))
    return jax.shard_map(shards, mesh=mesh, in_specs=in_specs, out_specs=out_specs, check_vma=False)
```

```python
import functools

import jax
import jax.numpy as jnp
from jax import lax
from jax.experimental import pallas as pl
from jax.experimental.pallas import tpu as pltpu
from jax.sharding import PartitionSpec as P

COLS_DEV = 256
ROWS_DEV = 16
CELLS = ROWS_DEV * COLS_DEV
LANES = 128
CAP = 80
BLOCK = 88
SUMS = 8
SPARE = 6
HALO = 2 * ROWS_DEV
DUMP = CELLS + HALO
EDGE = 16
PACK_VMEM = 40 * 2**20
ADD_VMEM = 32 * 2**20
MOVES = 512
TOGETHER = 8


def pack_kernel(
    across, count_ref, cell_ref, tile_ref, feats_ref, out_ref,
    rows, slots, pos_f, pos_s, hits, coded, twins, twin_code, twin_f, twin_s,
    sem, twin_sem,
):
    count = count_ref[0]
    width = 2 * LANES
    points = tile_ref.shape[1]
    chunks = points // width
    tiles = out_ref.shape[0]
    tile_id = lax.broadcasted_iota(jnp.int32, (tiles, width), 0)
    lane = lax.broadcasted_iota(jnp.int32, (1, width), 1)
    source = lax.broadcasted_iota(jnp.int32, (width, width + LANES), 0)
    column = lax.broadcasted_iota(jnp.int32, (width, width + LANES), 1)
    one, zero = jnp.ones((), jnp.bfloat16), jnp.zeros((), jnp.bfloat16)
    upto = jnp.where((source <= column) | (column >= width), 1.0, 0.0).astype(jnp.bfloat16)
    tile_mark = tile_id.astype(jnp.float32).astype(jnp.bfloat16)
    spare_id = lax.broadcasted_iota(jnp.int32, (8, width), 0)
    nothing = jnp.zeros((8, width), jnp.float32)

    def as_bf16(x):
        return x.astype(jnp.float32).astype(jnp.bfloat16)

    def pick(mark, found, before):
        place = found[:, :width].astype(jnp.bfloat16) + jnp.concatenate([before] * (width // LANES), axis=1)
        place = jnp.where(mark, place, zero)
        while place.shape[0] > 16:
            half = place.shape[0] // 2
            place = place[:half, :] + place[half:, :]
        order = jnp.sum(place.astype(jnp.float32), axis=0, keepdims=True).astype(jnp.int32) - 1
        return order, before + found[:, width:].astype(jnp.bfloat16)

    def rank(g, befores):
        before, twin_before = befores
        marks, twin_marks, info = [], [], []
        for c in range(TOGETHER):
            i = g * TOGETHER + c
            here = pl.ds(pl.multiple_of(i * width, width), width)
            live = i * width + lane < count
            tile = jnp.where(live, tile_ref[:, here], tiles)
            match = tile_mark == as_bf16(tile)
            mark = jnp.where(match, one, zero)
            hits[:, here] = mark
            marks.append(mark)
            cell = cell_ref[:, here]
            along = cell & (COLS_DEV - 1)
            place = tile & (across - 1)
            west = live & (along == 0) & (place > 0)
            east = live & (along == COLS_DEV - 1) & (place < across - 1)
            twin = jnp.where(west, tile - 1, jnp.where(east, tile + 1, tiles))
            twin_match = tile_mark == as_bf16(twin)
            twin_mark = jnp.where(twin_match, one, zero)
            twins[:, here] = twin_mark
            twin_marks.append(twin_mark)
            code = jnp.where(west, ROWS_DEV, 0) + lax.shift_right_logical(cell, 8)
            info.append((tile, live, here, i, cell, code, match, twin_match))
        found = jnp.dot(jnp.concatenate(marks, axis=0), upto, preferred_element_type=jnp.float32)
        twin_found = jnp.dot(jnp.concatenate(twin_marks, axis=0), upto, preferred_element_type=jnp.float32)
        for c in range(TOGETHER):
            tile, live, here, i, cell, code, match, twin_match = info[c]
            level, before = pick(match, found[c * tiles : (c + 1) * tiles, :], before)
            slot = jnp.where(live, tile * LANES + level, tiles * LANES - 1)
            pos_f[pl.ds(pl.multiple_of(i * width, width), width)] = slot.reshape(width)
            at_level = tile_mark[:CAP, :] == as_bf16(level)
            coded[:CAP, here] = jnp.where(at_level, as_bf16(lax.shift_right_logical(cell, 6)), zero)
            coded[CAP:, here] = jnp.where(at_level, as_bf16(cell & 63), zero)
            order, twin_before = pick(twin_match, twin_found[c * tiles : (c + 1) * tiles, :], twin_before)
            at_order = spare_id == order
            point = i * width + lane
            high = jnp.where(at_order, (point & -LANES).astype(jnp.float32), nothing)
            low = jnp.where(at_order, (point & (LANES - 1)).astype(jnp.float32), nothing)
            value = jnp.where(at_order, code.astype(jnp.float32), nothing)
            twin_code[:16, here] = jnp.concatenate([high, low], axis=0).astype(jnp.bfloat16)
            twin_code[16:, here] = jnp.concatenate([value, nothing], axis=0).astype(jnp.bfloat16)
        return before, twin_before

    start = jnp.zeros((tiles, LANES), jnp.bfloat16)
    total, twin_total = lax.fori_loop(0, chunks // TOGETHER, rank, (start, start))
    total, twin_total = total.astype(jnp.float32), twin_total.astype(jnp.float32)
    to_smem = pltpu.make_async_copy(pos_f, pos_s, sem)
    to_smem.start()
    across_lanes = (((1,), (1,)), ((), ()))
    extra = lax.dot_general(twin_code[...], twins[...], across_lanes, preferred_element_type=jnp.float32)
    twin_f[...] = (extra[:8, :] + extra[8:16, :]).astype(jnp.int32).reshape(8 * tiles)
    twins_to_smem = pltpu.make_async_copy(twin_f, twin_s, twin_sem)
    twins_to_smem.start()
    spot = lax.broadcasted_iota(jnp.int32, (tiles, LANES), 1).astype(jnp.float32)
    blank = jnp.zeros((CAP, tiles), jnp.float32)
    codes = jnp.concatenate([blank, extra[16:, :], jnp.zeros((LANES - CAP - 16, tiles), jnp.float32)], axis=0).T
    rows[...] = feats_ref[...].astype(jnp.float32)
    cells = lax.dot_general(coded[...], hits[...], across_lanes, preferred_element_type=jnp.float32)
    filler = jnp.zeros((LANES - CAP, tiles), jnp.float32)
    to_smem.wait()

    def move(i, carry):
        for k in range(MOVES):
            slot = pos_s.at[pl.ds(k, points - MOVES + 1)][i * MOVES]
            slots[pl.ds(slot, 1), :] = rows[pl.ds(i * MOVES + k, 1), :]
        return carry

    lax.fori_loop(0, (count + (MOVES - 1)) // MOVES, move, 0)
    twins_to_smem.wait()

    def move_twins(t, carry):
        for u in range(8):
            for j in range(SPARE):
                point = twin_s.at[pl.ds(j * tiles + u, tiles - 7)][t * 8]
                slots[pl.ds(t * (8 * LANES) + u * LANES + CAP + 2 + j, 1), :] = rows[pl.ds(point, 1), :]
        return carry

    lax.fori_loop(0, tiles // 8, move_twins, 0)
    high = jnp.where(spot < total, jnp.concatenate([cells[:CAP, :], filler], axis=0).T, float(DUMP // 64))
    low = jnp.where(spot < total, jnp.concatenate([cells[CAP:, :], filler], axis=0).T, float(DUMP % 64))
    low = jnp.where((spot >= CAP) & (spot - CAP < jnp.minimum(twin_total, float(SPARE))), codes, low)
    full = jnp.max(twin_total, axis=0, keepdims=True) > SPARE
    high = jnp.where(spot == LANES - 1, 0.0, high)
    low = jnp.where(spot == LANES - 1, jnp.where(full, 1.0, 0.0), low)
    slots[pl.ds(CAP, tiles, LANES), :] = high
    slots[pl.ds(CAP + 1, tiles, LANES), :] = low

    def narrow(t, carry):
        out_ref[t] = slots[pl.ds(pl.multiple_of(t * LANES, LANES), BLOCK), :].astype(jnp.bfloat16)
        return carry

    lax.fori_loop(0, tiles, narrow, 0, unroll=4)


def add_kernel(
    got_ref, out_ref, top_ref, bottom_ref, sides_ref, full_ref,
    even, odd, coded, cells_f, cells_s, sem, *sums,
):
    sources = got_ref.shape[0]
    coded[...] = got_ref[:, CAP:, :].astype(jnp.float32).reshape(coded.shape)
    high = coded[pl.ds(0, sources, 8), :].astype(jnp.int32)
    low = coded[pl.ds(1, sources, 8), :].astype(jnp.int32)
    cells = high * 64 + low
    full_ref[0] = jnp.max(cells[:, LANES - 1 :])
    cells_f[...] = cells.reshape(sources * LANES)
    to_smem = pltpu.make_async_copy(cells_f, cells_s, sem)
    to_smem.start()

    def clear(i, carry):
        for part in sums:
            part[pl.ds(pl.multiple_of(i * 256, 256), 256), :] = jnp.zeros((256, LANES), jnp.float32)
        return carry

    lax.fori_loop(0, CELLS // 256, clear, 0)
    for part in sums:
        part[pl.ds(CELLS, HALO + 8), :] = jnp.zeros((HALO + 8, LANES), jnp.float32)

    def widen(s, rows):
        rows[...] = got_ref[jnp.minimum(s, sources - 1)].astype(jnp.float32)

    def add(s, rows):
        for j in range(CAP + SPARE):
            cell = pl.ds(cells_s.at[pl.ds(j, (sources - 1) * LANES + 1)][s * LANES], 1)
            part = sums[j % SUMS]
            k = j if j < CAP else j + 2
            part[cell, :] = part[cell, :] + rows[k : k + 1, :]

    def two(q, carry):
        widen(2 * q + 1, odd)
        add(2 * q, even)
        widen(2 * q + 2, even)
        add(2 * q + 1, odd)
        return carry

    to_smem.wait()
    widen(0, even)
    lax.fori_loop(0, sources // 2, two, 0)
    step = 256

    def close(i, carry):
        at = pl.ds(pl.multiple_of(i * step, step), step)
        total = sums[0][at, :]
        for part in sums[1:]:
            total = total + part[at, :]
        out_ref[at, :] = total.astype(jnp.bfloat16)
        return carry

    lax.fori_loop(0, CELLS // step, close, 0)

    def column(start, stride):
        at = pl.ds(start, ROWS_DEV, stride)
        total = sums[0][at, :]
        for part in sums[1:]:
            total = total + part[at, :]
        return total

    west, east = column(CELLS, 1), column(CELLS + ROWS_DEV, 1)
    sides_ref[:ROWS_DEV, :] = west.astype(jnp.bfloat16)
    sides_ref[ROWS_DEV:, :] = east.astype(jnp.bfloat16)
    spot = lax.broadcasted_iota(jnp.int32, (EDGE, LANES), 0)
    for ref, r in ((top_ref, 0), (bottom_ref, ROWS_DEV - 1)):
        ref[:COLS_DEV, :] = out_ref[r * COLS_DEV : (r + 1) * COLS_DEV, :]
        corners = jnp.where(spot == 0, west[r : r + 1, :], jnp.where(spot == 1, east[r : r + 1, :], 0.0))
        ref[COLS_DEV:, :] = corners.astype(jnp.bfloat16)


def fill_wide(weight_ref, wide):
    for i in range(4):
        for b in range(3):
            for o in range(2):
                block = (slice(i * LANES, (i + 1) * LANES), slice((2 * b + o) * LANES, (2 * b + o + 1) * LANES))
                wide[block] = weight_ref[i - o, b] if 0 <= i - o < 3 else jnp.zeros((LANES, LANES), jnp.bfloat16)


def conv_rows(row, pairs, west, east, bias, out_ref, wide, before, after):
    for k, p in enumerate(pairs):
        four = jnp.concatenate([row(2 * p - 1 + i) for i in range(4)], axis=1)
        taps = jnp.dot(four, wide[...], preferred_element_type=jnp.float32)
        before[7:8, :] = west[k : k + 1, :]
        before[8:, :] = taps[:, : 2 * LANES]
        after[:COLS_DEV, :] = taps[:, 4 * LANES :]
        after[COLS_DEV : COLS_DEV + 1, :] = east[k : k + 1, :]
        total = taps[:, 2 * LANES : 4 * LANES] + before[7 : 7 + COLS_DEV, :] + after[1 : 1 + COLS_DEV, :]
        done = jnp.maximum(total + jnp.concatenate([bias, bias], axis=1), 0.0).astype(jnp.bfloat16)
        out_ref[2 * k * COLS_DEV : (2 * k + 1) * COLS_DEV, :] = done[:, :LANES]
        out_ref[(2 * k + 1) * COLS_DEV : (2 * k + 2) * COLS_DEV, :] = done[:, LANES:]


def beside(corner, start, above, below, sides_ref, wide, side):
    side[:1, :] = above[corner : corner + 1, :]
    side[1 : ROWS_DEV + 1, :] = sides_ref[corner * ROWS_DEV : (corner + 1) * ROWS_DEV, :].astype(jnp.float32)
    side[ROWS_DEV + 1 : ROWS_DEV + 2, :] = below[corner : corner + 1, :]
    four = jnp.concatenate([side[pl.ds(i, ROWS_DEV // 2, 2), :] for i in range(4)], axis=1)
    return jnp.dot(four.astype(jnp.bfloat16), wide[:, start : start + 2 * LANES], preferred_element_type=jnp.float32)


def inner_kernel(bev_ref, sides_ref, weight_ref, bias_ref, out_hbm, out, wide, before, after, side, sem):
    fill_wide(weight_ref, wide)
    nothing = jnp.zeros((EDGE, LANES), jnp.float32)
    west = beside(0, 0, nothing, nothing, sides_ref, wide, side)
    east = beside(1, 4 * LANES, nothing, nothing, sides_ref, wide, side)

    def row(r):
        return bev_ref[r * COLS_DEV : (r + 1) * COLS_DEV, :]

    last = ROWS_DEV // 2 - 1
    conv_rows(row, range(1, last), west[1:last, :], east[1:last, :], bias_ref[...], out, wide, before, after)
    part = pl.ds(2 * COLS_DEV, (ROWS_DEV - 4) * COLS_DEV)
    store = pltpu.make_async_copy(out, out_hbm.at[part], sem)
    store.start()
    store.wait()


def outer_kernel(
    conv_ref, bev_ref, up_ref, down_ref, sides_ref, weight_ref, bias_ref,
    out_hbm, out, wide, before, after, side, sems,
):
    fill_wide(weight_ref, wide)
    above = up_ref[COLS_DEV:, :].astype(jnp.float32)
    below = down_ref[COLS_DEV:, :].astype(jnp.float32)
    west = beside(0, 0, above, below, sides_ref, wide, side)
    east = beside(1, 4 * LANES, above, below, sides_ref, wide, side)

    def row(r):
        if r < 0:
            return up_ref[:COLS_DEV, :]
        if r >= ROWS_DEV:
            return down_ref[:COLS_DEV, :]
        return bev_ref[r * COLS_DEV : (r + 1) * COLS_DEV, :]

    last = ROWS_DEV // 2 - 1
    ends = (0, last)
    pick = [jnp.concatenate([x[:1, :], x[last:, :]], axis=0) for x in (west, east)]
    conv_rows(row, ends, *pick, bias_ref[...], out, wide, before, after)
    size = 2 * COLS_DEV
    stores = [
        pltpu.make_async_copy(out.at[pl.ds(k * size, size)], out_hbm.at[pl.ds(p * size, size)], sems.at[k])
        for k, p in enumerate(ends)
    ]
    for store in stores:
        store.start()
    for store in stores:
        store.wait()


VMEM = pl.BlockSpec(memory_space=pltpu.VMEM)
SMEM = pl.BlockSpec(memory_space=pltpu.SMEM)
ANY = pl.BlockSpec(memory_space=pl.ANY)


def pack(point_feats, point_tile, point_cell, point_count, devices, across=8):
    points, channels = point_feats.shape
    if across & (across - 1):
        raise ValueError("across")
    bf16, f32, i32 = jnp.bfloat16, jnp.float32, jnp.int32
    return pl.pallas_call(
        functools.partial(pack_kernel, across),
        out_shape=jax.ShapeDtypeStruct((devices, BLOCK, channels), bf16),
        in_specs=[SMEM, VMEM, VMEM, VMEM],
        out_specs=VMEM,
        scratch_shapes=[
            pltpu.VMEM((points, channels), f32),
            pltpu.VMEM((devices * LANES, channels), f32),
            pltpu.VMEM((points,), i32),
            pltpu.SMEM((points,), i32),
            pltpu.VMEM((devices, points), bf16),
            pltpu.VMEM((2 * CAP, points), bf16),
            pltpu.VMEM((devices, points), bf16),
            pltpu.VMEM((32, points), bf16),
            pltpu.VMEM((devices * 8,), i32),
            pltpu.SMEM((devices * 8,), i32),
            pltpu.SemaphoreType.DMA,
            pltpu.SemaphoreType.DMA,
        ],
        compiler_params=pltpu.CompilerParams(vmem_limit_bytes=PACK_VMEM),
        name="pack",
    )(
        point_count,
        point_cell.reshape(1, points),
        point_tile.reshape(1, points),
        point_feats,
    )


def add_up(got):
    devices, block, channels = got.shape
    bf16, f32, i32 = jnp.bfloat16, jnp.float32, jnp.int32
    heights = (CELLS, COLS_DEV + EDGE, COLS_DEV + EDGE, HALO)
    return pl.pallas_call(
        add_kernel,
        out_shape=[jax.ShapeDtypeStruct((height, channels), bf16) for height in heights]
        + [jax.ShapeDtypeStruct((1,), i32)],
        in_specs=[VMEM],
        out_specs=[VMEM] * 4 + [SMEM],
        compiler_params=pltpu.CompilerParams(vmem_limit_bytes=ADD_VMEM),
        scratch_shapes=[
            pltpu.VMEM((block, channels), f32),
            pltpu.VMEM((block, channels), f32),
            pltpu.VMEM((devices * 8, channels), f32),
            pltpu.VMEM((devices * LANES,), i32),
            pltpu.SMEM((devices * LANES,), i32),
            pltpu.SemaphoreType.DMA,
        ]
        + [pltpu.VMEM((CELLS + HALO + 8, channels), f32)] * SUMS,
        name="add_up",
    )(got)


def shift(cells, axis, step):
    count = lax.axis_size(axis)
    pairs = [(i, i + step) for i in range(count) if 0 <= i + step < count]
    return lax.ppermute(cells, axis, pairs)


def conv_call(kernel, name, ins, rows, sems, aliases, flops, *operands):
    bev, channels = operands[-4 if len(ins) == 4 else 1], LANES
    bf16, f32 = jnp.bfloat16, jnp.float32
    return pl.pallas_call(
        kernel,
        out_shape=jax.ShapeDtypeStruct(bev.shape, bf16),
        in_specs=ins,
        out_specs=ANY,
        input_output_aliases=aliases,
        scratch_shapes=[
            pltpu.VMEM((rows * COLS_DEV, channels), bf16),
            pltpu.VMEM((4 * channels, 6 * channels), bf16),
            pltpu.VMEM((COLS_DEV + 8, 2 * channels), f32),
            pltpu.VMEM((COLS_DEV + 8, 2 * channels), f32),
            pltpu.VMEM((ROWS_DEV + 8, channels), f32),
            sems,
        ],
        compiler_params=pltpu.CompilerParams(vmem_limit_bytes=16 * 2**20),
        cost_estimate=pl.CostEstimate(flops=flops, bytes_accessed=2 * rows * COLS_DEV * channels, transcendentals=0),
        name=name,
    )(*operands)


def exchange_columns(bev, top, bottom, sides):
    cells = bev.reshape(ROWS_DEV, COLS_DEV, -1)
    west, east = shift(cells[:, -1], "gy", 1), shift(cells[:, 0], "gy", -1)
    rest = jnp.zeros((EDGE - 2, west.shape[1]), west.dtype)
    top = jnp.concatenate([top[:COLS_DEV], west[:1], east[:1], rest], axis=0)
    bottom = jnp.concatenate([bottom[:COLS_DEV], west[ROWS_DEV - 1 :], east[ROWS_DEV - 1 :], rest], axis=0)
    return top, bottom, jnp.concatenate([west, east], axis=0)


def keep_columns(bev, top, bottom, sides):
    return top, bottom, sides


def shards(point_feats, point_tile, point_cell, point_count, conv_weight, conv_bias):
    across = lax.axis_size("gy")
    devices = lax.axis_size("gx") * across
    channels = point_feats.shape[1]
    sent = pack(point_feats, point_tile, point_cell, point_count, devices, across)
    got = lax.all_to_all(sent, ("gx", "gy"), split_axis=0, concat_axis=0, tiled=True)
    bev, top, bottom, sides, full = add_up(got)
    top, bottom, sides = lax.switch(full[0], (keep_columns, exchange_columns), bev, top, bottom, sides)
    up = shift(bottom, "gx", 1)
    down = shift(top, "gx", -1)
    bias = conv_bias.reshape(1, channels)
    dma = pltpu.SemaphoreType.DMA
    work = 2 * CELLS * 9 * channels * channels
    inner = conv_call(
        inner_kernel, "inner", [VMEM] * 4, ROWS_DEV - 4, dma, {}, work, bev, sides, conv_weight, bias
    )
    conv_out = conv_call(
        outer_kernel, "outer", [ANY] + [VMEM] * 6, 4, dma((2,)), {0: 0}, work // 4,
        inner, bev, up, down, sides, conv_weight, bias,
    )
    whole = (ROWS_DEV, COLS_DEV, channels)
    return (bev.reshape(whole), conv_out.reshape(whole))


def solution(mesh):
    in_specs = (
        P(("gx", "gy"), None),
        P(("gx", "gy"), None),
        P(("gx", "gy")),
        P(("gx", "gy")),
        P(),
        P(),
    )
    out_specs = (P("gx", "gy", None), P("gx", "gy", None))
    return jax.shard_map(shards, mesh=mesh, in_specs=in_specs, out_specs=out_specs, check_vma=False)
```

```python
import functools

import jax
import jax.numpy as jnp
from jax import lax
from jax.experimental import pallas as pl
from jax.experimental.pallas import tpu as pltpu
from jax.sharding import PartitionSpec as P

COLS_DEV = 256
ROWS_DEV = 16
CELLS = ROWS_DEV * COLS_DEV
LANES = 128
CAP = 80
BLOCK = 88
SUMS = 8
SPARE = 6
HALO = 2 * ROWS_DEV
DUMP = CELLS + HALO
EDGE = 16
PACK_VMEM = 40 * 2**20
ADD_VMEM = 32 * 2**20
MOVES = 512
TOGETHER = 16


def place_kernel(
    across, count_ref, cell_ref, tile_ref, pos_f, twin_f, high_ref, low_ref, hits, coded, twins, twin_code,
):
    count = count_ref[0]
    width = 2 * LANES
    points = tile_ref.shape[1]
    chunks = points // width
    tiles = high_ref.shape[0]
    tile_id = lax.broadcasted_iota(jnp.int32, (tiles, width), 0)
    lane = lax.broadcasted_iota(jnp.int32, (1, width), 1)
    source = lax.broadcasted_iota(jnp.int32, (width, width + LANES), 0)
    column = lax.broadcasted_iota(jnp.int32, (width, width + LANES), 1)
    one, zero = jnp.ones((), jnp.bfloat16), jnp.zeros((), jnp.bfloat16)
    upto = jnp.where((source <= column) | (column >= width), 1.0, 0.0).astype(jnp.bfloat16)
    tile_mark = tile_id.astype(jnp.float32).astype(jnp.bfloat16)
    spare_id = lax.broadcasted_iota(jnp.int32, (8, width), 0)
    nothing = jnp.zeros((8, width), jnp.float32)

    def as_bf16(x):
        return x.astype(jnp.float32).astype(jnp.bfloat16)

    def pick(mark, found, before):
        place = found[:, :width].astype(jnp.bfloat16) + jnp.concatenate([before] * (width // LANES), axis=1)
        place = jnp.where(mark, place, zero)
        while place.shape[0] > 16:
            half = place.shape[0] // 2
            place = place[:half, :] + place[half:, :]
        order = jnp.sum(place.astype(jnp.float32), axis=0, keepdims=True).astype(jnp.int32) - 1
        return order, before + found[:, width:].astype(jnp.bfloat16)

    def rank(g, befores):
        before, twin_before = befores
        marks, twin_marks, info = [], [], []
        for c in range(TOGETHER):
            i = g * TOGETHER + c
            here = pl.ds(pl.multiple_of(i * width, width), width)
            live = i * width + lane < count
            tile = jnp.where(live, tile_ref[:, here], tiles)
            match = tile_mark == as_bf16(tile)
            mark = jnp.where(match, one, zero)
            hits[:, here] = mark
            marks.append(mark)
            cell = cell_ref[:, here]
            along = cell & (COLS_DEV - 1)
            place = tile & (across - 1)
            west = live & (along == 0) & (place > 0)
            east = live & (along == COLS_DEV - 1) & (place < across - 1)
            twin = jnp.where(west, tile - 1, jnp.where(east, tile + 1, tiles))
            twin_match = tile_mark == as_bf16(twin)
            twin_mark = jnp.where(twin_match, one, zero)
            twins[:, here] = twin_mark
            twin_marks.append(twin_mark)
            code = jnp.where(west, ROWS_DEV, 0) + lax.shift_right_logical(cell, 8)
            info.append((tile, live, here, i, cell, code, match, twin_match))
        found = jnp.dot(jnp.concatenate(marks, axis=0), upto, preferred_element_type=jnp.float32)
        twin_found = jnp.dot(jnp.concatenate(twin_marks, axis=0), upto, preferred_element_type=jnp.float32)
        for c in range(TOGETHER):
            tile, live, here, i, cell, code, match, twin_match = info[c]
            level, before = pick(match, found[c * tiles : (c + 1) * tiles, :], before)
            slot = jnp.where(live, tile * LANES + level, tiles * LANES - 1)
            pos_f[pl.ds(pl.multiple_of(i * width, width), width)] = slot.reshape(width)
            at_level = tile_mark[:CAP, :] == as_bf16(level)
            coded[:CAP, here] = jnp.where(at_level, as_bf16(lax.shift_right_logical(cell, 6)), zero)
            coded[CAP:, here] = jnp.where(at_level, as_bf16(cell & 63), zero)
            order, twin_before = pick(twin_match, twin_found[c * tiles : (c + 1) * tiles, :], twin_before)
            at_order = spare_id == order
            point = i * width + lane
            high = jnp.where(at_order, (point & -LANES).astype(jnp.float32), nothing)
            low = jnp.where(at_order, (point & (LANES - 1)).astype(jnp.float32), nothing)
            value = jnp.where(at_order, code.astype(jnp.float32), nothing)
            twin_code[:16, here] = jnp.concatenate([high, low], axis=0).astype(jnp.bfloat16)
            twin_code[16:, here] = jnp.concatenate([value, nothing], axis=0).astype(jnp.bfloat16)
        return before, twin_before

    start = jnp.zeros((tiles, LANES), jnp.bfloat16)
    total, twin_total = lax.fori_loop(0, chunks // TOGETHER, rank, (start, start))
    total, twin_total = total.astype(jnp.float32), twin_total.astype(jnp.float32)
    across_lanes = (((1,), (1,)), ((), ()))
    extra = lax.dot_general(twin_code[...], twins[...], across_lanes, preferred_element_type=jnp.float32)
    twin_f[...] = (extra[:8, :] + extra[8:16, :]).astype(jnp.int32).reshape(8 * tiles)
    spot = lax.broadcasted_iota(jnp.int32, (tiles, LANES), 1).astype(jnp.float32)
    blank = jnp.zeros((CAP, tiles), jnp.float32)
    codes = jnp.concatenate([blank, extra[16:, :], jnp.zeros((LANES - CAP - 16, tiles), jnp.float32)], axis=0).T
    cells = lax.dot_general(coded[...], hits[...], across_lanes, preferred_element_type=jnp.float32)
    filler = jnp.zeros((LANES - CAP, tiles), jnp.float32)
    high = jnp.where(spot < total, jnp.concatenate([cells[:CAP, :], filler], axis=0).T, float(DUMP // 64))
    low = jnp.where(spot < total, jnp.concatenate([cells[CAP:, :], filler], axis=0).T, float(DUMP % 64))
    low = jnp.where((spot >= CAP) & (spot - CAP < jnp.minimum(twin_total, float(SPARE))), codes, low)
    full = jnp.max(twin_total, axis=0, keepdims=True) > SPARE
    high = jnp.where(spot == LANES - 1, 0.0, high)
    low = jnp.where(spot == LANES - 1, jnp.where(full, 1.0, 0.0), low)
    high_ref[...] = high
    low_ref[...] = low


def pack_kernel(
    count_ref, pos_f, twin_f, high_ref, low_ref, feats_ref, out_ref, rows, slots, pos_s, twin_s, sem, twin_sem
):
    count = count_ref[0]
    points = feats_ref.shape[0]
    tiles = out_ref.shape[0]
    to_smem = pltpu.make_async_copy(pos_f, pos_s, sem)
    to_smem.start()
    twins_to_smem = pltpu.make_async_copy(twin_f, twin_s, twin_sem)
    twins_to_smem.start()
    rows[...] = feats_ref[...].astype(jnp.float32)
    to_smem.wait()

    def move(i, carry):
        for k in range(MOVES):
            slot = pos_s.at[pl.ds(k, points - MOVES + 1)][i * MOVES]
            slots[pl.ds(slot, 1), :] = rows[pl.ds(i * MOVES + k, 1), :]
        return carry

    lax.fori_loop(0, (count + (MOVES - 1)) // MOVES, move, 0)
    twins_to_smem.wait()

    def move_twins(t, carry):
        for u in range(8):
            for j in range(SPARE):
                point = twin_s.at[pl.ds(j * tiles + u, tiles - 7)][t * 8]
                slots[pl.ds(t * (8 * LANES) + u * LANES + CAP + 2 + j, 1), :] = rows[pl.ds(point, 1), :]
        return carry

    lax.fori_loop(0, tiles // 8, move_twins, 0)
    slots[pl.ds(CAP, tiles, LANES), :] = high_ref[...]
    slots[pl.ds(CAP + 1, tiles, LANES), :] = low_ref[...]

    def narrow(t, carry):
        out_ref[t] = slots[pl.ds(pl.multiple_of(t * LANES, LANES), BLOCK), :].astype(jnp.bfloat16)
        return carry

    lax.fori_loop(0, tiles, narrow, 0, unroll=4)


def add_kernel(
    got_ref, out_ref, top_ref, bottom_ref, sides_ref, full_ref,
    even, odd, coded, cells_f, cells_s, sem, *sums,
):
    sources = got_ref.shape[0]
    coded[...] = got_ref[:, CAP:, :].astype(jnp.float32).reshape(coded.shape)
    high = coded[pl.ds(0, sources, 8), :].astype(jnp.int32)
    low = coded[pl.ds(1, sources, 8), :].astype(jnp.int32)
    cells = high * 64 + low
    full_ref[0] = jnp.max(cells[:, LANES - 1 :])
    cells_f[...] = cells.reshape(sources * LANES)
    to_smem = pltpu.make_async_copy(cells_f, cells_s, sem)
    to_smem.start()

    def clear(i, carry):
        for part in sums:
            part[pl.ds(pl.multiple_of(i * 256, 256), 256), :] = jnp.zeros((256, LANES), jnp.float32)
        return carry

    lax.fori_loop(0, CELLS // 256, clear, 0)
    for part in sums:
        part[pl.ds(CELLS, HALO + 8), :] = jnp.zeros((HALO + 8, LANES), jnp.float32)

    def widen(s, rows):
        rows[...] = got_ref[jnp.minimum(s, sources - 1)].astype(jnp.float32)

    def add(s, rows):
        for j in range(CAP + SPARE):
            cell = pl.ds(cells_s.at[pl.ds(j, (sources - 1) * LANES + 1)][s * LANES], 1)
            part = sums[j % SUMS]
            k = j if j < CAP else j + 2
            part[cell, :] = part[cell, :] + rows[k : k + 1, :]

    def two(q, carry):
        widen(2 * q + 1, odd)
        add(2 * q, even)
        widen(2 * q + 2, even)
        add(2 * q + 1, odd)
        return carry

    to_smem.wait()
    widen(0, even)
    lax.fori_loop(0, sources // 2, two, 0)
    step = 256

    def close(i, carry):
        at = pl.ds(pl.multiple_of(i * step, step), step)
        total = sums[0][at, :]
        for part in sums[1:]:
            total = total + part[at, :]
        out_ref[at, :] = total.astype(jnp.bfloat16)
        return carry

    lax.fori_loop(0, CELLS // step, close, 0)

    def column(start, stride):
        at = pl.ds(start, ROWS_DEV, stride)
        total = sums[0][at, :]
        for part in sums[1:]:
            total = total + part[at, :]
        return total

    west, east = column(CELLS, 1), column(CELLS + ROWS_DEV, 1)
    sides_ref[:ROWS_DEV, :] = west.astype(jnp.bfloat16)
    sides_ref[ROWS_DEV:, :] = east.astype(jnp.bfloat16)
    spot = lax.broadcasted_iota(jnp.int32, (EDGE, LANES), 0)
    for ref, r in ((top_ref, 0), (bottom_ref, ROWS_DEV - 1)):
        ref[:COLS_DEV, :] = out_ref[r * COLS_DEV : (r + 1) * COLS_DEV, :]
        corners = jnp.where(spot == 0, west[r : r + 1, :], jnp.where(spot == 1, east[r : r + 1, :], 0.0))
        ref[COLS_DEV:, :] = corners.astype(jnp.bfloat16)


def fill_wide(weight_ref, wide):
    for i in range(4):
        for b in range(3):
            for o in range(2):
                block = (slice(i * LANES, (i + 1) * LANES), slice((2 * b + o) * LANES, (2 * b + o + 1) * LANES))
                wide[block] = weight_ref[i - o, b] if 0 <= i - o < 3 else jnp.zeros((LANES, LANES), jnp.bfloat16)


def conv_rows(row, pairs, west, east, bias, out_ref, wide, before, after):
    for k, p in enumerate(pairs):
        four = jnp.concatenate([row(2 * p - 1 + i) for i in range(4)], axis=1)
        taps = jnp.dot(four, wide[...], preferred_element_type=jnp.float32)
        before[7:8, :] = west[k : k + 1, :]
        before[8:, :] = taps[:, : 2 * LANES]
        after[:COLS_DEV, :] = taps[:, 4 * LANES :]
        after[COLS_DEV : COLS_DEV + 1, :] = east[k : k + 1, :]
        total = taps[:, 2 * LANES : 4 * LANES] + before[7 : 7 + COLS_DEV, :] + after[1 : 1 + COLS_DEV, :]
        done = jnp.maximum(total + jnp.concatenate([bias, bias], axis=1), 0.0).astype(jnp.bfloat16)
        out_ref[2 * k * COLS_DEV : (2 * k + 1) * COLS_DEV, :] = done[:, :LANES]
        out_ref[(2 * k + 1) * COLS_DEV : (2 * k + 2) * COLS_DEV, :] = done[:, LANES:]


def beside(corner, start, above, below, sides_ref, wide, side):
    side[:1, :] = above[corner : corner + 1, :]
    side[1 : ROWS_DEV + 1, :] = sides_ref[corner * ROWS_DEV : (corner + 1) * ROWS_DEV, :].astype(jnp.float32)
    side[ROWS_DEV + 1 : ROWS_DEV + 2, :] = below[corner : corner + 1, :]
    four = jnp.concatenate([side[pl.ds(i, ROWS_DEV // 2, 2), :] for i in range(4)], axis=1)
    return jnp.dot(four.astype(jnp.bfloat16), wide[:, start : start + 2 * LANES], preferred_element_type=jnp.float32)


def inner_kernel(bev_ref, sides_ref, weight_ref, bias_ref, out_hbm, out, wide, before, after, side, sem):
    fill_wide(weight_ref, wide)
    nothing = jnp.zeros((EDGE, LANES), jnp.float32)
    west = beside(0, 0, nothing, nothing, sides_ref, wide, side)
    east = beside(1, 4 * LANES, nothing, nothing, sides_ref, wide, side)

    def row(r):
        return bev_ref[r * COLS_DEV : (r + 1) * COLS_DEV, :]

    last = ROWS_DEV // 2 - 1
    conv_rows(row, range(1, last), west[1:last, :], east[1:last, :], bias_ref[...], out, wide, before, after)
    part = pl.ds(2 * COLS_DEV, (ROWS_DEV - 4) * COLS_DEV)
    store = pltpu.make_async_copy(out, out_hbm.at[part], sem)
    store.start()
    store.wait()


def outer_kernel(
    conv_ref, bev_ref, up_ref, down_ref, sides_ref, weight_ref, bias_ref,
    out_hbm, out, wide, before, after, side, sems,
):
    fill_wide(weight_ref, wide)
    above = up_ref[COLS_DEV:, :].astype(jnp.float32)
    below = down_ref[COLS_DEV:, :].astype(jnp.float32)
    west = beside(0, 0, above, below, sides_ref, wide, side)
    east = beside(1, 4 * LANES, above, below, sides_ref, wide, side)

    def row(r):
        if r < 0:
            return up_ref[:COLS_DEV, :]
        if r >= ROWS_DEV:
            return down_ref[:COLS_DEV, :]
        return bev_ref[r * COLS_DEV : (r + 1) * COLS_DEV, :]

    last = ROWS_DEV // 2 - 1
    ends = (0, last)
    pick = [jnp.concatenate([x[:1, :], x[last:, :]], axis=0) for x in (west, east)]
    conv_rows(row, ends, *pick, bias_ref[...], out, wide, before, after)
    size = 2 * COLS_DEV
    stores = [
        pltpu.make_async_copy(out.at[pl.ds(k * size, size)], out_hbm.at[pl.ds(p * size, size)], sems.at[k])
        for k, p in enumerate(ends)
    ]
    for store in stores:
        store.start()
    for store in stores:
        store.wait()


VMEM = pl.BlockSpec(memory_space=pltpu.VMEM)
SMEM = pl.BlockSpec(memory_space=pltpu.SMEM)
ANY = pl.BlockSpec(memory_space=pl.ANY)


def pack(point_feats, point_tile, point_cell, point_count, devices, across=8):
    points, channels = point_feats.shape
    if across & (across - 1):
        raise ValueError("across")
    bf16, f32, i32 = jnp.bfloat16, jnp.float32, jnp.int32
    params = pltpu.CompilerParams(vmem_limit_bytes=PACK_VMEM)
    placed = pl.pallas_call(
        functools.partial(place_kernel, across),
        out_shape=[
            jax.ShapeDtypeStruct((points,), i32),
            jax.ShapeDtypeStruct((devices * 8,), i32),
            jax.ShapeDtypeStruct((devices, LANES), f32),
            jax.ShapeDtypeStruct((devices, LANES), f32),
        ],
        in_specs=[SMEM, VMEM, VMEM],
        out_specs=[VMEM] * 4,
        scratch_shapes=[
            pltpu.VMEM((devices, points), bf16),
            pltpu.VMEM((2 * CAP, points), bf16),
            pltpu.VMEM((devices, points), bf16),
            pltpu.VMEM((32, points), bf16),
        ],
        compiler_params=params,
        cost_estimate=pl.CostEstimate(flops=2 * points * devices * 1024, bytes_accessed=8 * points, transcendentals=0),
        name="place",
    )(point_count, point_cell.reshape(1, points), point_tile.reshape(1, points))
    return pl.pallas_call(
        pack_kernel,
        out_shape=jax.ShapeDtypeStruct((devices, BLOCK, channels), bf16),
        in_specs=[SMEM] + [VMEM] * 5,
        out_specs=VMEM,
        scratch_shapes=[
            pltpu.VMEM((points, channels), f32),
            pltpu.VMEM((devices * LANES, channels), f32),
            pltpu.SMEM((points,), i32),
            pltpu.SMEM((devices * 8,), i32),
            pltpu.SemaphoreType.DMA,
            pltpu.SemaphoreType.DMA,
        ],
        compiler_params=params,
        name="pack",
    )(point_count, *placed, point_feats)


def add_up(got):
    devices, block, channels = got.shape
    bf16, f32, i32 = jnp.bfloat16, jnp.float32, jnp.int32
    heights = (CELLS, COLS_DEV + EDGE, COLS_DEV + EDGE, HALO)
    return pl.pallas_call(
        add_kernel,
        out_shape=[jax.ShapeDtypeStruct((height, channels), bf16) for height in heights]
        + [jax.ShapeDtypeStruct((1,), i32)],
        in_specs=[VMEM],
        out_specs=[VMEM] * 4 + [SMEM],
        compiler_params=pltpu.CompilerParams(vmem_limit_bytes=ADD_VMEM),
        scratch_shapes=[
            pltpu.VMEM((block, channels), f32),
            pltpu.VMEM((block, channels), f32),
            pltpu.VMEM((devices * 8, channels), f32),
            pltpu.VMEM((devices * LANES,), i32),
            pltpu.SMEM((devices * LANES,), i32),
            pltpu.SemaphoreType.DMA,
        ]
        + [pltpu.VMEM((CELLS + HALO + 8, channels), f32)] * SUMS,
        name="add_up",
    )(got)


def shift(cells, axis, step):
    count = lax.axis_size(axis)
    pairs = [(i, i + step) for i in range(count) if 0 <= i + step < count]
    return lax.ppermute(cells, axis, pairs)


def conv_call(kernel, name, ins, rows, sems, aliases, flops, *operands):
    bev, channels = operands[-4 if len(ins) == 4 else 1], LANES
    bf16, f32 = jnp.bfloat16, jnp.float32
    return pl.pallas_call(
        kernel,
        out_shape=jax.ShapeDtypeStruct(bev.shape, bf16),
        in_specs=ins,
        out_specs=ANY,
        input_output_aliases=aliases,
        scratch_shapes=[
            pltpu.VMEM((rows * COLS_DEV, channels), bf16),
            pltpu.VMEM((4 * channels, 6 * channels), bf16),
            pltpu.VMEM((COLS_DEV + 8, 2 * channels), f32),
            pltpu.VMEM((COLS_DEV + 8, 2 * channels), f32),
            pltpu.VMEM((ROWS_DEV + 8, channels), f32),
            sems,
        ],
        compiler_params=pltpu.CompilerParams(vmem_limit_bytes=16 * 2**20),
        cost_estimate=pl.CostEstimate(flops=flops, bytes_accessed=2 * rows * COLS_DEV * channels, transcendentals=0),
        name=name,
    )(*operands)


def exchange_columns(bev, top, bottom, sides):
    cells = bev.reshape(ROWS_DEV, COLS_DEV, -1)
    west, east = shift(cells[:, -1], "gy", 1), shift(cells[:, 0], "gy", -1)
    rest = jnp.zeros((EDGE - 2, west.shape[1]), west.dtype)
    top = jnp.concatenate([top[:COLS_DEV], west[:1], east[:1], rest], axis=0)
    bottom = jnp.concatenate([bottom[:COLS_DEV], west[ROWS_DEV - 1 :], east[ROWS_DEV - 1 :], rest], axis=0)
    return top, bottom, jnp.concatenate([west, east], axis=0)


def keep_columns(bev, top, bottom, sides):
    return top, bottom, sides


def shards(point_feats, point_tile, point_cell, point_count, conv_weight, conv_bias):
    across = lax.axis_size("gy")
    devices = lax.axis_size("gx") * across
    channels = point_feats.shape[1]
    sent = pack(point_feats, point_tile, point_cell, point_count, devices, across)
    got = lax.all_to_all(sent, ("gx", "gy"), split_axis=0, concat_axis=0, tiled=True)
    bev, top, bottom, sides, full = add_up(got)
    top, bottom, sides = lax.switch(full[0], (keep_columns, exchange_columns), bev, top, bottom, sides)
    up = shift(bottom, "gx", 1)
    down = shift(top, "gx", -1)
    bias = conv_bias.reshape(1, channels)
    dma = pltpu.SemaphoreType.DMA
    work = 2 * CELLS * 9 * channels * channels
    inner = conv_call(
        inner_kernel, "inner", [VMEM] * 4, ROWS_DEV - 4, dma, {}, work, bev, sides, conv_weight, bias
    )
    conv_out = conv_call(
        outer_kernel, "outer", [ANY] + [VMEM] * 6, 4, dma((2,)), {0: 0}, work // 4,
        inner, bev, up, down, sides, conv_weight, bias,
    )
    whole = (ROWS_DEV, COLS_DEV, channels)
    return (bev.reshape(whole), conv_out.reshape(whole))


def solution(mesh):
    in_specs = (
        P(("gx", "gy"), None),
        P(("gx", "gy"), None),
        P(("gx", "gy")),
        P(("gx", "gy")),
        P(),
        P(),
    )
    out_specs = (P("gx", "gy", None), P("gx", "gy", None))
    return jax.shard_map(shards, mesh=mesh, in_specs=in_specs, out_specs=out_specs, check_vma=False)
```

```python
import functools

import jax
import jax.numpy as jnp
from jax import lax
from jax.experimental import pallas as pl
from jax.experimental.pallas import tpu as pltpu
from jax.sharding import PartitionSpec as P

COLS_DEV = 256
ROWS_DEV = 16
CELLS = ROWS_DEV * COLS_DEV
LANES = 128
CAP = 80
BLOCK = 88
SUMS = 8
SPARE = 6
HALO = 2 * ROWS_DEV
DUMP = CELLS + HALO
EDGE = 16
PACK_VMEM = 40 * 2**20
ADD_VMEM = 32 * 2**20
MOVES = 512
TOGETHER = 16


def place_kernel(
    across, count_ref, cell_ref, tile_ref, pos_f, twin_f, high_ref, low_ref, hits, coded, twins, twin_code,
):
    count = count_ref[0]
    width = 2 * LANES
    points = tile_ref.shape[1]
    chunks = points // width
    tiles = high_ref.shape[0]
    tile_id = lax.broadcasted_iota(jnp.int32, (tiles, width), 0)
    lane = lax.broadcasted_iota(jnp.int32, (1, width), 1)
    source = lax.broadcasted_iota(jnp.int32, (width, width + LANES), 0)
    column = lax.broadcasted_iota(jnp.int32, (width, width + LANES), 1)
    one, zero = jnp.ones((), jnp.bfloat16), jnp.zeros((), jnp.bfloat16)
    upto = jnp.where((source <= column) | (column >= width), 1.0, 0.0).astype(jnp.bfloat16)
    tile_mark = tile_id.astype(jnp.float32).astype(jnp.bfloat16)
    spare_id = lax.broadcasted_iota(jnp.int32, (8, width), 0)
    nothing = jnp.zeros((8, width), jnp.float32)

    def as_bf16(x):
        return x.astype(jnp.float32).astype(jnp.bfloat16)

    def pick(mark, found, before):
        place = found[:, :width].astype(jnp.bfloat16) + jnp.concatenate([before] * (width // LANES), axis=1)
        place = jnp.where(mark, place, zero)
        while place.shape[0] > 16:
            half = place.shape[0] // 2
            place = place[:half, :] + place[half:, :]
        order = jnp.sum(place.astype(jnp.float32), axis=0, keepdims=True).astype(jnp.int32) - 1
        return order, before + found[:, width:].astype(jnp.bfloat16)

    def rank(g, befores):
        before, twin_before = befores
        marks, twin_marks, info = [], [], []
        for c in range(TOGETHER):
            i = g * TOGETHER + c
            here = pl.ds(pl.multiple_of(i * width, width), width)
            live = i * width + lane < count
            tile = jnp.where(live, tile_ref[:, here], tiles)
            match = tile_mark == as_bf16(tile)
            mark = jnp.where(match, one, zero)
            hits[:, here] = mark
            marks.append(mark)
            cell = cell_ref[:, here]
            along = cell & (COLS_DEV - 1)
            place = tile & (across - 1)
            west = live & (along == 0) & (place > 0)
            east = live & (along == COLS_DEV - 1) & (place < across - 1)
            twin = jnp.where(west, tile - 1, jnp.where(east, tile + 1, tiles))
            twin_match = tile_mark == as_bf16(twin)
            twin_mark = jnp.where(twin_match, one, zero)
            twins[:, here] = twin_mark
            twin_marks.append(twin_mark)
            code = jnp.where(west, ROWS_DEV, 0) + lax.shift_right_logical(cell, 8)
            info.append((tile, live, here, i, cell, code, match, twin_match))
        found = jnp.dot(jnp.concatenate(marks, axis=0), upto, preferred_element_type=jnp.float32)
        twin_found = jnp.dot(jnp.concatenate(twin_marks, axis=0), upto, preferred_element_type=jnp.float32)
        for c in range(TOGETHER):
            tile, live, here, i, cell, code, match, twin_match = info[c]
            level, before = pick(match, found[c * tiles : (c + 1) * tiles, :], before)
            slot = jnp.where(live, tile * LANES + level, tiles * LANES - 1)
            pos_f[pl.ds(pl.multiple_of(i * width, width), width)] = slot.reshape(width)
            at_level = tile_mark[:CAP, :] == as_bf16(level)
            coded[:CAP, here] = jnp.where(at_level, as_bf16(lax.shift_right_logical(cell, 6)), zero)
            coded[CAP:, here] = jnp.where(at_level, as_bf16(cell & 63), zero)
            order, twin_before = pick(twin_match, twin_found[c * tiles : (c + 1) * tiles, :], twin_before)
            at_order = spare_id == order
            point = i * width + lane
            high = jnp.where(at_order, (point & -LANES).astype(jnp.float32), nothing)
            low = jnp.where(at_order, (point & (LANES - 1)).astype(jnp.float32), nothing)
            value = jnp.where(at_order, code.astype(jnp.float32), nothing)
            twin_code[:16, here] = jnp.concatenate([high, low], axis=0).astype(jnp.bfloat16)
            twin_code[16:, here] = jnp.concatenate([value, nothing], axis=0).astype(jnp.bfloat16)
        return before, twin_before

    start = jnp.zeros((tiles, LANES), jnp.bfloat16)
    total, twin_total = lax.fori_loop(0, chunks // TOGETHER, rank, (start, start))
    total, twin_total = total.astype(jnp.float32), twin_total.astype(jnp.float32)
    across_lanes = (((1,), (1,)), ((), ()))
    extra = lax.dot_general(twin_code[...], twins[...], across_lanes, preferred_element_type=jnp.float32)
    twin_f[...] = (extra[:8, :] + extra[8:16, :]).astype(jnp.int32).reshape(8 * tiles)
    spot = lax.broadcasted_iota(jnp.int32, (tiles, LANES), 1).astype(jnp.float32)
    blank = jnp.zeros((CAP, tiles), jnp.float32)
    codes = jnp.concatenate([blank, extra[16:, :], jnp.zeros((LANES - CAP - 16, tiles), jnp.float32)], axis=0).T
    cells = lax.dot_general(coded[...], hits[...], across_lanes, preferred_element_type=jnp.float32)
    filler = jnp.zeros((LANES - CAP, tiles), jnp.float32)
    high = jnp.where(spot < total, jnp.concatenate([cells[:CAP, :], filler], axis=0).T, float(DUMP // 64))
    low = jnp.where(spot < total, jnp.concatenate([cells[CAP:, :], filler], axis=0).T, float(DUMP % 64))
    low = jnp.where((spot >= CAP) & (spot - CAP < jnp.minimum(twin_total, float(SPARE))), codes, low)
    full = jnp.max(twin_total, axis=0, keepdims=True) > SPARE
    high = jnp.where(spot == LANES - 1, 0.0, high)
    low = jnp.where(spot == LANES - 1, jnp.where(full, 1.0, 0.0), low)
    high_ref[...] = high
    low_ref[...] = low


def pack_kernel(
    count_ref, pos_f, twin_f, high_ref, low_ref, feats_ref, out_ref, rows, slots, pos_s, twin_s, sem, twin_sem
):
    count = count_ref[0]
    points = feats_ref.shape[0]
    tiles = out_ref.shape[0]
    to_smem = pltpu.make_async_copy(pos_f, pos_s, sem)
    to_smem.start()
    twins_to_smem = pltpu.make_async_copy(twin_f, twin_s, twin_sem)
    twins_to_smem.start()
    rows[...] = feats_ref[...].astype(jnp.float32)
    to_smem.wait()

    def move(i, carry):
        for k in range(MOVES):
            slot = pos_s.at[pl.ds(k, points - MOVES + 1)][i * MOVES]
            slots[pl.ds(slot, 1), :] = rows[pl.ds(i * MOVES + k, 1), :]
        return carry

    lax.fori_loop(0, (count + (MOVES - 1)) // MOVES, move, 0)
    twins_to_smem.wait()

    def move_twins(t, carry):
        for u in range(8):
            for j in range(SPARE):
                point = twin_s.at[pl.ds(j * tiles + u, tiles - 7)][t * 8]
                slots[pl.ds(t * (8 * LANES) + u * LANES + CAP + 2 + j, 1), :] = rows[pl.ds(point, 1), :]
        return carry

    lax.fori_loop(0, tiles // 8, move_twins, 0)
    slots[pl.ds(CAP, tiles, LANES), :] = high_ref[...]
    slots[pl.ds(CAP + 1, tiles, LANES), :] = low_ref[...]

    def narrow(t, carry):
        out_ref[t] = slots[pl.ds(pl.multiple_of(t * LANES, LANES), BLOCK), :].astype(jnp.bfloat16)
        return carry

    lax.fori_loop(0, tiles, narrow, 0, unroll=4)


def add_kernel(
    got_ref, out_ref, top_ref, bottom_ref, sides_ref, full_ref,
    even, odd, coded, cells_f, cells_s, sem, *sums,
):
    sources = got_ref.shape[0]
    coded[...] = got_ref[:, CAP:, :].astype(jnp.float32).reshape(coded.shape)
    high = coded[pl.ds(0, sources, 8), :].astype(jnp.int32)
    low = coded[pl.ds(1, sources, 8), :].astype(jnp.int32)
    cells = high * 64 + low
    full_ref[0] = jnp.max(cells[:, LANES - 1 :])
    cells_f[...] = cells.reshape(sources * LANES)
    to_smem = pltpu.make_async_copy(cells_f, cells_s, sem)
    to_smem.start()

    def clear(i, carry):
        for part in sums:
            part[pl.ds(pl.multiple_of(i * 256, 256), 256), :] = jnp.zeros((256, LANES), jnp.float32)
        return carry

    lax.fori_loop(0, CELLS // 256, clear, 0)
    for part in sums:
        part[pl.ds(CELLS, HALO + 8), :] = jnp.zeros((HALO + 8, LANES), jnp.float32)

    def widen(s, rows):
        rows[...] = got_ref[jnp.minimum(s, sources - 1)].astype(jnp.float32)

    def add(s, rows):
        for j in range(CAP + SPARE):
            cell = pl.ds(cells_s.at[pl.ds(j, (sources - 1) * LANES + 1)][s * LANES], 1)
            part = sums[j % SUMS]
            k = j if j < CAP else j + 2
            part[cell, :] = part[cell, :] + rows[k : k + 1, :]

    def two(q, carry):
        widen(2 * q + 1, odd)
        add(2 * q, even)
        widen(2 * q + 2, even)
        add(2 * q + 1, odd)
        return carry

    to_smem.wait()
    widen(0, even)
    lax.fori_loop(0, sources // 2, two, 0)
    step = 256

    def close(i, carry):
        at = pl.ds(pl.multiple_of(i * step, step), step)
        total = sums[0][at, :]
        for part in sums[1:]:
            total = total + part[at, :]
        out_ref[at, :] = total.astype(jnp.bfloat16)
        return carry

    lax.fori_loop(0, CELLS // step, close, 0)

    def column(start, stride):
        at = pl.ds(start, ROWS_DEV, stride)
        total = sums[0][at, :]
        for part in sums[1:]:
            total = total + part[at, :]
        return total

    west, east = column(CELLS, 1), column(CELLS + ROWS_DEV, 1)
    sides_ref[:ROWS_DEV, :] = west.astype(jnp.bfloat16)
    sides_ref[ROWS_DEV:, :] = east.astype(jnp.bfloat16)
    spot = lax.broadcasted_iota(jnp.int32, (EDGE, LANES), 0)
    for ref, r in ((top_ref, 0), (bottom_ref, ROWS_DEV - 1)):
        ref[:COLS_DEV, :] = out_ref[r * COLS_DEV : (r + 1) * COLS_DEV, :]
        corners = jnp.where(spot == 0, west[r : r + 1, :], jnp.where(spot == 1, east[r : r + 1, :], 0.0))
        ref[COLS_DEV:, :] = corners.astype(jnp.bfloat16)


def fill_wide(weight_ref, wide):
    for i in range(4):
        for b in range(3):
            for o in range(2):
                block = (slice(i * LANES, (i + 1) * LANES), slice((2 * b + o) * LANES, (2 * b + o + 1) * LANES))
                wide[block] = weight_ref[i - o, b] if 0 <= i - o < 3 else jnp.zeros((LANES, LANES), jnp.bfloat16)


def conv_rows(row, pairs, west, east, bias, out_ref, wide, before, after):
    for k, p in enumerate(pairs):
        four = jnp.concatenate([row(2 * p - 1 + i) for i in range(4)], axis=1)
        taps = jnp.dot(four, wide[...], preferred_element_type=jnp.float32)
        before[7:8, :] = west[k : k + 1, :]
        before[8:, :] = taps[:, : 2 * LANES]
        after[:COLS_DEV, :] = taps[:, 4 * LANES :]
        after[COLS_DEV : COLS_DEV + 1, :] = east[k : k + 1, :]
        total = taps[:, 2 * LANES : 4 * LANES] + before[7 : 7 + COLS_DEV, :] + after[1 : 1 + COLS_DEV, :]
        done = jnp.maximum(total + jnp.concatenate([bias, bias], axis=1), 0.0).astype(jnp.bfloat16)
        out_ref[2 * k * COLS_DEV : (2 * k + 1) * COLS_DEV, :] = done[:, :LANES]
        out_ref[(2 * k + 1) * COLS_DEV : (2 * k + 2) * COLS_DEV, :] = done[:, LANES:]


def beside(corner, start, above, below, sides_ref, wide, side):
    side[:1, :] = above[corner : corner + 1, :]
    side[1 : ROWS_DEV + 1, :] = sides_ref[corner * ROWS_DEV : (corner + 1) * ROWS_DEV, :].astype(jnp.float32)
    side[ROWS_DEV + 1 : ROWS_DEV + 2, :] = below[corner : corner + 1, :]
    four = jnp.concatenate([side[pl.ds(i, ROWS_DEV // 2, 2), :] for i in range(4)], axis=1)
    return jnp.dot(four.astype(jnp.bfloat16), wide[:, start : start + 2 * LANES], preferred_element_type=jnp.float32)


def inner_kernel(bev_ref, sides_ref, weight_ref, bias_ref, out_hbm, wide, out, before, after, side, sem):
    fill_wide(weight_ref, wide)
    nothing = jnp.zeros((EDGE, LANES), jnp.float32)
    west = beside(0, 0, nothing, nothing, sides_ref, wide, side)
    east = beside(1, 4 * LANES, nothing, nothing, sides_ref, wide, side)

    def row(r):
        return bev_ref[r * COLS_DEV : (r + 1) * COLS_DEV, :]

    last = ROWS_DEV // 2 - 1
    conv_rows(row, range(1, last), west[1:last, :], east[1:last, :], bias_ref[...], out, wide, before, after)
    part = pl.ds(2 * COLS_DEV, (ROWS_DEV - 4) * COLS_DEV)
    store = pltpu.make_async_copy(out, out_hbm.at[part], sem)
    store.start()
    store.wait()


def outer_kernel(
    conv_ref, bev_ref, up_ref, down_ref, sides_ref, wide, bias_ref,
    out_hbm, out, before, after, side, sems,
):
    above = up_ref[COLS_DEV:, :].astype(jnp.float32)
    below = down_ref[COLS_DEV:, :].astype(jnp.float32)
    west = beside(0, 0, above, below, sides_ref, wide, side)
    east = beside(1, 4 * LANES, above, below, sides_ref, wide, side)

    def row(r):
        if r < 0:
            return up_ref[:COLS_DEV, :]
        if r >= ROWS_DEV:
            return down_ref[:COLS_DEV, :]
        return bev_ref[r * COLS_DEV : (r + 1) * COLS_DEV, :]

    last = ROWS_DEV // 2 - 1
    ends = (0, last)
    pick = [jnp.concatenate([x[:1, :], x[last:, :]], axis=0) for x in (west, east)]
    conv_rows(row, ends, *pick, bias_ref[...], out, wide, before, after)
    size = 2 * COLS_DEV
    stores = [
        pltpu.make_async_copy(out.at[pl.ds(k * size, size)], out_hbm.at[pl.ds(p * size, size)], sems.at[k])
        for k, p in enumerate(ends)
    ]
    for store in stores:
        store.start()
    for store in stores:
        store.wait()


VMEM = pl.BlockSpec(memory_space=pltpu.VMEM)
SMEM = pl.BlockSpec(memory_space=pltpu.SMEM)
ANY = pl.BlockSpec(memory_space=pl.ANY)


def pack(point_feats, point_tile, point_cell, point_count, devices, across=8):
    points, channels = point_feats.shape
    if across & (across - 1):
        raise ValueError("across")
    bf16, f32, i32 = jnp.bfloat16, jnp.float32, jnp.int32
    params = pltpu.CompilerParams(vmem_limit_bytes=PACK_VMEM)
    placed = pl.pallas_call(
        functools.partial(place_kernel, across),
        out_shape=[
            jax.ShapeDtypeStruct((points,), i32),
            jax.ShapeDtypeStruct((devices * 8,), i32),
            jax.ShapeDtypeStruct((devices, LANES), f32),
            jax.ShapeDtypeStruct((devices, LANES), f32),
        ],
        in_specs=[SMEM, VMEM, VMEM],
        out_specs=[VMEM] * 4,
        scratch_shapes=[
            pltpu.VMEM((devices, points), bf16),
            pltpu.VMEM((2 * CAP, points), bf16),
            pltpu.VMEM((devices, points), bf16),
            pltpu.VMEM((32, points), bf16),
        ],
        compiler_params=params,
        cost_estimate=pl.CostEstimate(flops=2 * points * devices * 1024, bytes_accessed=8 * points, transcendentals=0),
        name="place",
    )(point_count, point_cell.reshape(1, points), point_tile.reshape(1, points))
    return pl.pallas_call(
        pack_kernel,
        out_shape=jax.ShapeDtypeStruct((devices, BLOCK, channels), bf16),
        in_specs=[SMEM] + [VMEM] * 5,
        out_specs=VMEM,
        scratch_shapes=[
            pltpu.VMEM((points, channels), f32),
            pltpu.VMEM((devices * LANES, channels), f32),
            pltpu.SMEM((points,), i32),
            pltpu.SMEM((devices * 8,), i32),
            pltpu.SemaphoreType.DMA,
            pltpu.SemaphoreType.DMA,
        ],
        compiler_params=params,
        name="pack",
    )(point_count, *placed, point_feats)


def add_up(got):
    devices, block, channels = got.shape
    bf16, f32, i32 = jnp.bfloat16, jnp.float32, jnp.int32
    heights = (CELLS, COLS_DEV + EDGE, COLS_DEV + EDGE, HALO)
    return pl.pallas_call(
        add_kernel,
        out_shape=[jax.ShapeDtypeStruct((height, channels), bf16) for height in heights]
        + [jax.ShapeDtypeStruct((1,), i32)],
        in_specs=[VMEM],
        out_specs=[VMEM] * 4 + [SMEM],
        compiler_params=pltpu.CompilerParams(vmem_limit_bytes=ADD_VMEM),
        scratch_shapes=[
            pltpu.VMEM((block, channels), f32),
            pltpu.VMEM((block, channels), f32),
            pltpu.VMEM((devices * 8, channels), f32),
            pltpu.VMEM((devices * LANES,), i32),
            pltpu.SMEM((devices * LANES,), i32),
            pltpu.SemaphoreType.DMA,
        ]
        + [pltpu.VMEM((CELLS + HALO + 8, channels), f32)] * SUMS,
        name="add_up",
    )(got)


def shift(cells, axis, step):
    count = lax.axis_size(axis)
    pairs = [(i, i + step) for i in range(count) if 0 <= i + step < count]
    return lax.ppermute(cells, axis, pairs)


def conv_call(kernel, name, ins, rows, sems, aliases, flops, extra, *operands):
    bev, channels = operands[-4 if len(ins) == 4 else 1], LANES
    bf16, f32 = jnp.bfloat16, jnp.float32
    return pl.pallas_call(
        kernel,
        out_shape=[jax.ShapeDtypeStruct(bev.shape, bf16)] + extra,
        in_specs=ins,
        out_specs=[ANY] + [VMEM] * len(extra),
        input_output_aliases=aliases,
        scratch_shapes=[
            pltpu.VMEM((rows * COLS_DEV, channels), bf16),
            pltpu.VMEM((COLS_DEV + 8, 2 * channels), f32),
            pltpu.VMEM((COLS_DEV + 8, 2 * channels), f32),
            pltpu.VMEM((ROWS_DEV + 8, channels), f32),
            sems,
        ],
        compiler_params=pltpu.CompilerParams(vmem_limit_bytes=16 * 2**20),
        cost_estimate=pl.CostEstimate(flops=flops, bytes_accessed=2 * rows * COLS_DEV * channels, transcendentals=0),
        name=name,
    )(*operands)


def exchange_columns(bev, top, bottom, sides):
    cells = bev.reshape(ROWS_DEV, COLS_DEV, -1)
    west, east = shift(cells[:, -1], "gy", 1), shift(cells[:, 0], "gy", -1)
    rest = jnp.zeros((EDGE - 2, west.shape[1]), west.dtype)
    top = jnp.concatenate([top[:COLS_DEV], west[:1], east[:1], rest], axis=0)
    bottom = jnp.concatenate([bottom[:COLS_DEV], west[ROWS_DEV - 1 :], east[ROWS_DEV - 1 :], rest], axis=0)
    return top, bottom, jnp.concatenate([west, east], axis=0)


def keep_columns(bev, top, bottom, sides):
    return top, bottom, sides


def shards(point_feats, point_tile, point_cell, point_count, conv_weight, conv_bias):
    across = lax.axis_size("gy")
    devices = lax.axis_size("gx") * across
    channels = point_feats.shape[1]
    sent = pack(point_feats, point_tile, point_cell, point_count, devices, across)
    got = lax.all_to_all(sent, ("gx", "gy"), split_axis=0, concat_axis=0, tiled=True)
    bev, top, bottom, sides, full = add_up(got)
    top, bottom, sides = lax.switch(full[0], (keep_columns, exchange_columns), bev, top, bottom, sides)
    up = shift(bottom, "gx", 1)
    down = shift(top, "gx", -1)
    bias = conv_bias.reshape(1, channels)
    dma = pltpu.SemaphoreType.DMA
    work = 2 * CELLS * 9 * channels * channels
    inner, wide = conv_call(
        inner_kernel, "inner", [VMEM] * 4, ROWS_DEV - 4, dma, {}, work,
        [jax.ShapeDtypeStruct((4 * channels, 6 * channels), jnp.bfloat16)], bev, sides, conv_weight, bias
    )
    (conv_out,) = conv_call(
        outer_kernel, "outer", [ANY] + [VMEM] * 6, 4, dma((2,)), {0: 0}, work // 4, [],
        inner, bev, up, down, sides, wide, bias,
    )
    whole = (ROWS_DEV, COLS_DEV, channels)
    return (bev.reshape(whole), conv_out.reshape(whole))


def solution(mesh):
    in_specs = (
        P(("gx", "gy"), None),
        P(("gx", "gy"), None),
        P(("gx", "gy")),
        P(("gx", "gy")),
        P(),
        P(),
    )
    out_specs = (P("gx", "gy", None), P("gx", "gy", None))
    return jax.shard_map(shards, mesh=mesh, in_specs=in_specs, out_specs=out_specs, check_vma=False)
```

```python
import functools

import jax
import jax.numpy as jnp
from jax import lax
from jax.experimental import pallas as pl
from jax.experimental.pallas import tpu as pltpu
from jax.sharding import PartitionSpec as P

COLS_DEV = 256
ROWS_DEV = 16
CELLS = ROWS_DEV * COLS_DEV
LANES = 128
CAP = 80
BLOCK = 88
SUMS = 8
SPARE = 6
HALO = 2 * ROWS_DEV
DUMP = CELLS + HALO
EDGE = 16
PACK_VMEM = 40 * 2**20
ADD_VMEM = 32 * 2**20
MOVES = 512
TOGETHER = 32


def place_kernel(
    across, count_ref, cell_ref, tile_ref, pos_f, twin_f, high_ref, low_ref, hits, coded, twins, twin_code,
):
    count = count_ref[0]
    width = 2 * LANES
    points = tile_ref.shape[1]
    chunks = points // width
    tiles = high_ref.shape[0]
    tile_id = lax.broadcasted_iota(jnp.int32, (tiles, width), 0)
    lane = lax.broadcasted_iota(jnp.int32, (1, width), 1)
    source = lax.broadcasted_iota(jnp.int32, (width, width + LANES), 0)
    column = lax.broadcasted_iota(jnp.int32, (width, width + LANES), 1)
    one, zero = jnp.ones((), jnp.bfloat16), jnp.zeros((), jnp.bfloat16)
    upto = jnp.where((source <= column) | (column >= width), 1.0, 0.0).astype(jnp.bfloat16)
    tile_mark = tile_id.astype(jnp.float32).astype(jnp.bfloat16)
    spare_id = lax.broadcasted_iota(jnp.int32, (8, width), 0)
    nothing = jnp.zeros((8, width), jnp.float32)

    def as_bf16(x):
        return x.astype(jnp.float32).astype(jnp.bfloat16)

    def pick(mark, found, before):
        place = found[:, :width].astype(jnp.bfloat16) + jnp.concatenate([before] * (width // LANES), axis=1)
        place = jnp.where(mark, place, zero)
        while place.shape[0] > 16:
            half = place.shape[0] // 2
            place = place[:half, :] + place[half:, :]
        order = jnp.sum(place.astype(jnp.float32), axis=0, keepdims=True).astype(jnp.int32) - 1
        return order, before + found[:, width:].astype(jnp.bfloat16)

    def rank(g, befores):
        before, twin_before = befores
        marks, twin_marks, info = [], [], []
        for c in range(TOGETHER):
            i = g * TOGETHER + c
            here = pl.ds(pl.multiple_of(i * width, width), width)
            live = i * width + lane < count
            tile = jnp.where(live, tile_ref[:, here], tiles)
            match = tile_mark == as_bf16(tile)
            mark = jnp.where(match, one, zero)
            hits[:, here] = mark
            marks.append(mark)
            cell = cell_ref[:, here]
            along = cell & (COLS_DEV - 1)
            place = tile & (across - 1)
            west = live & (along == 0) & (place > 0)
            east = live & (along == COLS_DEV - 1) & (place < across - 1)
            twin = jnp.where(west, tile - 1, jnp.where(east, tile + 1, tiles))
            twin_match = tile_mark == as_bf16(twin)
            twin_mark = jnp.where(twin_match, one, zero)
            twins[:, here] = twin_mark
            twin_marks.append(twin_mark)
            code = jnp.where(west, ROWS_DEV, 0) + lax.shift_right_logical(cell, 8)
            info.append((tile, live, here, i, cell, code, match, twin_match))
        found = jnp.dot(jnp.concatenate(marks, axis=0), upto, preferred_element_type=jnp.float32)
        twin_found = jnp.dot(jnp.concatenate(twin_marks, axis=0), upto, preferred_element_type=jnp.float32)
        for c in range(TOGETHER):
            tile, live, here, i, cell, code, match, twin_match = info[c]
            level, before = pick(match, found[c * tiles : (c + 1) * tiles, :], before)
            slot = jnp.where(live, tile * LANES + level, tiles * LANES - 1)
            pos_f[pl.ds(pl.multiple_of(i * width, width), width)] = slot.reshape(width)
            at_level = tile_mark[:CAP, :] == as_bf16(level)
            coded[:CAP, here] = jnp.where(at_level, as_bf16(lax.shift_right_logical(cell, 6)), zero)
            coded[CAP:, here] = jnp.where(at_level, as_bf16(cell & 63), zero)
            order, twin_before = pick(twin_match, twin_found[c * tiles : (c + 1) * tiles, :], twin_before)
            at_order = spare_id == order
            point = i * width + lane
            high = jnp.where(at_order, (point & -LANES).astype(jnp.float32), nothing)
            low = jnp.where(at_order, (point & (LANES - 1)).astype(jnp.float32), nothing)
            value = jnp.where(at_order, code.astype(jnp.float32), nothing)
            twin_code[:16, here] = jnp.concatenate([high, low], axis=0).astype(jnp.bfloat16)
            twin_code[16:, here] = jnp.concatenate([value, nothing], axis=0).astype(jnp.bfloat16)
        return before, twin_before

    start = jnp.zeros((tiles, LANES), jnp.bfloat16)
    total, twin_total = lax.fori_loop(0, chunks // TOGETHER, rank, (start, start))
    total, twin_total = total.astype(jnp.float32), twin_total.astype(jnp.float32)
    across_lanes = (((1,), (1,)), ((), ()))
    extra = lax.dot_general(twin_code[...], twins[...], across_lanes, preferred_element_type=jnp.float32)
    twin_f[...] = (extra[:8, :] + extra[8:16, :]).astype(jnp.int32).reshape(8 * tiles)
    spot = lax.broadcasted_iota(jnp.int32, (tiles, LANES), 1).astype(jnp.float32)
    blank = jnp.zeros((CAP, tiles), jnp.float32)
    codes = jnp.concatenate([blank, extra[16:, :], jnp.zeros((LANES - CAP - 16, tiles), jnp.float32)], axis=0).T
    cells = lax.dot_general(coded[...], hits[...], across_lanes, preferred_element_type=jnp.float32)
    filler = jnp.zeros((LANES - CAP, tiles), jnp.float32)
    high = jnp.where(spot < total, jnp.concatenate([cells[:CAP, :], filler], axis=0).T, float(DUMP // 64))
    low = jnp.where(spot < total, jnp.concatenate([cells[CAP:, :], filler], axis=0).T, float(DUMP % 64))
    low = jnp.where((spot >= CAP) & (spot - CAP < jnp.minimum(twin_total, float(SPARE))), codes, low)
    full = jnp.max(twin_total, axis=0, keepdims=True) > SPARE
    high = jnp.where(spot == LANES - 1, 0.0, high)
    low = jnp.where(spot == LANES - 1, jnp.where(full, 1.0, 0.0), low)
    high_ref[...] = high
    low_ref[...] = low


def pack_kernel(
    count_ref, pos_f, twin_f, high_ref, low_ref, feats_ref, out_ref, rows, slots, pos_s, twin_s, sem, twin_sem
):
    count = count_ref[0]
    points = feats_ref.shape[0]
    tiles = out_ref.shape[0]
    to_smem = pltpu.make_async_copy(pos_f, pos_s, sem)
    to_smem.start()
    twins_to_smem = pltpu.make_async_copy(twin_f, twin_s, twin_sem)
    twins_to_smem.start()
    rows[...] = feats_ref[...].astype(jnp.float32)
    to_smem.wait()

    def move(i, carry):
        for k in range(MOVES):
            slot = pos_s.at[pl.ds(k, points - MOVES + 1)][i * MOVES]
            slots[pl.ds(slot, 1), :] = rows[pl.ds(i * MOVES + k, 1), :]
        return carry

    lax.fori_loop(0, (count + (MOVES - 1)) // MOVES, move, 0)
    twins_to_smem.wait()

    def move_twins(t, carry):
        for u in range(8):
            for j in range(SPARE):
                point = twin_s.at[pl.ds(j * tiles + u, tiles - 7)][t * 8]
                slots[pl.ds(t * (8 * LANES) + u * LANES + CAP + 2 + j, 1), :] = rows[pl.ds(point, 1), :]
        return carry

    lax.fori_loop(0, tiles // 8, move_twins, 0)
    slots[pl.ds(CAP, tiles, LANES), :] = high_ref[...]
    slots[pl.ds(CAP + 1, tiles, LANES), :] = low_ref[...]

    def narrow(t, carry):
        out_ref[t] = slots[pl.ds(pl.multiple_of(t * LANES, LANES), BLOCK), :].astype(jnp.bfloat16)
        return carry

    lax.fori_loop(0, tiles, narrow, 0, unroll=4)


def add_kernel(
    got_ref, out_ref, top_ref, bottom_ref, sides_ref, full_ref,
    even, odd, coded, cells_f, cells_s, sem, *sums,
):
    sources = got_ref.shape[0]
    coded[...] = got_ref[:, CAP:, :].astype(jnp.float32).reshape(coded.shape)
    high = coded[pl.ds(0, sources, 8), :].astype(jnp.int32)
    low = coded[pl.ds(1, sources, 8), :].astype(jnp.int32)
    cells = high * 64 + low
    full_ref[0] = jnp.max(cells[:, LANES - 1 :])
    cells_f[...] = cells.reshape(sources * LANES)
    to_smem = pltpu.make_async_copy(cells_f, cells_s, sem)
    to_smem.start()

    def clear(i, carry):
        for part in sums:
            part[pl.ds(pl.multiple_of(i * 256, 256), 256), :] = jnp.zeros((256, LANES), jnp.float32)
        return carry

    lax.fori_loop(0, CELLS // 256, clear, 0)
    for part in sums:
        part[pl.ds(CELLS, HALO + 8), :] = jnp.zeros((HALO + 8, LANES), jnp.float32)

    def widen(s, rows):
        rows[...] = got_ref[jnp.minimum(s, sources - 1)].astype(jnp.float32)

    def add(s, rows):
        for j in range(CAP + SPARE):
            cell = pl.ds(cells_s.at[pl.ds(j, (sources - 1) * LANES + 1)][s * LANES], 1)
            part = sums[j % SUMS]
            k = j if j < CAP else j + 2
            part[cell, :] = part[cell, :] + rows[k : k + 1, :]

    def two(q, carry):
        widen(2 * q + 1, odd)
        add(2 * q, even)
        widen(2 * q + 2, even)
        add(2 * q + 1, odd)
        return carry

    to_smem.wait()
    widen(0, even)
    lax.fori_loop(0, sources // 2, two, 0)
    step = 256

    def close(i, carry):
        at = pl.ds(pl.multiple_of(i * step, step), step)
        total = sums[0][at, :]
        for part in sums[1:]:
            total = total + part[at, :]
        out_ref[at, :] = total.astype(jnp.bfloat16)
        return carry

    lax.fori_loop(0, CELLS // step, close, 0)

    def column(start, stride):
        at = pl.ds(start, ROWS_DEV, stride)
        total = sums[0][at, :]
        for part in sums[1:]:
            total = total + part[at, :]
        return total

    west, east = column(CELLS, 1), column(CELLS + ROWS_DEV, 1)
    sides_ref[:ROWS_DEV, :] = west.astype(jnp.bfloat16)
    sides_ref[ROWS_DEV:, :] = east.astype(jnp.bfloat16)
    spot = lax.broadcasted_iota(jnp.int32, (EDGE, LANES), 0)
    for ref, r in ((top_ref, 0), (bottom_ref, ROWS_DEV - 1)):
        ref[:COLS_DEV, :] = out_ref[r * COLS_DEV : (r + 1) * COLS_DEV, :]
        corners = jnp.where(spot == 0, west[r : r + 1, :], jnp.where(spot == 1, east[r : r + 1, :], 0.0))
        ref[COLS_DEV:, :] = corners.astype(jnp.bfloat16)


def fill_wide(weight_ref, wide):
    for i in range(4):
        for b in range(3):
            for o in range(2):
                block = (slice(i * LANES, (i + 1) * LANES), slice((2 * b + o) * LANES, (2 * b + o + 1) * LANES))
                wide[block] = weight_ref[i - o, b] if 0 <= i - o < 3 else jnp.zeros((LANES, LANES), jnp.bfloat16)


def conv_rows(row, pairs, west, east, bias, out_ref, wide, before, after):
    for k, p in enumerate(pairs):
        four = jnp.concatenate([row(2 * p - 1 + i) for i in range(4)], axis=1)
        taps = jnp.dot(four, wide[...], preferred_element_type=jnp.float32)
        before[7:8, :] = west[k : k + 1, :]
        before[8:, :] = taps[:, : 2 * LANES]
        after[:COLS_DEV, :] = taps[:, 4 * LANES :]
        after[COLS_DEV : COLS_DEV + 1, :] = east[k : k + 1, :]
        total = taps[:, 2 * LANES : 4 * LANES] + before[7 : 7 + COLS_DEV, :] + after[1 : 1 + COLS_DEV, :]
        done = jnp.maximum(total + jnp.concatenate([bias, bias], axis=1), 0.0).astype(jnp.bfloat16)
        out_ref[2 * k * COLS_DEV : (2 * k + 1) * COLS_DEV, :] = done[:, :LANES]
        out_ref[(2 * k + 1) * COLS_DEV : (2 * k + 2) * COLS_DEV, :] = done[:, LANES:]


def beside(corner, start, above, below, sides_ref, wide, side):
    side[:1, :] = above[corner : corner + 1, :]
    side[1 : ROWS_DEV + 1, :] = sides_ref[corner * ROWS_DEV : (corner + 1) * ROWS_DEV, :].astype(jnp.float32)
    side[ROWS_DEV + 1 : ROWS_DEV + 2, :] = below[corner : corner + 1, :]
    four = jnp.concatenate([side[pl.ds(i, ROWS_DEV // 2, 2), :] for i in range(4)], axis=1)
    return jnp.dot(four.astype(jnp.bfloat16), wide[:, start : start + 2 * LANES], preferred_element_type=jnp.float32)


def inner_kernel(bev_ref, sides_ref, weight_ref, bias_ref, out_hbm, wide, out, before, after, side, sem):
    fill_wide(weight_ref, wide)
    nothing = jnp.zeros((EDGE, LANES), jnp.float32)
    west = beside(0, 0, nothing, nothing, sides_ref, wide, side)
    east = beside(1, 4 * LANES, nothing, nothing, sides_ref, wide, side)

    def row(r):
        return bev_ref[r * COLS_DEV : (r + 1) * COLS_DEV, :]

    last = ROWS_DEV // 2 - 1
    conv_rows(row, range(1, last), west[1:last, :], east[1:last, :], bias_ref[...], out, wide, before, after)
    part = pl.ds(2 * COLS_DEV, (ROWS_DEV - 4) * COLS_DEV)
    store = pltpu.make_async_copy(out, out_hbm.at[part], sem)
    store.start()
    store.wait()


def outer_kernel(
    conv_ref, bev_ref, up_ref, down_ref, sides_ref, wide, bias_ref,
    out_hbm, out, before, after, side, sems,
):
    above = up_ref[COLS_DEV:, :].astype(jnp.float32)
    below = down_ref[COLS_DEV:, :].astype(jnp.float32)
    west = beside(0, 0, above, below, sides_ref, wide, side)
    east = beside(1, 4 * LANES, above, below, sides_ref, wide, side)

    def row(r):
        if r < 0:
            return up_ref[:COLS_DEV, :]
        if r >= ROWS_DEV:
            return down_ref[:COLS_DEV, :]
        return bev_ref[r * COLS_DEV : (r + 1) * COLS_DEV, :]

    last = ROWS_DEV // 2 - 1
    ends = (0, last)
    pick = [jnp.concatenate([x[:1, :], x[last:, :]], axis=0) for x in (west, east)]
    conv_rows(row, ends, *pick, bias_ref[...], out, wide, before, after)
    size = 2 * COLS_DEV
    stores = [
        pltpu.make_async_copy(out.at[pl.ds(k * size, size)], out_hbm.at[pl.ds(p * size, size)], sems.at[k])
        for k, p in enumerate(ends)
    ]
    for store in stores:
        store.start()
    for store in stores:
        store.wait()


VMEM = pl.BlockSpec(memory_space=pltpu.VMEM)
SMEM = pl.BlockSpec(memory_space=pltpu.SMEM)
ANY = pl.BlockSpec(memory_space=pl.ANY)


def pack(point_feats, point_tile, point_cell, point_count, devices, across=8):
    points, channels = point_feats.shape
    if across & (across - 1):
        raise ValueError("across")
    bf16, f32, i32 = jnp.bfloat16, jnp.float32, jnp.int32
    params = pltpu.CompilerParams(vmem_limit_bytes=PACK_VMEM)
    placed = pl.pallas_call(
        functools.partial(place_kernel, across),
        out_shape=[
            jax.ShapeDtypeStruct((points,), i32),
            jax.ShapeDtypeStruct((devices * 8,), i32),
            jax.ShapeDtypeStruct((devices, LANES), f32),
            jax.ShapeDtypeStruct((devices, LANES), f32),
        ],
        in_specs=[SMEM, VMEM, VMEM],
        out_specs=[VMEM] * 4,
        scratch_shapes=[
            pltpu.VMEM((devices, points), bf16),
            pltpu.VMEM((2 * CAP, points), bf16),
            pltpu.VMEM((devices, points), bf16),
            pltpu.VMEM((32, points), bf16),
        ],
        compiler_params=params,
        cost_estimate=pl.CostEstimate(flops=2 * points * devices * 1024, bytes_accessed=8 * points, transcendentals=0),
        name="place",
    )(point_count, point_cell.reshape(1, points), point_tile.reshape(1, points))
    return pl.pallas_call(
        pack_kernel,
        out_shape=jax.ShapeDtypeStruct((devices, BLOCK, channels), bf16),
        in_specs=[SMEM] + [VMEM] * 5,
        out_specs=VMEM,
        scratch_shapes=[
            pltpu.VMEM((points, channels), f32),
            pltpu.VMEM((devices * LANES, channels), f32),
            pltpu.SMEM((points,), i32),
            pltpu.SMEM((devices * 8,), i32),
            pltpu.SemaphoreType.DMA,
            pltpu.SemaphoreType.DMA,
        ],
        compiler_params=params,
        name="pack",
    )(point_count, *placed, point_feats)


def add_up(got):
    devices, block, channels = got.shape
    bf16, f32, i32 = jnp.bfloat16, jnp.float32, jnp.int32
    heights = (CELLS, COLS_DEV + EDGE, COLS_DEV + EDGE, HALO)
    return pl.pallas_call(
        add_kernel,
        out_shape=[jax.ShapeDtypeStruct((height, channels), bf16) for height in heights]
        + [jax.ShapeDtypeStruct((1,), i32)],
        in_specs=[VMEM],
        out_specs=[VMEM] * 4 + [SMEM],
        compiler_params=pltpu.CompilerParams(vmem_limit_bytes=ADD_VMEM),
        scratch_shapes=[
            pltpu.VMEM((block, channels), f32),
            pltpu.VMEM((block, channels), f32),
            pltpu.VMEM((devices * 8, channels), f32),
            pltpu.VMEM((devices * LANES,), i32),
            pltpu.SMEM((devices * LANES,), i32),
            pltpu.SemaphoreType.DMA,
        ]
        + [pltpu.VMEM((CELLS + HALO + 8, channels), f32)] * SUMS,
        name="add_up",
    )(got)


def shift(cells, axis, step):
    count = lax.axis_size(axis)
    pairs = [(i, i + step) for i in range(count) if 0 <= i + step < count]
    return lax.ppermute(cells, axis, pairs)


def conv_call(kernel, name, ins, rows, sems, aliases, flops, extra, *operands):
    bev, channels = operands[-4 if len(ins) == 4 else 1], LANES
    bf16, f32 = jnp.bfloat16, jnp.float32
    return pl.pallas_call(
        kernel,
        out_shape=[jax.ShapeDtypeStruct(bev.shape, bf16)] + extra,
        in_specs=ins,
        out_specs=[ANY] + [VMEM] * len(extra),
        input_output_aliases=aliases,
        scratch_shapes=[
            pltpu.VMEM((rows * COLS_DEV, channels), bf16),
            pltpu.VMEM((COLS_DEV + 8, 2 * channels), f32),
            pltpu.VMEM((COLS_DEV + 8, 2 * channels), f32),
            pltpu.VMEM((ROWS_DEV + 8, channels), f32),
            sems,
        ],
        compiler_params=pltpu.CompilerParams(vmem_limit_bytes=16 * 2**20),
        cost_estimate=pl.CostEstimate(flops=flops, bytes_accessed=2 * rows * COLS_DEV * channels, transcendentals=0),
        name=name,
    )(*operands)


def exchange_columns(bev, top, bottom, sides):
    cells = bev.reshape(ROWS_DEV, COLS_DEV, -1)
    west, east = shift(cells[:, -1], "gy", 1), shift(cells[:, 0], "gy", -1)
    rest = jnp.zeros((EDGE - 2, west.shape[1]), west.dtype)
    top = jnp.concatenate([top[:COLS_DEV], west[:1], east[:1], rest], axis=0)
    bottom = jnp.concatenate([bottom[:COLS_DEV], west[ROWS_DEV - 1 :], east[ROWS_DEV - 1 :], rest], axis=0)
    return top, bottom, jnp.concatenate([west, east], axis=0)


def keep_columns(bev, top, bottom, sides):
    return top, bottom, sides


def shards(point_feats, point_tile, point_cell, point_count, conv_weight, conv_bias):
    across = lax.axis_size("gy")
    devices = lax.axis_size("gx") * across
    channels = point_feats.shape[1]
    sent = pack(point_feats, point_tile, point_cell, point_count, devices, across)
    got = lax.all_to_all(sent, ("gx", "gy"), split_axis=0, concat_axis=0, tiled=True)
    bev, top, bottom, sides, full = add_up(got)
    top, bottom, sides = lax.switch(full[0], (keep_columns, exchange_columns), bev, top, bottom, sides)
    up = shift(bottom, "gx", 1)
    down = shift(top, "gx", -1)
    bias = conv_bias.reshape(1, channels)
    dma = pltpu.SemaphoreType.DMA
    work = 2 * CELLS * 9 * channels * channels
    inner, wide = conv_call(
        inner_kernel, "inner", [VMEM] * 4, ROWS_DEV - 4, dma, {}, work,
        [jax.ShapeDtypeStruct((4 * channels, 6 * channels), jnp.bfloat16)], bev, sides, conv_weight, bias
    )
    (conv_out,) = conv_call(
        outer_kernel, "outer", [ANY] + [VMEM] * 6, 4, dma((2,)), {0: 0}, work // 4, [],
        inner, bev, up, down, sides, wide, bias,
    )
    whole = (ROWS_DEV, COLS_DEV, channels)
    return (bev.reshape(whole), conv_out.reshape(whole))


def solution(mesh):
    in_specs = (
        P(("gx", "gy"), None),
        P(("gx", "gy"), None),
        P(("gx", "gy")),
        P(("gx", "gy")),
        P(),
        P(),
    )
    out_specs = (P("gx", "gy", None), P("gx", "gy", None))
    return jax.shard_map(shards, mesh=mesh, in_specs=in_specs, out_specs=out_specs, check_vma=False)
```
